32 devices in a mesh: bx: 4 (over z), by: 2 (over x), bz: 4 (over y, core).
Axes of the slice: x: 2, y: 2, z: 4, core: 2. Of those that a mesh axis runs over, the one named last changes fastest.
Arguments:
- estimate: float32 [64, 32, 512], P('bx', 'by', 'bz'), may hold values from 0.2 to 5
- observed: float32 [8, 64, 32, 512], P(None, 'bx', 'by', 'bz'), may hold values from 0.3 to 180, as said below
- coverage: int32 [8, 4, 2, 4], P(None, 'bx', 'by', 'bz'), may hold values from 0 to 1, as said below
- psf_taps: float32 [8, 3, 17], replicated, may hold values from 0.05 to 1
Outputs:
- refined: float32 [64, 32, 512], P('bx', 'by', 'bz')
The draws below stay inside these ranges and needn't reach their ends.
Inputs may be any that keep to these rules, and one draw needn't show every extreme that they name: `coverage`: each block is covered by 2 to 8 views; in every draw some block is covered by all 8. `observed`: positive.
All inputs are finite; a program needn't handle non-finite values.
Results may differ from the reference program's by a relative error of at most 0.0001.
Values sent between devices are 32-bit elements; how exact they have to be, the bound alone decides.
A program may use at most 64 MiB of HBM per device.

```python
import math
import jax
import jax.numpy as jnp
from jax import lax

V = 8
R = 8
CX = 16
CY = 16
CZ = 128
NX = 64
NY = 32
NZ = 512
N_BX = 4
N_BY = 2
N_BZ = 4


def draw_observed(key, part):
    first, second = jax.random.split(key, 2)
    blocks_x = NX // CX
    blocks_y = NY // CY
    blocks_z = NZ // CZ
    coarse = jnp.exp(jax.random.uniform(first, (blocks_x, blocks_y, blocks_z), jnp.float32, 0.0, jnp.log(10.0)))
    ramp = 1.0 + 2.0 * jnp.arange(blocks_y, dtype=jnp.float32) / max(blocks_y - 1, 1)
    coarse = coarse * ramp[None, :, None]
    grown = jnp.repeat(jnp.repeat(jnp.repeat(coarse, CX, axis=0), CY, axis=1), CZ, axis=2)
    voxel = jnp.exp(jax.random.uniform(second, (V, NX, NY, NZ), jnp.float32, jnp.log(0.3), jnp.log(3.0)))
    values = voxel * grown[None]
    return values.astype(jnp.float32)


def draw_coverage(key, part):
    blocks = NX // CX * (NY // CY) * (NZ // CZ)
    first, second, third = jax.random.split(jax.random.fold_in(key, 7), 3)
    counts = jax.random.randint(first, (blocks,), 2, V + 1)
    fullest = jax.random.randint(second, (), 0, blocks)
    counts = counts.at[fullest].set(V)
    ranks = jax.vmap(lambda each: jax.random.permutation(each, V))(jax.random.split(third, blocks))
    covered = (ranks < counts[:, None]).astype(jnp.int32)
    return covered.T.reshape(V, NX // CX, NY // CY, NZ // CZ)


def levels(key, dims, cuts, least, high):
    def one(position, shards_of):
        steps = jax.random.uniform(jax.random.fold_in(jax.random.fold_in(key, 6), position), (shards_of,), jnp.float32, least / len(cuts), high / len(cuts))
        return jnp.repeat(jnp.exp(steps), dims[position] // shards_of).reshape((-1,) + (1,) * (len(dims) - position - 1))

    factor_of = one(*cuts[0])
    for cut in cuts[1:]:
        factor_of = factor_of * one(*cut)
    return factor_of


def setup_inputs(seed: int = 0) -> dict:
    key_list = jax.random.split(jax.random.key(seed), 5)
    return {
        "estimate": jnp.clip(jnp.exp(math.log(5.0) - 3.218876 * jax.random.uniform(key_list[0], (NX, NY, NZ), jnp.float32) ** levels(key_list[0], (NX, NY, NZ), ((0, 4), (1, 2), (2, 4)), -0.2, 0.2)), 0.2, 5.0),
        "observed": draw_observed(jax.random.fold_in(key_list[4], 71), 0),
        "coverage": draw_coverage(jax.random.fold_in(key_list[4], 71), 0),
        "psf_taps": jnp.clip(jnp.exp(jax.random.uniform(key_list[3], (V, 3, 2 * R + 1), jnp.float32, math.log(0.05), math.log(1.0))), 0.05, 1.0),
    }


def blur_axis(field, taps_row, axis):
    moved = jnp.moveaxis(field, axis, -1)
    shape = moved.shape
    flat = moved.reshape(-1, 1, shape[-1])
    kernel = taps_row.reshape(1, 1, -1)
    width = (taps_row.shape[0] - 1) // 2
    result = lax.conv_general_dilated(flat, kernel, (1,), [(width, width)], precision=lax.Precision.HIGHEST)
    return jnp.moveaxis(result.reshape(shape), -1, axis)


def blur_volume(field, kernels):
    result = field
    for axis in range(3):
        result = blur_axis(result, kernels[axis], axis)
    return result


def spread(block_values):
    grown = jnp.broadcast_to(block_values[:, None, :, None, :, None], (N_BX, CX, N_BY, CY, N_BZ, CZ))
    return grown.reshape(NX, NY, NZ)


def reference(estimate, observed, coverage, psf_taps):
    taps = psf_taps / jnp.sum(psf_taps, axis=2, keepdims=True)
    weights = coverage.astype(jnp.float32)
    count = spread(jnp.sum(weights, axis=0))
    summed = jnp.zeros((NX, NY, NZ), jnp.float32)
    target_field = jnp.zeros((NX, NY, NZ), jnp.float32)
    for view in range(V):
        blurred = blur_volume(estimate, taps[view])
        ratio = observed[view] / blurred
        back = blur_volume(ratio, taps[view][:, ::-1])
        weight_full = spread(weights[view])
        summed = summed + weight_full * back
        target_field = target_field + weight_full * observed[view]
    updated = estimate * (summed / count)
    target = jnp.sum(target_field / count)
    total = jnp.sum(updated)
    return updated * (target / total)
```

```python
import functools

import jax
import jax.numpy as jnp
from jax import lax
from jax.experimental import pallas as pl
from jax.experimental.pallas import tpu as pltpu
from jax.sharding import PartitionSpec as P

F32 = jnp.float32
BF16 = jnp.bfloat16
MESH = pl.DeviceIdType.MESH


def split(values):
    high = values.astype(BF16)
    low = (values - high.astype(F32)).astype(BF16)
    return high, low


def dot(left, right, dims=((1,), (0,))):
    return lax.dot_general(left, right, (dims, ((), ())), preferred_element_type=F32)


def folded(values):
    half = values.shape[1] // 2
    return values[:, :half] + values[:, half:]


def rings(sizes):
    offsets = [(i, j, k) for i in range(sizes[0]) for j in range(sizes[1]) for k in range(sizes[2])]
    offsets = offsets[1:]
    if len(offsets) < 64:
        return offsets, offsets, []
    return (
        offsets,
        [offset for offset in offsets if offset[0] == 0],
        [offset for offset in offsets if offset[1:] == (0, 0)],
    )


def kernel(
    sizes,
    taps_hbm,
    cover_hbm,
    est_hbm,
    obs_hbm,
    out_ref,
    taps_ref,
    cover_ref,
    obs,
    ext,
    ext_hi,
    ext_lo,
    pack,
    from_left,
    from_right,
    edge,
    weight,
    scale,
    inverses,
    band,
    twin,
    gath_hi,
    gath_lo,
    scat,
    lined,
    spread,
    total,
    fringe,
    back_pack,
    back_left,
    back_right,
    back_xy,
    stat,
    stat_a,
    stat_b,
    part_a,
    fetch_sem,
    hop_sem,
    out_send,
    out_recv,
    back_send,
    back_recv,
    a_send,
    a_recv,
    b_send,
    b_recv,
):
    n_x, n_y, n_z = sizes
    views, rows, cols, lanes = obs.shape
    length = taps_ref.shape[2]
    rad = (length - 1) // 2
    wide_x, wide_y = rows + 2 * rad, cols + 2 * rad
    groups = wide_x // 8
    me_x, me_y, me_z = lax.axis_index("bx"), lax.axis_index("by"), lax.axis_index("bz")

    own_x, own_y = slice(rad, rad + rows), slice(rad, rad + cols)
    own = ext.at[own_x, own_y, :]
    loads = [
        pltpu.make_async_copy(source, target, fetch_sem.at[which])
        for which, (source, target) in enumerate(
            ((est_hbm, own), (cover_hbm, cover_ref), (taps_hbm, taps_ref), (obs_hbm, obs))
        )
    ]
    for load in loads:
        load.start()

    def exists(dx, dy, dz):
        ok = None
        for step, me, count in ((dx, me_x, n_x), (dy, me_y, n_y), (dz, me_z, n_z)):
            if step == 0:
                continue
            inside = (me + step >= 0) & (me + step < count)
            ok = inside if ok is None else ok & inside
        return ok

    def device(dx, dy, dz):
        return {"bx": me_x + dx, "by": me_y + dy, "bz": me_z + dz}

    steps = (-1, 0, 1)
    around = [(dx, dy, dz) for dz in steps for dx in steps for dy in steps if (dx, dy, dz) != (0, 0, 0)]
    ring_all, ring_a, ring_b = rings(sizes)

    def partner(i, j, k):
        return {
            "bx": lax.rem(me_x + i, n_x),
            "by": lax.rem(me_y + j, n_y),
            "bz": lax.rem(me_z + k, n_z),
        }

    for part in ((slice(0, rad), slice(0, wide_y)), (slice(rad + rows, wide_x), slice(0, wide_y))):
        ext[part[0], part[1], :] = jnp.zeros((rad, wide_y, lanes), F32)
    for part in (slice(0, rad), slice(rad + cols, wide_y)):
        ext[own_x, part, :] = jnp.zeros((rows, rad, lanes), F32)
    from_left[...] = jnp.zeros(from_left.shape, F32)
    from_right[...] = jnp.zeros(from_right.shape, F32)
    weight[...] = jnp.zeros(weight.shape, F32)

    barrier = pltpu.get_barrier_semaphore()
    faces = [offset for offset in around if sum(map(abs, offset)) == 1]
    near_by = sum(exists(*offset).astype(jnp.int32) for offset in faces)
    rounds = n_x + n_y + n_z - 3

    def greet(which):
        semaphore = barrier if which == 0 else hop_sem.at[which - 1]
        for offset in faces:

            @pl.when(exists(*offset))
            def _():
                pl.semaphore_signal(semaphore, inc=1, device_id=device(*offset), device_id_type=MESH)

    def meet(which):
        pl.semaphore_wait(barrier if which == 0 else hop_sem.at[which - 1], near_by)
        if which + 1 < rounds:
            greet(which + 1)

    greet(0)

    back_xy[...] = jnp.zeros(back_xy.shape, F32)
    back_left[...] = jnp.zeros(back_left.shape, F32)
    back_right[...] = jnp.zeros(back_right.shape, F32)
    total[...] = jnp.zeros(total.shape, F32)
    fringe[...] = jnp.zeros(fringe.shape, F32)

    loads[1].wait()
    lane = lax.broadcasted_iota(jnp.int32, (1, lanes), 1)
    row = jnp.zeros((1, lanes), F32)
    for v in range(views):
        mine = jnp.full((1, lanes), cover_ref[v], jnp.int32).astype(F32)
        row = jnp.where(lane // (lanes // views) == v, mine, row)
    weight[13] = row
    loads[0].wait()

    lane = lax.broadcasted_iota(jnp.int32, (cols, lanes), 1)
    for g in range(rows // 8):
        merged = jnp.zeros((cols, lanes), F32)
        for i in range(8):
            rolled = pltpu.roll(ext[rad + 8 * g + i, own_y, :], 2 * rad * i + rad, 1)
            merged = jnp.where(lane // (2 * rad) == i, rolled, merged)
        pack[g] = merged

    def cut(step, size, width):
        return pl.ds(0, size) if step == 0 else pl.ds(0 if step < 0 else size - width, width)

    def wide(step, size, width):
        return pl.ds(width, size) if step == 0 else pl.ds(0 if step < 0 else width + size, width)

    pack_rows, pack_rad = rows // 8, rad // 8

    def slot_of(dx, dy, dz):
        return 9 * (dz + 1) + 3 * (dx + 1) + dy + 1

    def out_copies(hops):
        for dx, dy, dz in sorted(around, key=lambda offset: abs(offset[2])):
            if sum(map(abs, (dx, dy, dz))) not in hops:
                continue
            slot = slot_of(dx, dy, dz)
            size, width = (rows, rad) if dz == 0 else (pack_rows, pack_rad)
            source = own if dz == 0 else pack
            target = (from_right, ext, from_left)[dz + 1]
            pairs = (
                (weight.at[13], weight.at[slot_of(-dx, -dy, -dz)]),
                (
                    source.at[cut(dx, size, width), cut(dy, cols, rad), :],
                    target.at[wide(-dx, size, width), wide(-dy, cols, rad), :],
                ),
            )
            copies = [
                pltpu.make_async_remote_copy(
                    src_ref=pair[0],
                    dst_ref=pair[1],
                    send_sem=out_send.at[slot, which],
                    recv_sem=out_recv.at[slot, which],
                    device_id=device(dx, dy, dz),
                    device_id_type=MESH,
                )
                for which, pair in enumerate(pairs)
            ]
            yield exists(dx, dy, dz), exists(-dx, -dy, -dz), copies

    def back_copies():
        for dx, dy, dz in sorted(around, key=lambda offset: abs(offset[2])):
            slot = slot_of(dx, dy, dz)
            size, width = (rows, rad) if dz == 0 else (pack_rows, pack_rad)
            source = total if dz == 0 else back_pack
            target = (back_right, back_xy, back_left)[dz + 1]
            copy = pltpu.make_async_remote_copy(
                src_ref=source.at[wide(dx, size, width), wide(dy, cols, rad), :],
                dst_ref=target.at[wide(-dx, size, width), wide(-dy, cols, rad), :],
                send_sem=back_send.at[slot],
                recv_sem=back_recv.at[slot],
                device_id=device(dx, dy, dz),
                device_id_type=MESH,
            )
            yield exists(dx, dy, dz), exists(-dx, -dy, -dz), [copy]

    def start(family):
        for sends, _, copies in family:

            @pl.when(sends)
            def _():
                for copy in copies:
                    copy.start()

    def arrive(family):
        for _, takes, copies in family:

            @pl.when(takes)
            def _():
                for copy in copies:
                    copy.wait_recv()

    def leave(family):
        for sends, _, copies in family:

            @pl.when(sends)
            def _():
                for copy in copies:
                    copy.wait_send()

    def build(v, carry):
        def summed(dim):
            values = [taps_ref[dim, v, k] for k in range(length)]
            while len(values) > 1:
                values = [sum(values[i : i + 2]) for i in range(0, len(values), 2)]
            return jnp.full((8, lanes), values[0], F32)

        inverse = 1.0 / (summed(0) * summed(1) * summed(2))

        def chosen(offset, dim):
            result = jnp.zeros(offset.shape, F32)
            for k in range(length):
                result = jnp.where(offset == k, taps_ref[dim, v, k], result)
            return result

        def iota(shape, dim):
            return lax.broadcasted_iota(jnp.int32, shape, dim)

        shape = (lanes, lanes)
        main = chosen(iota(shape, 0) - iota(shape, 1) + rad, 2)
        shape = (2 * rad, lanes)
        row, col = iota(shape, 0), iota(shape, 1)
        edge = chosen(jnp.where(row < rad, row, row + lanes) - col, 2)
        for first, part in ((0, main), (lanes, edge)):
            part = (part.reshape(-1, 8, lanes) * inverse[None]).reshape(part.shape)
            high, low = split(part)
            band[v, first : first + part.shape[0], :] = jnp.concatenate([high, low], axis=1)
            twin[v, first : first + part.shape[0], :] = jnp.concatenate([high, high], axis=1)
        rest = band.shape[1] - lanes - 2 * rad
        band[v, lanes + 2 * rad :, :] = jnp.zeros((rest, 2 * lanes), BF16)
        twin[v, lanes + 2 * rad :, :] = jnp.zeros((rest, 2 * lanes), BF16)
        shape = (8 * cols, 8 * wide_y)
        row, col = iota(shape, 0), iota(shape, 1)
        offset = jnp.where(row // cols == col // wide_y, col % wide_y - row % cols, -1)
        high, low = split(chosen(offset, 1))
        gath_hi[v], gath_lo[v] = high, low
        shape = (8 * wide_y, 8 * cols)
        row, col = iota(shape, 0), iota(shape, 1)
        offset = jnp.where(row // wide_y == col // cols, row % wide_y - col % cols, -1)
        high, low = split(chosen(offset, 1))
        scat[v] = jnp.concatenate([high, low], axis=1)
        return carry

    meet(0)
    start(out_copies((1,)))
    loads[2].wait()
    stops = [min(stop, views) for stop in (0, 2, 4, 6, views)]
    for hop in range(1, 5):
        lax.fori_loop(stops[hop - 1], stops[hop], build, 0)
        if hop < rounds:
            meet(hop)
        if hop in (1, 2):
            start(out_copies((hop + 1,)))

    loads[3].wait()
    def weight_of(rows_of, v):
        first = v * (lanes // views)
        return jnp.broadcast_to(rows_of[:, first : first + 1], rows_of.shape)

    mine = jnp.broadcast_to(weight[13], (8, lanes))
    count = jnp.zeros((8, lanes), F32)
    seen = jnp.zeros((8, lanes), F32)
    for v in range(views):
        weight_v = weight_of(mine, v)
        count = count + weight_v
        seen = seen + weight_v * jnp.sum(obs[v].reshape(-1, 8, lanes), axis=0)
    count = count[0:1]
    stat[0:1] = jnp.sum(seen, axis=0, keepdims=True) / count
    for hop in range(5, rounds):
        meet(hop)

    arrive(out_copies((1, 2, 3)))
    lane = lax.broadcasted_iota(jnp.int32, (wide_y, lanes), 1)
    high, low = split(ext[...].reshape(wide_x * wide_y, lanes))
    ext_hi[:, :lanes] = high
    ext_lo[:, :lanes] = low
    for g in range(groups):
        merged = jnp.where(lane % (2 * rad) < rad, from_left[g], from_right[g])
        edge[g] = merged
        for i in range(8):
            shift = (lanes - 2 * rad * i) % lanes
            rolled = pltpu.roll(merged, shift, 1) if shift else merged
            high, low = split(rolled)
            first = (8 * g + i) * wide_y
            ext_hi[first : first + wide_y, lanes:] = high
            ext_lo[first : first + wide_y, lanes:] = low

    thin = lax.broadcasted_iota(jnp.int32, (rad, lanes), 1)
    everyone = jnp.concatenate([weight[slot] for slot in range(27)] + [jnp.zeros((5, lanes), F32)], axis=0)
    counts = jnp.zeros(everyone.shape, F32)
    for v in range(views):
        theirs = weight_of(everyone, v)
        counts = counts + theirs

        def spread_of(dx, dy, dz):
            slot = 9 * dz + 3 * dx + dy
            return jnp.broadcast_to(theirs[slot : slot + 1], (rad, lanes))

        for dx in range(3):
            for dy in range(3):
                mid, left, right = (spread_of(dx, dy, dz) for dz in (1, 0, 2))
                side = jnp.where(thin < rad, left, jnp.where(thin < 2 * rad, right, 0.0))
                first, last = ((0, rad), (rad, rad + cols), (rad + cols, wide_y))[dy]
                for at in range(first, last, rad):
                    scale[v, dx, at : at + rad, :lanes] = mid
                    scale[v, dx, at : at + rad, lanes:] = side
    inverses[...] = jnp.where(counts > 0.0, 1.0 / jnp.maximum(counts, 1.0), 0.0)

    def one_view(v, carry):
        size = 8 * wide_y
        high_part = slice(0, lanes)
        for g in range(groups):
            here = slice(g * size, (g + 1) * size)
            blurred = folded(dot(ext_hi[here, :], band[v])) + dot(ext_lo[here, :], band[v, :, high_part])
            high, low = split(blurred)
            line = folded(dot(gath_hi[v], jnp.concatenate([high, low], axis=1))) + dot(gath_lo[v], high)
            lined[8 * g : 8 * g + 8] = line.reshape(8, cols, lanes)
        blur = taps_ref[0, v, 0] * lined[0:rows]
        for k in range(1, length):
            blur = blur + taps_ref[0, v, k] * lined[k : k + rows]
        spread[...] = obs[v] / blur
        for g in range(groups):
            pieces = []
            for e in range(8 * g, 8 * g + 8):
                piece = None
                for a in range(rows):
                    if 0 <= e - a < length:
                        term = taps_ref[0, v, e - a] * spread[a]
                        piece = term if piece is None else piece + term
                pieces.append(piece)
            piece = jnp.concatenate(pieces, axis=0)
            both = jnp.concatenate(split(piece), axis=1)
            piece = folded(dot(scat[v], jnp.concatenate([both, both], axis=0)))
            high, low = split(piece)
            flip = ((1,), (1,))
            piece = dot(jnp.concatenate([high, low], axis=1), twin[v], flip)
            piece = piece + dot(high, band[v, :, lanes:], flip)
            piece = piece.reshape(8, wide_y, 2 * lanes)
            dx = 0 if 8 * g < rad else (1 if 8 * g < rad + rows else 2)
            piece = piece * scale[v, dx][None]
            total[8 * g : 8 * g + 8] += piece[:, :, :lanes]
            fringe[8 * g : 8 * g + 8] += piece[:, :, lanes:]
        return carry

    lax.fori_loop(0, views, one_view, 0, unroll=2)

    for g in range(groups):
        merged = fringe[8 * g]
        for i in range(1, 8):
            merged = merged + pltpu.roll(fringe[8 * g + i], 2 * rad * i, 1)
        back_pack[g] = merged
    seen = jnp.zeros((8, lanes), F32)
    for dx in range(3):
        for dy in range(3):
            first_y, last_y = ((0, rad), (rad, rad + cols), (rad + cols, wide_y))[dy]
            first_x, last_x = ((0, rad), (rad, rad + rows), (rad + rows, wide_x))[dx]
            part_y = slice(first_y, last_y)
            part = total[first_x:last_x, part_y, :] * ext[first_x:last_x, part_y, :]
            part = jnp.sum(part.reshape(-1, 8, lanes), axis=0)
            slot = 9 + 3 * dx + dy
            seen = seen + part * inverses[slot : slot + 1, :]
            part_x = slice(first_x // 8, last_x // 8)
            part = back_pack[part_x, part_y, :] * edge[part_x, part_y, :]
            part = jnp.sum(part.reshape(-1, 8, lanes), axis=0)
            left, right = (inverses[at : at + 1, :] for at in (slot - 9, slot + 9))
            seen = seen + part * jnp.where(lane[0:1] % (2 * rad) < rad, left, right)
    stat[1:2] = jnp.sum(seen, axis=0, keepdims=True)

    def sums_a():
        for slot, offset in enumerate(ring_a):
            yield pltpu.make_async_remote_copy(
                src_ref=stat,
                dst_ref=stat_a.at[slot],
                send_sem=a_send.at[slot],
                recv_sem=a_recv.at[slot],
                device_id=partner(*offset),
                device_id_type=MESH,
            )

    def sums_b():
        for slot, offset in enumerate(ring_b):
            yield pltpu.make_async_remote_copy(
                src_ref=part_a,
                dst_ref=stat_b.at[slot],
                send_sem=b_send.at[slot],
                recv_sem=b_recv.at[slot],
                device_id=partner(*offset),
                device_id_type=MESH,
            )

    for copy in sums_a():
        copy.start()
    start(back_copies())
    arrive(back_copies())
    near = back_xy[...]

    def fold(values, size, rad, axis):
        low = lax.slice_in_dim(values, 0, rad, axis=axis)
        mid = lax.slice_in_dim(values, rad, rad + size, axis=axis)
        top = lax.slice_in_dim(values, rad + size, 2 * rad + size, axis=axis)
        if size == 2 * rad:
            return mid + jnp.concatenate([low, top], axis=axis)
        gap_shape = list(low.shape)
        gap_shape[axis] = size - rad
        gap = jnp.zeros(gap_shape, F32)
        return mid + jnp.concatenate([low, gap], axis=axis) + jnp.concatenate([gap, top], axis=axis)

    near = fold(fold(near, rows, rad, 0), cols, rad, 1)
    ends = jnp.where((lane % (2 * rad) < rad)[None], back_right[...], back_left[...])
    ends = fold(fold(ends, pack_rows, pack_rad, 0), cols, rad, 1)
    lane = lax.broadcasted_iota(jnp.int32, (cols, lanes), 1)
    outer = (lane < rad) | (lane >= lanes - rad)
    for x in range(rows):
        rolled = pltpu.roll(ends[x // 8], lanes - (2 * rad * (x % 8) + rad), 1)
        summed = total[rad + x, rad : rad + cols, :] + near[x] + jnp.where(outer, rolled, 0.0)
        updated = ext[rad + x, own_y, :] * (summed / count)
        out_ref[x] = updated

    for copy in sums_a():
        copy.wait_recv()
    everything = stat[...] + jnp.sum(stat_a[...], axis=0)
    if ring_b:
        part_a[...] = everything
        for copy in sums_b():
            copy.start()
        for copy in sums_b():
            copy.wait_recv()
        everything = part_a[...] + jnp.sum(stat_b[...], axis=0)
    wanted = jnp.sum(everything[0:1], axis=1, keepdims=True)
    gotten = jnp.sum(everything[1:2], axis=1, keepdims=True)
    factor = jnp.broadcast_to(wanted, (1, lanes)) / jnp.broadcast_to(gotten, (1, lanes))
    out_ref[...] = out_ref[...] * factor.reshape(1, 1, lanes)

    for family in (out_copies((1, 2, 3)), back_copies()):
        leave(family)
    for copy in sums_a():
        copy.wait_send()
    for copy in sums_b():
        copy.wait_send()


def on_device(sizes, estimate, observed, coverage, psf_taps):
    rows, cols, lanes = estimate.shape
    views = observed.shape[0]
    rad = (psf_taps.shape[2] - 1) // 2
    wide_x, wide_y = rows + 2 * rad, cols + 2 * rad
    groups = wide_x // 8
    _, ring_a, ring_b = rings(sizes)
    n_a, n_b = len(ring_a), max(1, len(ring_b))

    def vm(*shape, dtype=F32):
        return pltpu.VMEM(shape, dtype)

    def dma(*shape):
        return pltpu.SemaphoreType.DMA(shape)

    views_all, dims, length = psf_taps.shape
    scratch = [
        pltpu.SMEM((dims, views_all, length), F32),
        pltpu.SMEM((views,), jnp.int32),
        vm(*observed.shape),
        vm(wide_x, wide_y, lanes),
        vm(wide_x * wide_y, 2 * lanes, dtype=BF16),
        vm(wide_x * wide_y, 2 * lanes, dtype=BF16),
        vm(rows // 8, cols, lanes),
        vm(groups, wide_y, lanes),
        vm(groups, wide_y, lanes),
        vm(groups, wide_y, lanes),
        vm(27, 1, lanes),
        vm(views, 3, wide_y, 2 * lanes),
        vm(32, lanes),
        vm(views, 2 * lanes, 2 * lanes, dtype=BF16),
        vm(views, 2 * lanes, 2 * lanes, dtype=BF16),
        vm(views, 8 * cols, 8 * wide_y, dtype=BF16),
        vm(views, 8 * cols, 8 * wide_y, dtype=BF16),
        vm(views, 8 * wide_y, 16 * cols, dtype=BF16),
        vm(wide_x, cols, lanes),
        vm(rows, cols, lanes),
        vm(wide_x, wide_y, lanes),
        vm(wide_x, wide_y, lanes),
        vm(groups, wide_y, lanes),
        vm(groups, wide_y, lanes),
        vm(groups, wide_y, lanes),
        vm(wide_x, wide_y, lanes),
        vm(2, lanes),
        vm(n_a, 2, lanes),
        vm(n_b, 2, lanes),
        vm(2, lanes),
        dma(4),
        pltpu.SemaphoreType.REGULAR((max(1, sum(sizes) - 4),)),
        dma(27, 2),
        dma(27, 2),
        dma(27),
        dma(27),
        dma(n_a),
        dma(n_a),
        dma(n_b),
        dma(n_b),
    ]
    return pl.pallas_call(
        functools.partial(kernel, sizes),
        out_shape=jax.ShapeDtypeStruct(estimate.shape, F32),
        in_specs=[
            pl.BlockSpec(memory_space=pl.ANY),
            pl.BlockSpec(memory_space=pl.ANY),
            pl.BlockSpec(memory_space=pl.ANY),
            pl.BlockSpec(memory_space=pl.ANY),
        ],
        out_specs=pl.BlockSpec(memory_space=pltpu.VMEM),
        scratch_shapes=scratch,
        compiler_params=pltpu.CompilerParams(collective_id=0, has_side_effects=True),
    )(jnp.transpose(psf_taps, (1, 0, 2)), coverage.reshape(views), estimate, observed)


def solution(mesh):
    sizes = tuple(mesh.shape[axis] for axis in ("bx", "by", "bz"))
    return jax.shard_map(
        functools.partial(on_device, sizes),
        mesh=mesh,
        in_specs=(P("bx", "by", "bz"), P(None, "bx", "by", "bz"), P(None, "bx", "by", "bz"), P()),
        out_specs=P("bx", "by", "bz"),
        check_vma=False,
    )
```

```python
import functools

import jax
import jax.numpy as jnp
from jax import lax
from jax.experimental import pallas as pl
from jax.experimental.pallas import tpu as pltpu
from jax.sharding import PartitionSpec as P

F32 = jnp.float32
BF16 = jnp.bfloat16
MESH = pl.DeviceIdType.MESH


def split(values):
    high = values.astype(BF16)
    low = (values - high.astype(F32)).astype(BF16)
    return high, low


def dot(left, right, dims=((1,), (0,))):
    return lax.dot_general(left, right, (dims, ((), ())), preferred_element_type=F32)


def folded(values):
    half = values.shape[1] // 2
    return values[:, :half] + values[:, half:]


def rings(sizes):
    offsets = [(i, j, k) for i in range(sizes[0]) for j in range(sizes[1]) for k in range(sizes[2])]
    offsets = offsets[1:]
    if len(offsets) < 64:
        return offsets, offsets, []
    return (
        offsets,
        [offset for offset in offsets if offset[0] == 0],
        [offset for offset in offsets if offset[1:] == (0, 0)],
    )


def kernel(
    sizes,
    taps_hbm,
    cover_hbm,
    est_hbm,
    obs_hbm,
    out_ref,
    factor_ref,
    taps_ref,
    cover_ref,
    obs,
    ext,
    ext_hi,
    ext_lo,
    pack,
    from_left,
    from_right,
    edge,
    weight,
    scale,
    inverses,
    band,
    twin,
    gath_hi,
    gath_lo,
    scat,
    lined,
    spread,
    total,
    fringe,
    back_pack,
    back_left,
    back_right,
    back_xy,
    stat,
    stat_a,
    stat_b,
    part_a,
    marks,
    fetch_sem,
    hop_sem,
    out_send,
    out_recv,
    back_send,
    back_recv,
    a_send,
    a_recv,
    b_send,
    b_recv,
):
    n_x, n_y, n_z = sizes
    views, rows, cols, lanes = obs.shape
    length = taps_ref.shape[2]
    rad = (length - 1) // 2
    wide_x, wide_y = rows + 2 * rad, cols + 2 * rad
    groups = wide_x // 8
    me_x, me_y, me_z = lax.axis_index("bx"), lax.axis_index("by"), lax.axis_index("bz")

    own_x, own_y = slice(rad, rad + rows), slice(rad, rad + cols)
    own = ext.at[own_x, own_y, :]
    loads = [
        pltpu.make_async_copy(source, target, fetch_sem.at[which])
        for which, (source, target) in enumerate(
            ((est_hbm, own), (cover_hbm, cover_ref), (taps_hbm, taps_ref), (obs_hbm, obs))
        )
    ]
    for load in loads:
        load.start()

    def exists(dx, dy, dz):
        ok = None
        for step, me, count in ((dx, me_x, n_x), (dy, me_y, n_y), (dz, me_z, n_z)):
            if step == 0:
                continue
            inside = (me + step >= 0) & (me + step < count)
            ok = inside if ok is None else ok & inside
        return ok

    def device(dx, dy, dz):
        return {"bx": me_x + dx, "by": me_y + dy, "bz": me_z + dz}

    steps = (-1, 0, 1)
    around = [(dx, dy, dz) for dz in steps for dx in steps for dy in steps if (dx, dy, dz) != (0, 0, 0)]
    ring_all, ring_a, ring_b = rings(sizes)

    def partner(i, j, k):
        return {
            "bx": lax.rem(me_x + i, n_x),
            "by": lax.rem(me_y + j, n_y),
            "bz": lax.rem(me_z + k, n_z),
        }

    for part in ((slice(0, rad), slice(0, wide_y)), (slice(rad + rows, wide_x), slice(0, wide_y))):
        ext[part[0], part[1], :] = jnp.zeros((rad, wide_y, lanes), F32)
    for part in (slice(0, rad), slice(rad + cols, wide_y)):
        ext[own_x, part, :] = jnp.zeros((rows, rad, lanes), F32)
    from_left[...] = jnp.zeros(from_left.shape, F32)
    from_right[...] = jnp.zeros(from_right.shape, F32)
    weight[...] = jnp.zeros(weight.shape, F32)

    barrier = pltpu.get_barrier_semaphore()
    faces = [offset for offset in around if sum(map(abs, offset)) == 1]
    near_by = sum(exists(*offset).astype(jnp.int32) for offset in faces)
    rounds = n_x + n_y + n_z - 3

    def greet(which):
        semaphore = barrier if which == 0 else hop_sem.at[which - 1]
        for offset in faces:

            @pl.when(exists(*offset))
            def _():
                pl.semaphore_signal(semaphore, inc=1, device_id=device(*offset), device_id_type=MESH)

    def meet(which):
        pl.semaphore_wait(barrier if which == 0 else hop_sem.at[which - 1], near_by)
        if which + 1 < rounds:
            greet(which + 1)

    greet(0)

    back_xy[...] = jnp.zeros(back_xy.shape, F32)
    back_left[...] = jnp.zeros(back_left.shape, F32)
    back_right[...] = jnp.zeros(back_right.shape, F32)
    total[...] = jnp.zeros(total.shape, F32)
    fringe[...] = jnp.zeros(fringe.shape, F32)

    loads[1].wait()
    lane = lax.broadcasted_iota(jnp.int32, (1, lanes), 1)
    row = jnp.zeros((1, lanes), F32)
    for v in range(views):
        mine = jnp.full((1, lanes), cover_ref[v], jnp.int32).astype(F32)
        row = jnp.where(lane // (lanes // views) == v, mine, row)
    weight[13] = row
    loads[0].wait()

    lane = lax.broadcasted_iota(jnp.int32, (cols, lanes), 1)
    for g in range(rows // 8):
        merged = jnp.zeros((cols, lanes), F32)
        for i in range(8):
            rolled = pltpu.roll(ext[rad + 8 * g + i, own_y, :], 2 * rad * i + rad, 1)
            merged = jnp.where(lane // (2 * rad) == i, rolled, merged)
        pack[g] = merged

    def cut(step, size, width):
        return pl.ds(0, size) if step == 0 else pl.ds(0 if step < 0 else size - width, width)

    def wide(step, size, width):
        return pl.ds(width, size) if step == 0 else pl.ds(0 if step < 0 else width + size, width)

    pack_rows, pack_rad = rows // 8, rad // 8

    def slot_of(dx, dy, dz):
        return 9 * (dz + 1) + 3 * (dx + 1) + dy + 1

    def out_copies(hops):
        for dx, dy, dz in sorted(around, key=lambda offset: abs(offset[2])):
            if sum(map(abs, (dx, dy, dz))) not in hops:
                continue
            slot = slot_of(dx, dy, dz)
            size, width = (rows, rad) if dz == 0 else (pack_rows, pack_rad)
            source = own if dz == 0 else pack
            target = (from_right, ext, from_left)[dz + 1]
            pairs = (
                (weight.at[13], weight.at[slot_of(-dx, -dy, -dz)]),
                (
                    source.at[cut(dx, size, width), cut(dy, cols, rad), :],
                    target.at[wide(-dx, size, width), wide(-dy, cols, rad), :],
                ),
            )
            copies = [
                pltpu.make_async_remote_copy(
                    src_ref=pair[0],
                    dst_ref=pair[1],
                    send_sem=out_send,
                    recv_sem=out_recv,
                    device_id=device(dx, dy, dz),
                    device_id_type=MESH,
                )
                for which, pair in enumerate(pairs)
            ]
            yield exists(dx, dy, dz), copies

    def back_copies():
        for dx, dy, dz in sorted(around, key=lambda offset: abs(offset[2])):
            size, width = (rows, rad) if dz == 0 else (pack_rows, pack_rad)
            source = total if dz == 0 else back_pack
            target = (back_right, back_xy, back_left)[dz + 1]
            copy = pltpu.make_async_remote_copy(
                src_ref=source.at[wide(dx, size, width), wide(dy, cols, rad), :],
                dst_ref=target.at[wide(-dx, size, width), wide(-dy, cols, rad), :],
                send_sem=back_send,
                recv_sem=back_recv,
                device_id=device(dx, dy, dz),
                device_id_type=MESH,
            )
            yield exists(dx, dy, dz), [copy]

    def start(family):
        for sends, copies in family:

            @pl.when(sends)
            def _():
                for copy in copies:
                    copy.start()

    def drain(semaphore, amount):
        bytes_of = marks.at[pl.ds(0, amount)]
        pltpu.make_async_remote_copy(
            src_ref=bytes_of,
            dst_ref=bytes_of,
            send_sem=semaphore,
            recv_sem=semaphore,
            device_id=partner(*ring_all[0]),
            device_id_type=MESH,
        ).wait_recv()

    def drain_all(semaphore, extra):
        counts_of = [
            (min(count - 1, 2), (me > 0).astype(jnp.int32) + (me < count - 1).astype(jnp.int32))
            for me, count in ((me_x, n_x), (me_y, n_y), (me_z, n_z))
        ]
        for c_x in range(min(1, n_x - 1), counts_of[0][0] + 1):
            for c_y in range(min(1, n_y - 1), counts_of[1][0] + 1):
                for c_z in range(min(1, n_z - 1), counts_of[2][0] + 1):
                    amount = 0
                    for dx, dy, dz in ((i, j, k) for i in (0, 1) for j in (0, 1) for k in (0, 1)):
                        if (dx, dy, dz) == (0, 0, 0):
                            continue
                        size, width = (rows, rad) if dz == 0 else (pack_rows, pack_rad)
                        message = (width if dx else size) * (rad if dy else cols) + extra
                        amount += (c_x if dx else 1) * (c_y if dy else 1) * (c_z if dz else 1) * message

                    @pl.when((counts_of[0][1] == c_x) & (counts_of[1][1] == c_y) & (counts_of[2][1] == c_z))
                    def _():
                        drain(semaphore, amount)

    def build(v, carry):
        def summed(dim):
            values = [taps_ref[dim, v, k] for k in range(length)]
            while len(values) > 1:
                values = [sum(values[i : i + 2]) for i in range(0, len(values), 2)]
            return jnp.full((8, lanes), values[0], F32)

        inverse = 1.0 / (summed(0) * summed(1) * summed(2))

        def chosen(offset, dim):
            result = jnp.zeros(offset.shape, F32)
            for k in range(length):
                result = jnp.where(offset == k, taps_ref[dim, v, k], result)
            return result

        def iota(shape, dim):
            return lax.broadcasted_iota(jnp.int32, shape, dim)

        shape = (lanes, lanes)
        main = chosen(iota(shape, 0) - iota(shape, 1) + rad, 2)
        shape = (2 * rad, lanes)
        row, col = iota(shape, 0), iota(shape, 1)
        edge = chosen(jnp.where(row < rad, row, row + lanes) - col, 2)
        for first, part in ((0, main), (lanes, edge)):
            part = (part.reshape(-1, 8, lanes) * inverse[None]).reshape(part.shape)
            high, low = split(part)
            band[v, first : first + part.shape[0], :] = jnp.concatenate([high, low], axis=1)
            twin[v, first : first + part.shape[0], :] = jnp.concatenate([high, high], axis=1)
        rest = band.shape[1] - lanes - 2 * rad
        band[v, lanes + 2 * rad :, :] = jnp.zeros((rest, 2 * lanes), BF16)
        twin[v, lanes + 2 * rad :, :] = jnp.zeros((rest, 2 * lanes), BF16)
        shape = (8 * cols, 8 * wide_y)
        row, col = iota(shape, 0), iota(shape, 1)
        offset = jnp.where(row // cols == col // wide_y, col % wide_y - row % cols, -1)
        high, low = split(chosen(offset, 1))
        gath_hi[v], gath_lo[v] = high, low
        shape = (8 * wide_y, 8 * cols)
        row, col = iota(shape, 0), iota(shape, 1)
        offset = jnp.where(row // wide_y == col // cols, row % wide_y - col % cols, -1)
        high, low = split(chosen(offset, 1))
        scat[v] = jnp.concatenate([high, low], axis=1)
        return carry

    meet(0)
    start(out_copies((1,)))
    loads[2].wait()
    stops = [min(stop, views) for stop in (0, 2, 4, views)]
    for hop in range(1, 4):
        lax.fori_loop(stops[hop - 1], stops[hop], build, 0)
        if hop < min(3, rounds):
            meet(hop)
        if hop in (1, 2):
            start(out_copies((hop + 1,)))

    loads[3].wait()
    def weight_of(rows_of, v):
        first = v * (lanes // views)
        return jnp.broadcast_to(rows_of[:, first : first + 1], rows_of.shape)

    mine = jnp.broadcast_to(weight[13], (8, lanes))
    count = jnp.zeros((8, lanes), F32)
    seen = jnp.zeros((8, lanes), F32)
    for v in range(views):
        weight_v = weight_of(mine, v)
        count = count + weight_v
        seen = seen + weight_v * jnp.sum(obs[v].reshape(-1, 8, lanes), axis=0)
    count = count[0:1]
    stat[0:1] = jnp.sum(seen, axis=0, keepdims=True) / count

    drain_all(out_recv, 1)
    lane = lax.broadcasted_iota(jnp.int32, (wide_y, lanes), 1)
    high, low = split(ext[...].reshape(wide_x * wide_y, lanes))
    ext_hi[:, :lanes] = high
    ext_lo[:, :lanes] = low
    for g in range(groups):
        merged = jnp.where(lane % (2 * rad) < rad, from_left[g], from_right[g])
        edge[g] = merged
        for i in range(8):
            shift = (lanes - 2 * rad * i) % lanes
            rolled = pltpu.roll(merged, shift, 1) if shift else merged
            high, low = split(rolled)
            first = (8 * g + i) * wide_y
            ext_hi[first : first + wide_y, lanes:] = high
            ext_lo[first : first + wide_y, lanes:] = low

    thin = lax.broadcasted_iota(jnp.int32, (rad, lanes), 1)
    everyone = jnp.concatenate([weight[slot] for slot in range(27)] + [jnp.zeros((5, lanes), F32)], axis=0)
    counts = jnp.zeros(everyone.shape, F32)
    for v in range(views):
        theirs = weight_of(everyone, v)
        counts = counts + theirs

        def spread_of(dx, dy, dz):
            slot = 9 * dz + 3 * dx + dy
            return jnp.broadcast_to(theirs[slot : slot + 1], (rad, lanes))

        for dx in range(3):
            for dy in range(3):
                mid, left, right = (spread_of(dx, dy, dz) for dz in (1, 0, 2))
                side = jnp.where(thin < rad, left, jnp.where(thin < 2 * rad, right, 0.0))
                first, last = ((0, rad), (rad, rad + cols), (rad + cols, wide_y))[dy]
                for at in range(first, last, rad):
                    scale[v, dx, at : at + rad, :lanes] = mid
                    scale[v, dx, at : at + rad, lanes:] = side
    inverses[...] = jnp.where(counts > 0.0, 1.0 / jnp.maximum(counts, 1.0), 0.0)

    def one_view(v, carry):
        size = 8 * wide_y
        high_part = slice(0, lanes)
        for g in range(groups):
            here = slice(g * size, (g + 1) * size)
            blurred = folded(dot(ext_hi[here, :], band[v])) + dot(ext_lo[here, :], band[v, :, high_part])
            high, low = split(blurred)
            line = folded(dot(gath_hi[v], jnp.concatenate([high, low], axis=1))) + dot(gath_lo[v], high)
            lined[8 * g : 8 * g + 8] = line.reshape(8, cols, lanes)
        blur = taps_ref[0, v, 0] * lined[0:rows]
        for k in range(1, length):
            blur = blur + taps_ref[0, v, k] * lined[k : k + rows]
        spread[...] = obs[v] / blur
        for g in range(groups):
            pieces = []
            for e in range(8 * g, 8 * g + 8):
                piece = None
                for a in range(rows):
                    if 0 <= e - a < length:
                        term = taps_ref[0, v, e - a] * spread[a]
                        piece = term if piece is None else piece + term
                pieces.append(piece)
            piece = jnp.concatenate(pieces, axis=0)
            both = jnp.concatenate(split(piece), axis=1)
            piece = folded(dot(scat[v], jnp.concatenate([both, both], axis=0)))
            high, low = split(piece)
            flip = ((1,), (1,))
            piece = dot(jnp.concatenate([high, low], axis=1), twin[v], flip)
            piece = piece + dot(high, band[v, :, lanes:], flip)
            piece = piece.reshape(8, wide_y, 2 * lanes)
            dx = 0 if 8 * g < rad else (1 if 8 * g < rad + rows else 2)
            piece = piece * scale[v, dx][None]
            total[8 * g : 8 * g + 8] += piece[:, :, :lanes]
            fringe[8 * g : 8 * g + 8] += piece[:, :, lanes:]
        return carry

    width_of = 2 if views % 2 == 0 else 1

    def some_views(p, carry):
        for hop in range(3, rounds):

            @pl.when(p == min(hop - 3, views // width_of - 1))
            def _():
                meet(hop)

        for v in range(width_of):
            one_view(width_of * p + v, carry)
        return carry

    lax.fori_loop(0, views // width_of, some_views, 0)

    for g in range(groups):
        merged = fringe[8 * g]
        for i in range(1, 8):
            merged = merged + pltpu.roll(fringe[8 * g + i], 2 * rad * i, 1)
        back_pack[g] = merged
    seen = jnp.zeros((8, lanes), F32)
    for dx in range(3):
        for dy in range(3):
            first_y, last_y = ((0, rad), (rad, rad + cols), (rad + cols, wide_y))[dy]
            first_x, last_x = ((0, rad), (rad, rad + rows), (rad + rows, wide_x))[dx]
            part_y = slice(first_y, last_y)
            part = total[first_x:last_x, part_y, :] * ext[first_x:last_x, part_y, :]
            part = jnp.sum(part.reshape(-1, 8, lanes), axis=0)
            slot = 9 + 3 * dx + dy
            seen = seen + part * inverses[slot : slot + 1, :]
            part_x = slice(first_x // 8, last_x // 8)
            part = back_pack[part_x, part_y, :] * edge[part_x, part_y, :]
            part = jnp.sum(part.reshape(-1, 8, lanes), axis=0)
            left, right = (inverses[at : at + 1, :] for at in (slot - 9, slot + 9))
            seen = seen + part * jnp.where(lane[0:1] % (2 * rad) < rad, left, right)
    stat[1:2] = jnp.sum(seen, axis=0, keepdims=True)

    def sums_a():
        for slot, offset in enumerate(ring_a):
            yield pltpu.make_async_remote_copy(
                src_ref=stat,
                dst_ref=stat_a.at[slot],
                send_sem=a_send,
                recv_sem=a_recv,
                device_id=partner(*offset),
                device_id_type=MESH,
            )

    def sums_b():
        for slot, offset in enumerate(ring_b):
            yield pltpu.make_async_remote_copy(
                src_ref=part_a,
                dst_ref=stat_b.at[slot],
                send_sem=b_send,
                recv_sem=b_recv,
                device_id=partner(*offset),
                device_id_type=MESH,
            )

    for copy in sums_a():
        copy.start()
    start(back_copies())
    drain_all(back_recv, 0)
    near = back_xy[...]

    def fold(values, size, rad, axis):
        low = lax.slice_in_dim(values, 0, rad, axis=axis)
        mid = lax.slice_in_dim(values, rad, rad + size, axis=axis)
        top = lax.slice_in_dim(values, rad + size, 2 * rad + size, axis=axis)
        if size == 2 * rad:
            return mid + jnp.concatenate([low, top], axis=axis)
        gap_shape = list(low.shape)
        gap_shape[axis] = size - rad
        gap = jnp.zeros(gap_shape, F32)
        return mid + jnp.concatenate([low, gap], axis=axis) + jnp.concatenate([gap, top], axis=axis)

    near = fold(fold(near, rows, rad, 0), cols, rad, 1)
    ends = jnp.where((lane % (2 * rad) < rad)[None], back_right[...], back_left[...])
    ends = fold(fold(ends, pack_rows, pack_rad, 0), cols, rad, 1)
    lane = lax.broadcasted_iota(jnp.int32, (cols, lanes), 1)
    outer = (lane < rad) | (lane >= lanes - rad)
    for x in range(rows):
        rolled = pltpu.roll(ends[x // 8], lanes - (2 * rad * (x % 8) + rad), 1)
        summed = total[rad + x, rad : rad + cols, :] + near[x] + jnp.where(outer, rolled, 0.0)
        updated = ext[rad + x, own_y, :] * (summed / count)
        out_ref[x] = updated

    drain(a_recv, 2 * len(ring_a))
    everything = stat[...] + jnp.sum(stat_a[...], axis=0)
    if ring_b:
        part_a[...] = everything
        for copy in sums_b():
            copy.start()
        drain(b_recv, 2 * len(ring_b))
        everything = part_a[...] + jnp.sum(stat_b[...], axis=0)
    wanted = jnp.sum(everything[0:1], axis=1, keepdims=True)
    gotten = jnp.sum(everything[1:2], axis=1, keepdims=True)
    factor = jnp.broadcast_to(wanted, (1, lanes)) / jnp.broadcast_to(gotten, (1, lanes))
    factor_ref[...] = factor

    drain_all(out_send, 1)
    drain_all(back_send, 0)
    drain(a_send, 2 * len(ring_a))
    if ring_b:
        drain(b_send, 2 * len(ring_b))


def on_device(sizes, estimate, observed, coverage, psf_taps):
    rows, cols, lanes = estimate.shape
    views = observed.shape[0]
    rad = (psf_taps.shape[2] - 1) // 2
    wide_x, wide_y = rows + 2 * rad, cols + 2 * rad
    groups = wide_x // 8
    _, ring_a, ring_b = rings(sizes)
    n_a, n_b = len(ring_a), max(1, len(ring_b))

    def vm(*shape, dtype=F32):
        return pltpu.VMEM(shape, dtype)

    def dma(*shape):
        return pltpu.SemaphoreType.DMA(shape)

    def in_hbm(values):
        return pltpu.with_memory_space_constraint(values, pltpu.HBM)

    views_all, dims, length = psf_taps.shape
    scratch = [
        pltpu.SMEM((dims, views_all, length), F32),
        pltpu.SMEM((views,), jnp.int32),
        vm(*observed.shape),
        vm(wide_x, wide_y, lanes),
        vm(wide_x * wide_y, 2 * lanes, dtype=BF16),
        vm(wide_x * wide_y, 2 * lanes, dtype=BF16),
        vm(rows // 8, cols, lanes),
        vm(groups, wide_y, lanes),
        vm(groups, wide_y, lanes),
        vm(groups, wide_y, lanes),
        vm(27, 1, lanes),
        vm(views, 3, wide_y, 2 * lanes),
        vm(32, lanes),
        vm(views, 2 * lanes, 2 * lanes, dtype=BF16),
        vm(views, 2 * lanes, 2 * lanes, dtype=BF16),
        vm(views, 8 * cols, 8 * wide_y, dtype=BF16),
        vm(views, 8 * cols, 8 * wide_y, dtype=BF16),
        vm(views, 8 * wide_y, 16 * cols, dtype=BF16),
        vm(wide_x, cols, lanes),
        vm(rows, cols, lanes),
        vm(wide_x, wide_y, lanes),
        vm(wide_x, wide_y, lanes),
        vm(groups, wide_y, lanes),
        vm(groups, wide_y, lanes),
        vm(groups, wide_y, lanes),
        vm(wide_x, wide_y, lanes),
        vm(2, lanes),
        vm(n_a, 2, lanes),
        vm(n_b, 2, lanes),
        vm(2, lanes),
        vm(5 * rows * cols, 1, lanes),
        dma(4),
        pltpu.SemaphoreType.REGULAR((max(1, sum(sizes) - 4),)),
        *[pltpu.SemaphoreType.DMA] * 8,
    ]
    updated, factor = pl.pallas_call(
        functools.partial(kernel, sizes),
        out_shape=(jax.ShapeDtypeStruct(estimate.shape, F32), jax.ShapeDtypeStruct((1, lanes), F32)),
        in_specs=[
            pl.BlockSpec(memory_space=pl.ANY),
            pl.BlockSpec(memory_space=pl.ANY),
            pl.BlockSpec(memory_space=pl.ANY),
            pl.BlockSpec(memory_space=pl.ANY),
        ],
        out_specs=(pl.BlockSpec(memory_space=pltpu.VMEM), pl.BlockSpec(memory_space=pltpu.VMEM)),
        scratch_shapes=scratch,
        compiler_params=pltpu.CompilerParams(collective_id=0, has_side_effects=True, vmem_limit_bytes=40 * 1024 * 1024),
    )(*map(in_hbm, (jnp.transpose(psf_taps, (1, 0, 2)), coverage.reshape(views), estimate, observed)))
    return updated * factor.reshape(1, 1, lanes)


def solution(mesh):
    sizes = tuple(mesh.shape[axis] for axis in ("bx", "by", "bz"))
    return jax.shard_map(
        functools.partial(on_device, sizes),
        mesh=mesh,
        in_specs=(P("bx", "by", "bz"), P(None, "bx", "by", "bz"), P(None, "bx", "by", "bz"), P()),
        out_specs=P("bx", "by", "bz"),
        check_vma=False,
    )
```

```python
import functools

import jax
import jax.numpy as jnp
from jax import lax
from jax.experimental import pallas as pl
from jax.experimental.pallas import tpu as pltpu
from jax.sharding import PartitionSpec as P

F32 = jnp.float32
BF16 = jnp.bfloat16
MESH = pl.DeviceIdType.MESH


def split(values):
    high = values.astype(BF16)
    low = (values - high.astype(F32)).astype(BF16)
    return high, low


def dot(left, right, dims=((1,), (0,))):
    return lax.dot_general(left, right, (dims, ((), ())), preferred_element_type=F32)


def folded(values):
    half = values.shape[1] // 2
    return values[:, :half] + values[:, half:]


def rings(sizes):
    offsets = [(i, j, k) for i in range(sizes[0]) for j in range(sizes[1]) for k in range(sizes[2])]
    offsets = offsets[1:]
    if len(offsets) < 64:
        return offsets, offsets, []
    return (
        offsets,
        [offset for offset in offsets if offset[0] == 0],
        [offset for offset in offsets if offset[1:] == (0, 0)],
    )


def kernel(
    sizes,
    taps_hbm,
    cover_hbm,
    est_hbm,
    obs_hbm,
    out_ref,
    factor_ref,
    taps_ref,
    cover_ref,
    obs,
    ext,
    wide_a,
    wide_b,
    pack,
    from_left,
    from_right,
    edge,
    weight,
    inverses,
    mask,
    mask_edge,
    ahead_a,
    ahead_b,
    gath,
    scat,
    astern,
    astern_edge,
    taps_x,
    scat_edge,
    blurred,
    lined,
    spread,
    fringe,
    total,
    back_pack,
    back_left,
    back_right,
    back_xy,
    stat,
    stat_a,
    stat_b,
    part_a,
    marks,
    fetch_sem,
    hop_sem,
    out_send,
    out_recv,
    back_send,
    back_recv,
    a_send,
    a_recv,
    b_send,
    b_recv,
):
    n_x, n_y, n_z = sizes
    views, rows, cols, lanes = obs.shape
    length = taps_ref.shape[2]
    rad = (length - 1) // 2
    wide_x, wide_y = rows + 2 * rad, cols + 2 * rad
    groups = wide_x // 8
    me_x, me_y, me_z = lax.axis_index("bx"), lax.axis_index("by"), lax.axis_index("bz")

    own_x, own_y = slice(rad, rad + rows), slice(rad, rad + cols)
    own = ext.at[own_x, own_y, :]
    loads = [
        pltpu.make_async_copy(source, target, fetch_sem.at[which])
        for which, (source, target) in enumerate(
            ((est_hbm, own), (cover_hbm, cover_ref), (taps_hbm, taps_ref), (obs_hbm, obs))
        )
    ]
    for load in loads:
        load.start()

    def exists(dx, dy, dz):
        ok = None
        for step, me, count in ((dx, me_x, n_x), (dy, me_y, n_y), (dz, me_z, n_z)):
            if step == 0:
                continue
            inside = (me + step >= 0) & (me + step < count)
            ok = inside if ok is None else ok & inside
        return ok

    def device(dx, dy, dz):
        return {"bx": me_x + dx, "by": me_y + dy, "bz": me_z + dz}

    steps = (-1, 0, 1)
    around = [(dx, dy, dz) for dz in steps for dx in steps for dy in steps if (dx, dy, dz) != (0, 0, 0)]
    ring_all, ring_a, ring_b = rings(sizes)

    def partner(i, j, k):
        return {
            "bx": lax.rem(me_x + i, n_x),
            "by": lax.rem(me_y + j, n_y),
            "bz": lax.rem(me_z + k, n_z),
        }

    for part in ((slice(0, rad), slice(0, wide_y)), (slice(rad + rows, wide_x), slice(0, wide_y))):
        ext[part[0], part[1], :] = jnp.zeros((rad, wide_y, lanes), F32)
    for part in (slice(0, rad), slice(rad + cols, wide_y)):
        ext[own_x, part, :] = jnp.zeros((rows, rad, lanes), F32)
    from_left[...] = jnp.zeros(from_left.shape, F32)
    from_right[...] = jnp.zeros(from_right.shape, F32)
    weight[...] = jnp.zeros(weight.shape, F32)

    barrier = pltpu.get_barrier_semaphore()
    faces = [offset for offset in around if sum(map(abs, offset)) == 1]
    near_by = sum(exists(*offset).astype(jnp.int32) for offset in faces)
    rounds = n_x + n_y + n_z - 3

    def greet(which):
        semaphore = barrier if which == 0 else hop_sem.at[which - 1]
        for offset in faces:

            @pl.when(exists(*offset))
            def _():
                pl.semaphore_signal(semaphore, inc=1, device_id=device(*offset), device_id_type=MESH)

    def meet(which):
        pl.semaphore_wait(barrier if which == 0 else hop_sem.at[which - 1], near_by)
        if which + 1 < rounds:
            greet(which + 1)

    greet(0)

    back_xy[...] = jnp.zeros(back_xy.shape, F32)
    back_left[...] = jnp.zeros(back_left.shape, F32)
    back_right[...] = jnp.zeros(back_right.shape, F32)
    total[...] = jnp.zeros(total.shape, F32)
    fringe[...] = jnp.zeros(fringe.shape, F32)

    loads[1].wait()
    lane = lax.broadcasted_iota(jnp.int32, (1, lanes), 1)
    row = jnp.zeros((1, lanes), F32)
    for v in range(views):
        mine = jnp.full((1, lanes), cover_ref[v], jnp.int32).astype(F32)
        row = jnp.where(lane // (lanes // views) == v, mine, row)
    weight[13] = row
    loads[0].wait()

    lane = lax.broadcasted_iota(jnp.int32, (cols, lanes), 1)
    for g in range(rows // 8):
        merged = jnp.zeros((cols, lanes), F32)
        for i in range(8):
            rolled = pltpu.roll(ext[rad + 8 * g + i, own_y, :], 2 * rad * i + rad, 1)
            merged = jnp.where(lane // (2 * rad) == i, rolled, merged)
        pack[g] = merged

    def cut(step, size, width):
        return pl.ds(0, size) if step == 0 else pl.ds(0 if step < 0 else size - width, width)

    def wide(step, size, width):
        return pl.ds(width, size) if step == 0 else pl.ds(0 if step < 0 else width + size, width)

    pack_rows, pack_rad = rows // 8, rad // 8

    def slot_of(dx, dy, dz):
        return 9 * (dz + 1) + 3 * (dx + 1) + dy + 1

    def out_copies(hops):
        for dx, dy, dz in sorted(around, key=lambda offset: abs(offset[2])):
            if sum(map(abs, (dx, dy, dz))) not in hops:
                continue
            slot = slot_of(dx, dy, dz)
            size, width = (rows, rad) if dz == 0 else (pack_rows, pack_rad)
            source = own if dz == 0 else pack
            target = (from_right, ext, from_left)[dz + 1]
            pairs = (
                (weight.at[13], weight.at[slot_of(-dx, -dy, -dz)]),
                (
                    source.at[cut(dx, size, width), cut(dy, cols, rad), :],
                    target.at[wide(-dx, size, width), wide(-dy, cols, rad), :],
                ),
            )
            copies = [
                pltpu.make_async_remote_copy(
                    src_ref=pair[0],
                    dst_ref=pair[1],
                    send_sem=out_send,
                    recv_sem=out_recv,
                    device_id=device(dx, dy, dz),
                    device_id_type=MESH,
                )
                for which, pair in enumerate(pairs)
            ]
            yield exists(dx, dy, dz), copies

    def back_copies():
        for dx, dy, dz in sorted(around, key=lambda offset: abs(offset[2])):
            size, width = (rows, rad) if dz == 0 else (pack_rows, pack_rad)
            source = total if dz == 0 else back_pack
            target = (back_right, back_xy, back_left)[dz + 1]
            copy = pltpu.make_async_remote_copy(
                src_ref=source.at[wide(dx, size, width), wide(dy, cols, rad), :],
                dst_ref=target.at[wide(-dx, size, width), wide(-dy, cols, rad), :],
                send_sem=back_send,
                recv_sem=back_recv,
                device_id=device(dx, dy, dz),
                device_id_type=MESH,
            )
            yield exists(dx, dy, dz), [copy]

    def start(family):
        for sends, copies in family:

            @pl.when(sends)
            def _():
                for copy in copies:
                    copy.start()

    def drain(semaphore, amount):
        bytes_of = marks.at[pl.ds(0, amount)]
        pltpu.make_async_remote_copy(
            src_ref=bytes_of,
            dst_ref=bytes_of,
            send_sem=semaphore,
            recv_sem=semaphore,
            device_id=partner(*ring_all[0]),
            device_id_type=MESH,
        ).wait_recv()

    def drain_all(semaphore, extra):
        counts_of = [
            (min(count - 1, 2), (me > 0).astype(jnp.int32) + (me < count - 1).astype(jnp.int32))
            for me, count in ((me_x, n_x), (me_y, n_y), (me_z, n_z))
        ]
        for c_x in range(min(1, n_x - 1), counts_of[0][0] + 1):
            for c_y in range(min(1, n_y - 1), counts_of[1][0] + 1):
                for c_z in range(min(1, n_z - 1), counts_of[2][0] + 1):
                    amount = 0
                    for dx, dy, dz in ((i, j, k) for i in (0, 1) for j in (0, 1) for k in (0, 1)):
                        if (dx, dy, dz) == (0, 0, 0):
                            continue
                        size, width = (rows, rad) if dz == 0 else (pack_rows, pack_rad)
                        message = (width if dx else size) * (rad if dy else cols) + extra
                        amount += (c_x if dx else 1) * (c_y if dy else 1) * (c_z if dz else 1) * message

                    @pl.when((counts_of[0][1] == c_x) & (counts_of[1][1] == c_y) & (counts_of[2][1] == c_z))
                    def _():
                        drain(semaphore, amount)

    def iota(shape, dim):
        return lax.broadcasted_iota(jnp.int32, shape, dim)

    span = 2 * rad
    block = lanes // wide_y

    def stack(*parts):
        return jnp.concatenate(parts, axis=0)

    def beside(*parts):
        return jnp.concatenate(parts, axis=1)

    def build(p, carry):
        for j in range(2):
            v = 2 * p + j

            def summed(dim):
                values = [taps_ref[dim, v, k] for k in range(length)]
                while len(values) > 1:
                    values = [sum(values[i : i + 2]) for i in range(0, len(values), 2)]
                return jnp.full((8, lanes), values[0], F32)

            inverse = 1.0 / (summed(0) * summed(1) * summed(2))

            def chosen(offset, dim):
                result = jnp.zeros(offset.shape, F32)
                for k in range(length):
                    result = jnp.where(offset == k, taps_ref[dim, v, k], result)
                return result

            def scaled(part):
                return (part.reshape(-1, 8, lanes) * inverse[None]).reshape(part.shape)

            here = slice(j * lanes, (j + 1) * lanes)
            square = (lanes, lanes)
            main = scaled(chosen(iota(square, 0) - iota(square, 1) + rad, 2))
            row, col = iota((span, lanes), 0), iota((span, lanes), 1)
            edges = scaled(chosen(jnp.where(row < rad, row, row + lanes) - col, 2))
            high, low = split(main)
            ahead_a[p, :, here] = stack(high, high)
            ahead_b[p, :lanes, here] = low
            high, low = split(edges)
            ahead_b[p, lanes:, here] = stack(high, high, low, jnp.zeros((lanes - 3 * span, lanes), BF16))
            high, low = split(main.T)
            astern[v] = stack(beside(high, low), beside(high, jnp.zeros(square, BF16)))
            turned = jnp.where(iota(square, 1) // span == v, stack(*[edges] * views).T, 0.0)
            high, low = split(turned)
            astern_edge[v] = stack(beside(high, low), beside(high, jnp.zeros(square, BF16)))
            shape = (block * cols, lanes)
            row, col = iota(shape, 0), iota(shape, 1)
            offset = jnp.where(row // cols == col // wide_y, col % wide_y - row % cols, -1)
            blur_y = chosen(offset, 1)
            high, low = split(blur_y)
            gath[v] = stack(beside(high, high), beside(low, jnp.zeros(shape, BF16)))
            turned = blur_y.T
            high = turned.astype(BF16).astype(F32)
            low = turned - high
            scat[v] = beside(high, high, low).astype(BF16)
        return carry

    def lines_of(dim):
        lane = iota((1, lanes), 1)
        lines = []
        for k in range(length):
            line = jnp.zeros((1, lanes), F32)
            for v in range(views):
                line = jnp.where(lane // span == v, taps_ref[dim, v, k], line)
            lines.append(line)
        return lines

    meet(0)
    start(out_copies((1,)))
    loads[2].wait()
    stops = [min(stop, views // 2) for stop in (0, 1, 2, views // 2)]
    for hop in range(1, 4):
        lax.fori_loop(stops[hop - 1], stops[hop], build, 0)
        if hop < min(3, rounds):
            meet(hop)
        if hop in (1, 2):
            start(out_copies((hop + 1,)))

    for k, line in enumerate(lines_of(0)):
        taps_x[k : k + 1] = line
    shape = (wide_y, lanes)
    offset = iota(shape, 0) - iota(shape, 1) % cols
    base = jnp.zeros(shape, F32)
    for k, line in enumerate(lines_of(1)):
        base = jnp.where(offset == k, line, base)
    high = base.astype(BF16).astype(F32)
    scat_edge[...] = beside(high, high, base - high)

    loads[3].wait()
    def weight_of(rows_of, v):
        first = v * (lanes // views)
        return jnp.broadcast_to(rows_of[:, first : first + 1], rows_of.shape)

    mine = jnp.broadcast_to(weight[13], (8, lanes))
    count = jnp.zeros((8, lanes), F32)
    seen = jnp.zeros((8, lanes), F32)
    for v in range(views):
        weight_v = weight_of(mine, v)
        count = count + weight_v
        seen = seen + weight_v * jnp.sum(obs[v].reshape(-1, 8, lanes), axis=0)
    count = count[0:1]
    stat[0:1] = jnp.sum(seen, axis=0, keepdims=True) / count

    drain_all(out_recv, 1)
    high, low = split(ext[...].reshape(wide_x * wide_y, lanes))
    wide_a[:, :lanes] = high
    wide_a[:, lanes:] = low
    wide_b[:, :lanes] = high
    lane = iota((wide_y, lanes), 1)
    for g in range(groups):
        merged = jnp.where(lane % span < rad, from_left[g], from_right[g])
        edge[g] = merged
        high = merged.astype(BF16).astype(F32)
        low = merged - high
        count_of = lanes // span
        highs = [pltpu.roll(high, span * i, 1) if i else high for i in range(count_of)]
        lows = [pltpu.roll(low, span * i, 1) if i else low for i in range(count_of)]
        for i in range(8):
            third = jnp.where(lane < 2 * span, lows[(1 - i) % count_of], highs[(2 - i) % count_of])
            terms = jnp.where(lane < span, highs[-i % count_of], third)
            first = (8 * g + i) * wide_y
            wide_b[first : first + wide_y, lanes:] = terms.astype(BF16)

    everyone = stack(*[weight[slot] for slot in range(27)], jnp.zeros((5, lanes), F32))
    counts = jnp.zeros(everyone.shape, F32)

    def along_y(rows_of, first):
        bands = [(rad, 0), (cols, 1), (rad, 2)]
        return stack(*[jnp.broadcast_to(rows_of[first + dy : first + dy + 1], (size, lanes)) for size, dy in bands])

    for v in range(views):
        theirs = weight_of(everyone, v)
        counts = counts + theirs
        for dx in range(3):
            mask[v, dx] = along_y(theirs, 9 + 3 * dx).astype(BF16)
    for dx in range(3):
        for side in range(2):
            part = along_y(everyone, 18 * side + 3 * dx)
            terms = scat_edge[...] * beside(part, part, part)
            mask_edge[dx, side * wide_y : (side + 1) * wide_y] = terms.astype(BF16)
    inverses[...] = jnp.where(counts > 0.0, 1.0 / jnp.maximum(counts, 1.0), 0.0)

    def side_of(g):
        return 0 if 8 * g < rad else (1 if 8 * g < rad + rows else 2)

    def spread_x(source, tap):
        pieces = []
        for e in range(wide_x):
            piece = None
            for a in range(rows):
                if 0 <= e - a < length:
                    term = tap(e - a) * source[a]
                    piece = term if piece is None else piece + term
            pieces.append(piece)
        return pieces

    def pairs_of(part, half):
        return beside(part[:half], part[half:])

    def two_views(p):
        blurred[...] = dot(wide_a[...], ahead_a[p]) + dot(wide_b[...], ahead_b[p])
        size = 8 * wide_y
        scattered = []
        for j in range(2):
            v = 2 * p + j
            for g in range(groups):
                high, low = split(blurred[g * size : (g + 1) * size, j * lanes : (j + 1) * lanes])
                line = dot(gath[v], stack(pairs_of(high, size // 2), pairs_of(low, size // 2)))
                half = block * cols
                line = line[:half] + line[half:]
                for which in range(2):
                    first = 8 * g + which * block
                    lined[j, first : first + block] = line[:, which * lanes : (which + 1) * lanes].reshape(block, cols, lanes)
            blur = taps_ref[0, v, 0] * lined[j, 0:rows]
            for k in range(1, length):
                blur = blur + taps_ref[0, v, k] * lined[j, k : k + rows]
            ratio = (obs[v] / blur).reshape(rows * cols, lanes)
            ratio = beside(*split(ratio))
            back = folded(dot(ratio, astern[v]))
            fringe[...] += dot(ratio, astern_edge[v])
            spread[j] = back.reshape(rows, cols, lanes)
            pieces = spread_x(spread.at[j], lambda k: taps_ref[0, v, k])
            sent = []
            for g in range(groups):
                high, low = split(stack(*pieces[8 * g : 8 * g + 8]))
                high, low = (pairs_of(part, block * cols) for part in (high, low))
                sent.append(stack(high, low, high))
            scattered.append(sent)
        for g in range(groups):
            dx = side_of(g)
            reach = None
            for j in range(2):
                v = 2 * p + j
                here = stack(*[mask[v, dx]] * block)
                here = scat[v] * beside(here, here)[:, : scat.shape[2]]
                part = dot(here, scattered[j][g])
                reach = part if reach is None else reach + part
            for which in range(2):
                first = 8 * g + which * block
                part = reach[:, which * lanes : (which + 1) * lanes]
                total[first : first + block] += part.reshape(block, wide_y, lanes)

    def some_views(p, carry):
        for hop in range(3, rounds):

            @pl.when(p == min(hop - 3, views // 2 - 1))
            def _():
                meet(hop)

        two_views(p)
        return carry

    lax.fori_loop(0, views // 2, some_views, 0)

    spread[0] = folded(fringe[...]).reshape(rows, cols, lanes)
    pieces = spread_x(spread.at[0], lambda k: taps_x[k : k + 1])
    lane = iota((cols, lanes), 1)
    for g in range(groups):
        turned = pieces[8 * g : 8 * g + 8]
        step = views // 2
        while step:
            low_half = (lane // span) // step % 2 == 0
            for i in range(views):
                if i // step % 2 == 0:
                    one, two = turned[i], turned[i + step]
                    turned[i] = jnp.where(low_half, one, pltpu.roll(two, step * span, 1))
                    turned[i + step] = jnp.where(low_half, pltpu.roll(one, lanes - step * span, 1), two)
            step //= 2
        high, low = split(stack(*turned))
        sides = dot(mask_edge[side_of(g)], stack(high, low, high))
        back_pack[g] = jnp.where(iota((wide_y, lanes), 1) % span < rad, sides[:wide_y], sides[wide_y:])
    lane = iota((wide_y, lanes), 1)
    seen = jnp.zeros((8, lanes), F32)
    for dx in range(3):
        for dy in range(3):
            first_y, last_y = ((0, rad), (rad, rad + cols), (rad + cols, wide_y))[dy]
            first_x, last_x = ((0, rad), (rad, rad + rows), (rad + rows, wide_x))[dx]
            part_y = slice(first_y, last_y)
            part = total[first_x:last_x, part_y, :] * ext[first_x:last_x, part_y, :]
            part = jnp.sum(part.reshape(-1, 8, lanes), axis=0)
            slot = 9 + 3 * dx + dy
            seen = seen + part * inverses[slot : slot + 1, :]
            part_x = slice(first_x // 8, last_x // 8)
            part = back_pack[part_x, part_y, :] * edge[part_x, part_y, :]
            part = jnp.sum(part.reshape(-1, 8, lanes), axis=0)
            left, right = (inverses[at : at + 1, :] for at in (slot - 9, slot + 9))
            seen = seen + part * jnp.where(lane[0:1] % (2 * rad) < rad, left, right)
    stat[1:2] = jnp.sum(seen, axis=0, keepdims=True)

    def sums_a():
        for slot, offset in enumerate(ring_a):
            yield pltpu.make_async_remote_copy(
                src_ref=stat,
                dst_ref=stat_a.at[slot],
                send_sem=a_send,
                recv_sem=a_recv,
                device_id=partner(*offset),
                device_id_type=MESH,
            )

    def sums_b():
        for slot, offset in enumerate(ring_b):
            yield pltpu.make_async_remote_copy(
                src_ref=part_a,
                dst_ref=stat_b.at[slot],
                send_sem=b_send,
                recv_sem=b_recv,
                device_id=partner(*offset),
                device_id_type=MESH,
            )

    for copy in sums_a():
        copy.start()
    start(back_copies())
    drain_all(back_recv, 0)
    near = back_xy[...]

    def fold(values, size, rad, axis):
        low = lax.slice_in_dim(values, 0, rad, axis=axis)
        mid = lax.slice_in_dim(values, rad, rad + size, axis=axis)
        top = lax.slice_in_dim(values, rad + size, 2 * rad + size, axis=axis)
        if size == 2 * rad:
            return mid + jnp.concatenate([low, top], axis=axis)
        gap_shape = list(low.shape)
        gap_shape[axis] = size - rad
        gap = jnp.zeros(gap_shape, F32)
        return mid + jnp.concatenate([low, gap], axis=axis) + jnp.concatenate([gap, top], axis=axis)

    near = fold(fold(near, rows, rad, 0), cols, rad, 1)
    ends = jnp.where((lane % (2 * rad) < rad)[None], back_right[...], back_left[...])
    ends = fold(fold(ends, pack_rows, pack_rad, 0), cols, rad, 1)
    lane = lax.broadcasted_iota(jnp.int32, (cols, lanes), 1)
    outer = (lane < rad) | (lane >= lanes - rad)
    for x in range(rows):
        rolled = pltpu.roll(ends[x // 8], lanes - (2 * rad * (x % 8) + rad), 1)
        summed = total[rad + x, rad : rad + cols, :] + near[x] + jnp.where(outer, rolled, 0.0)
        updated = ext[rad + x, own_y, :] * (summed / count)
        out_ref[x] = updated

    drain(a_recv, 2 * len(ring_a))
    everything = stat[...] + jnp.sum(stat_a[...], axis=0)
    if ring_b:
        part_a[...] = everything
        for copy in sums_b():
            copy.start()
        drain(b_recv, 2 * len(ring_b))
        everything = part_a[...] + jnp.sum(stat_b[...], axis=0)
    wanted = jnp.sum(everything[0:1], axis=1, keepdims=True)
    gotten = jnp.sum(everything[1:2], axis=1, keepdims=True)
    factor = jnp.broadcast_to(wanted, (1, lanes)) / jnp.broadcast_to(gotten, (1, lanes))
    factor_ref[...] = factor

    drain_all(out_send, 1)
    drain_all(back_send, 0)
    drain(a_send, 2 * len(ring_a))
    if ring_b:
        drain(b_send, 2 * len(ring_b))


def on_device(sizes, estimate, observed, coverage, psf_taps):
    rows, cols, lanes = estimate.shape
    views = observed.shape[0]
    rad = (psf_taps.shape[2] - 1) // 2
    wide_x, wide_y = rows + 2 * rad, cols + 2 * rad
    groups, block = wide_x // 8, lanes // wide_y
    _, ring_a, ring_b = rings(sizes)
    n_a, n_b = len(ring_a), max(1, len(ring_b))

    def vm(*shape, dtype=F32):
        return pltpu.VMEM(shape, dtype)

    def dma(*shape):
        return pltpu.SemaphoreType.DMA(shape)

    def in_hbm(values):
        return pltpu.with_memory_space_constraint(values, pltpu.HBM)

    views_all, dims, length = psf_taps.shape
    scratch = [
        pltpu.SMEM((dims, views_all, length), F32),
        pltpu.SMEM((views,), jnp.int32),
        vm(*observed.shape),
        vm(wide_x, wide_y, lanes),
        vm(wide_x * wide_y, 2 * lanes, dtype=BF16),
        vm(wide_x * wide_y, 2 * lanes, dtype=BF16),
        vm(rows // 8, cols, lanes),
        vm(groups, wide_y, lanes),
        vm(groups, wide_y, lanes),
        vm(groups, wide_y, lanes),
        vm(27, 1, lanes),
        vm(32, lanes),
        vm(views, 3, wide_y, lanes, dtype=BF16),
        vm(3, 2 * wide_y, 3 * lanes, dtype=BF16),
        vm(views // 2, 2 * lanes, 2 * lanes, dtype=BF16),
        vm(views // 2, 2 * lanes, 2 * lanes, dtype=BF16),
        vm(views, 2 * block * cols, 2 * lanes, dtype=BF16),
        vm(views, lanes, 3 * block * cols, dtype=BF16),
        vm(views, 2 * lanes, 2 * lanes, dtype=BF16),
        vm(views, 2 * lanes, 2 * lanes, dtype=BF16),
        vm(24, lanes),
        vm(wide_y, 3 * lanes),
        vm(wide_x * wide_y, 2 * lanes),
        vm(2, wide_x, cols, lanes),
        vm(2, rows, cols, lanes),
        vm(rows * cols, 2 * lanes),
        vm(wide_x, wide_y, lanes),
        vm(groups, wide_y, lanes),
        vm(groups, wide_y, lanes),
        vm(groups, wide_y, lanes),
        vm(wide_x, wide_y, lanes),
        vm(2, lanes),
        vm(n_a, 2, lanes),
        vm(n_b, 2, lanes),
        vm(2, lanes),
        vm(5 * rows * cols, 1, lanes),
        dma(4),
        pltpu.SemaphoreType.REGULAR((max(1, sum(sizes) - 4),)),
        *[pltpu.SemaphoreType.DMA] * 8,
    ]
    updated, factor = pl.pallas_call(
        functools.partial(kernel, sizes),
        out_shape=(jax.ShapeDtypeStruct(estimate.shape, F32), jax.ShapeDtypeStruct((1, lanes), F32)),
        in_specs=[
            pl.BlockSpec(memory_space=pl.ANY),
            pl.BlockSpec(memory_space=pl.ANY),
            pl.BlockSpec(memory_space=pl.ANY),
            pl.BlockSpec(memory_space=pl.ANY),
        ],
        out_specs=(pl.BlockSpec(memory_space=pltpu.VMEM), pl.BlockSpec(memory_space=pltpu.VMEM)),
        scratch_shapes=scratch,
        compiler_params=pltpu.CompilerParams(collective_id=0, has_side_effects=True, vmem_limit_bytes=40 * 1024 * 1024),
    )(*map(in_hbm, (jnp.transpose(psf_taps, (1, 0, 2)), coverage.reshape(views), estimate, observed)))
    return updated * factor.reshape(1, 1, lanes)


def solution(mesh):
    sizes = tuple(mesh.shape[axis] for axis in ("bx", "by", "bz"))
    return jax.shard_map(
        functools.partial(on_device, sizes),
        mesh=mesh,
        in_specs=(P("bx", "by", "bz"), P(None, "bx", "by", "bz"), P(None, "bx", "by", "bz"), P()),
        out_specs=P("bx", "by", "bz"),
        check_vma=False,
    )
```

```python
import functools

import jax
import jax.numpy as jnp
from jax import lax
from jax.experimental import pallas as pl
from jax.experimental.pallas import tpu as pltpu
from jax.sharding import PartitionSpec as P

F32 = jnp.float32
BF16 = jnp.bfloat16
MESH = pl.DeviceIdType.MESH


def split(values):
    high = values.astype(BF16)
    low = (values - high.astype(F32)).astype(BF16)
    return high, low


def dot(left, right, dims=((1,), (0,))):
    return lax.dot_general(left, right, (dims, ((), ())), preferred_element_type=F32)


def folded(values):
    half = values.shape[1] // 2
    return values[:, :half] + values[:, half:]


def rings(sizes):
    offsets = [(i, j, k) for i in range(sizes[0]) for j in range(sizes[1]) for k in range(sizes[2])]
    offsets = offsets[1:]
    if len(offsets) < 64:
        return offsets, offsets, []
    return (
        offsets,
        [offset for offset in offsets if offset[0] == 0],
        [offset for offset in offsets if offset[1:] == (0, 0)],
    )


def stage_of(dx, dy, dz):
    return 3 if dx and dy else abs(dx) + abs(dy) + abs(dz)


def late_rounds(sizes):
    steps = (-1, 0, 1)
    near = [(i, j, k) for i in steps for j in steps for k in steps if (i, j, k) != (0, 0, 0)]
    everyone = [(i, j, k) for i in range(sizes[0]) for j in range(sizes[1]) for k in range(sizes[2])]
    known = {at: {at} for at in everyone}

    def beyond(at, offset):
        return tuple(a + b for a, b in zip(at, offset))

    def heard(sets, stages):
        return {
            at: set().union(
                sets[-1][at],
                *[
                    sets[min(stage_of(*offset), len(sets) - 1)].get(beyond(at, offset), set())
                    for offset in near
                    if stage_of(*offset) in stages
                ],
            )
            for at in everyone
        }

    history = [known]
    for _ in range(min(3, sum(sizes) - 3)):
        history.append(heard([history[-1]] * 4, (1,)))
    now, rounds = heard(history, (1, 2, 3)), 0
    while any(len(now[at]) < len(everyone) for at in everyone):
        now, rounds = heard([now] * 4, (1,)), rounds + 1
    return rounds


def kernel(
    sizes,
    taps_hbm,
    cover_hbm,
    est_hbm,
    obs_hbm,
    out_ref,
    factor_ref,
    taps_ref,
    cover_ref,
    obs,
    ext,
    wide_a,
    wide_b,
    pack,
    from_left,
    from_right,
    edge,
    weight,
    inverses,
    mask,
    mask_edge,
    ahead_a,
    ahead_b,
    gath,
    scat,
    astern,
    astern_edge,
    taps_x,
    scat_edge,
    blurred,
    lined,
    spread,
    fringe,
    total,
    back_pack,
    back_left,
    back_right,
    back_xy,
    stat,
    stat_a,
    stat_b,
    part_a,
    marks,
    fetch_sem,
    hop_sem,
    out_send,
    out_recv,
    far_recv,
    weight_send,
    weight_recv,
    back_send,
    back_recv,
    a_send,
    a_recv,
    b_send,
    b_recv,
):
    n_x, n_y, n_z = sizes
    views, rows, cols, lanes = obs.shape
    length = taps_ref.shape[2]
    rad = (length - 1) // 2
    wide_x, wide_y = rows + 2 * rad, cols + 2 * rad
    groups = wide_x // 8
    me_x, me_y, me_z = lax.axis_index("bx"), lax.axis_index("by"), lax.axis_index("bz")

    own_x, own_y = slice(rad, rad + rows), slice(rad, rad + cols)
    own = ext.at[own_x, own_y, :]
    loads = [
        pltpu.make_async_copy(source, target, fetch_sem.at[which])
        for which, (source, target) in enumerate(
            ((est_hbm, own), (cover_hbm, cover_ref), (taps_hbm, taps_ref), (obs_hbm, obs))
        )
    ]
    for load in loads:
        load.start()

    def exists(dx, dy, dz):
        ok = None
        for step, me, count in ((dx, me_x, n_x), (dy, me_y, n_y), (dz, me_z, n_z)):
            if step == 0:
                continue
            inside = (me + step >= 0) & (me + step < count)
            ok = inside if ok is None else ok & inside
        return ok

    def device(dx, dy, dz):
        return {"bx": me_x + dx, "by": me_y + dy, "bz": me_z + dz}

    steps = (-1, 0, 1)
    around = [(dx, dy, dz) for dz in steps for dx in steps for dy in steps if (dx, dy, dz) != (0, 0, 0)]
    ring_all, ring_a, ring_b = rings(sizes)

    def partner(i, j, k):
        return {
            "bx": lax.rem(me_x + i, n_x),
            "by": lax.rem(me_y + j, n_y),
            "bz": lax.rem(me_z + k, n_z),
        }

    for part in ((slice(0, rad), slice(0, wide_y)), (slice(rad + rows, wide_x), slice(0, wide_y))):
        ext[part[0], part[1], :] = jnp.zeros((rad, wide_y, lanes), F32)
    for part in (slice(0, rad), slice(rad + cols, wide_y)):
        ext[own_x, part, :] = jnp.zeros((rows, rad, lanes), F32)
    from_left[...] = jnp.zeros(from_left.shape, F32)
    from_right[...] = jnp.zeros(from_right.shape, F32)
    weight[...] = jnp.zeros(weight.shape, F32)

    barrier = pltpu.get_barrier_semaphore()
    faces = [offset for offset in around if sum(map(abs, offset)) == 1]
    near_by = sum(exists(*offset).astype(jnp.int32) for offset in faces)
    early_rounds = min(3, n_x + n_y + n_z - 3)
    rounds = early_rounds + late_rounds(sizes)

    def greet(which):
        semaphore = barrier if which == 0 else hop_sem.at[which - 1]
        for offset in faces:

            @pl.when(exists(*offset))
            def _():
                pl.semaphore_signal(semaphore, inc=1, device_id=device(*offset), device_id_type=MESH)

    def meet(which):
        pl.semaphore_wait(barrier if which == 0 else hop_sem.at[which - 1], near_by)
        if which + 1 < rounds and which + 1 != early_rounds:
            greet(which + 1)

    greet(0)

    back_xy[...] = jnp.zeros(back_xy.shape, F32)
    back_left[...] = jnp.zeros(back_left.shape, F32)
    back_right[...] = jnp.zeros(back_right.shape, F32)
    total[...] = jnp.zeros(total.shape, F32)
    fringe[...] = jnp.zeros(fringe.shape, F32)

    loads[1].wait()
    lane = lax.broadcasted_iota(jnp.int32, (1, lanes), 1)
    row = jnp.zeros((1, lanes), F32)
    for v in range(views):
        mine = jnp.full((1, lanes), cover_ref[v], jnp.int32).astype(F32)
        row = jnp.where(lane // (lanes // views) == v, mine, row)
    weight[13] = row
    loads[0].wait()

    lane = lax.broadcasted_iota(jnp.int32, (cols, lanes), 1)
    for g in range(rows // 8):
        merged = jnp.zeros((cols, lanes), F32)
        for i in range(8):
            rolled = pltpu.roll(ext[rad + 8 * g + i, own_y, :], 2 * rad * i + rad, 1)
            merged = jnp.where(lane // (2 * rad) == i, rolled, merged)
        pack[g] = merged

    def cut(step, size, width):
        return pl.ds(0, size) if step == 0 else pl.ds(0 if step < 0 else size - width, width)

    def wide(step, size, width):
        return pl.ds(width, size) if step == 0 else pl.ds(0 if step < 0 else width + size, width)

    pack_rows, pack_rad = rows // 8, rad // 8

    def slot_of(dx, dy, dz):
        return 9 * (dz + 1) + 3 * (dx + 1) + dy + 1

    def out_copies(hops):
        for dx, dy, dz in sorted(around, key=lambda offset: (abs(offset[0]), abs(offset[2]))):
            if stage_of(dx, dy, dz) not in hops:
                continue
            slot = slot_of(dx, dy, dz)
            size, width = (rows, rad) if dz == 0 else (pack_rows, pack_rad)
            source = own if dz == 0 else pack
            target = (from_right, ext, from_left)[dz + 1]
            pairs = (
                (weight.at[13], weight.at[slot_of(-dx, -dy, -dz)]),
                (
                    source.at[cut(dx, size, width), cut(dy, cols, rad), :],
                    target.at[wide(-dx, size, width), wide(-dy, cols, rad), :],
                ),
            )
            sems = ((weight_send, weight_recv), (out_send, far_recv if dx else out_recv))
            copies = [
                pltpu.make_async_remote_copy(
                    src_ref=pair[0],
                    dst_ref=pair[1],
                    send_sem=send_sem,
                    recv_sem=recv_sem,
                    device_id=device(dx, dy, dz),
                    device_id_type=MESH,
                )
                for pair, (send_sem, recv_sem) in zip(pairs, sems)
            ]
            yield exists(dx, dy, dz), copies

    def back_copies(flat):
        for dx, dy, dz in around:
            if (dz == 0) != flat:
                continue
            size, width = (rows, rad) if dz == 0 else (pack_rows, pack_rad)
            source = total if dz == 0 else back_pack
            target = (back_right, back_xy, back_left)[dz + 1]
            copy = pltpu.make_async_remote_copy(
                src_ref=source.at[wide(dx, size, width), wide(dy, cols, rad), :],
                dst_ref=target.at[wide(-dx, size, width), wide(-dy, cols, rad), :],
                send_sem=back_send,
                recv_sem=back_recv,
                device_id=device(dx, dy, dz),
                device_id_type=MESH,
            )
            yield exists(dx, dy, dz), [copy]

    def start(family):
        for sends, copies in family:

            @pl.when(sends)
            def _():
                for copy in copies:
                    copy.start()

    def drain(semaphore, amount):
        bytes_of = marks.at[pl.ds(0, amount)]
        pltpu.make_async_remote_copy(
            src_ref=bytes_of,
            dst_ref=bytes_of,
            send_sem=semaphore,
            recv_sem=semaphore,
            device_id=partner(*ring_all[0]),
            device_id_type=MESH,
        ).wait_recv()

    def drain_all(semaphore, sides=(0, 1), rows_only=False):
        counts_of = [
            (min(count - 1, 2), (me > 0).astype(jnp.int32) + (me < count - 1).astype(jnp.int32))
            for me, count in ((me_x, n_x), (me_y, n_y), (me_z, n_z))
        ]
        for c_x in range(min(1, n_x - 1), counts_of[0][0] + 1):
            for c_y in range(min(1, n_y - 1), counts_of[1][0] + 1):
                for c_z in range(min(1, n_z - 1), counts_of[2][0] + 1):
                    amount = 0
                    for dx, dy, dz in ((i, j, k) for i in (0, 1) for j in (0, 1) for k in (0, 1)):
                        if (dx, dy, dz) == (0, 0, 0) or dx not in sides:
                            continue
                        size, width = (rows, rad) if dz == 0 else (pack_rows, pack_rad)
                        message = 1 if rows_only else (width if dx else size) * (rad if dy else cols)
                        amount += (c_x if dx else 1) * (c_y if dy else 1) * (c_z if dz else 1) * message

                    if not amount:
                        continue

                    @pl.when((counts_of[0][1] == c_x) & (counts_of[1][1] == c_y) & (counts_of[2][1] == c_z))
                    def _():
                        drain(semaphore, amount)

    def iota(shape, dim):
        return lax.broadcasted_iota(jnp.int32, shape, dim)

    span = 2 * rad
    block = lanes // wide_y

    def stack(*parts):
        return jnp.concatenate(parts, axis=0)

    def beside(*parts):
        return jnp.concatenate(parts, axis=1)

    def build(p, carry):
        for j in range(2):
            v = 2 * p + j

            def summed(dim):
                values = [taps_ref[dim, v, k] for k in range(length)]
                while len(values) > 1:
                    values = [sum(values[i : i + 2]) for i in range(0, len(values), 2)]
                return jnp.full((8, lanes), values[0], F32)

            inverse = 1.0 / (summed(0) * summed(1) * summed(2))

            def chosen(offset, dim):
                result = jnp.zeros(offset.shape, F32)
                for k in range(length):
                    result = jnp.where(offset == k, taps_ref[dim, v, k], result)
                return result

            def scaled(part):
                return (part.reshape(-1, 8, lanes) * inverse[None]).reshape(part.shape)

            here = slice(j * lanes, (j + 1) * lanes)
            square = (lanes, lanes)
            main = scaled(chosen(iota(square, 0) - iota(square, 1) + rad, 2))
            row, col = iota((span, lanes), 0), iota((span, lanes), 1)
            edges = scaled(chosen(jnp.where(row < rad, row, row + lanes) - col, 2))
            high, low = split(main)
            ahead_a[p, :, here] = stack(high, high)
            ahead_b[p, :lanes, here] = low
            high, low = split(edges)
            ahead_b[p, lanes:, here] = stack(high, high, low, jnp.zeros((lanes - 3 * span, lanes), BF16))
            high, low = split(main.T)
            astern[v] = stack(beside(high, low), beside(high, jnp.zeros(square, BF16)))
            turned = jnp.where(iota(square, 1) // span == v, stack(*[edges] * views).T, 0.0)
            high, low = split(turned)
            astern_edge[v] = stack(beside(high, low), beside(high, jnp.zeros(square, BF16)))
            shape = (block * cols, lanes)
            row, col = iota(shape, 0), iota(shape, 1)
            offset = jnp.where(row // cols == col // wide_y, col % wide_y - row % cols, -1)
            blur_y = chosen(offset, 1)
            high, low = split(blur_y)
            gath[v] = stack(beside(high, high), beside(low, jnp.zeros(shape, BF16)))
            turned = blur_y.T
            high = turned.astype(BF16).astype(F32)
            low = turned - high
            scat[v] = beside(high, high, low).astype(BF16)
        return carry

    def lines_of(dim):
        lane = iota((1, lanes), 1)
        lines = []
        for k in range(length):
            line = jnp.zeros((1, lanes), F32)
            for v in range(views):
                line = jnp.where(lane // span == v, taps_ref[dim, v, k], line)
            lines.append(line)
        return lines

    meet(0)
    start(out_copies((1,)))
    loads[2].wait()
    stops = [min(stop, views // 2) for stop in (0, 1, 2, views // 2)]
    for hop in range(1, 4):
        lax.fori_loop(stops[hop - 1], stops[hop], build, 0)
        if hop < early_rounds:
            meet(hop)
        if hop in (1, 2):
            start(out_copies((hop + 1,)))

    for k, line in enumerate(lines_of(0)):
        taps_x[k : k + 1] = line
    shape = (wide_y, lanes)
    offset = iota(shape, 0) - iota(shape, 1) % cols
    base = jnp.zeros(shape, F32)
    for k, line in enumerate(lines_of(1)):
        base = jnp.where(offset == k, line, base)
    high = base.astype(BF16).astype(F32)
    scat_edge[...] = beside(high, high, base - high)

    loads[3].wait()
    def weight_of(rows_of, v):
        first = v * (lanes // views)
        return jnp.broadcast_to(rows_of[:, first : first + 1], rows_of.shape)

    mine = jnp.broadcast_to(weight[13], (8, lanes))
    count = jnp.zeros((8, lanes), F32)
    seen = jnp.zeros((8, lanes), F32)
    for v in range(views):
        weight_v = weight_of(mine, v)
        count = count + weight_v
        seen = seen + weight_v * jnp.sum(obs[v].reshape(-1, 8, lanes), axis=0)
    count = count[0:1]
    wanted = jnp.sum(seen, axis=0, keepdims=True) / count

    def side_of(g):
        return 0 if 8 * g < rad else (1 if 8 * g < rad + rows else 2)

    inner = [g for g in range(groups) if side_of(g) == 1]
    outer = [g for g in range(groups) if side_of(g) != 1]
    place = {g: which for which, g in enumerate(inner + outer)}
    size = 8 * wide_y
    inner_rows, outer_rows = slice(0, size * len(inner)), slice(size * len(inner), size * groups)

    def prepare(chosen_groups):
        lane = iota((wide_y, lanes), 1)
        for g in chosen_groups:
            here = slice(size * place[g], size * (place[g] + 1))
            high, low = split(ext[8 * g : 8 * g + 8].reshape(size, lanes))
            wide_a[here, :lanes] = high
            wide_a[here, lanes:] = low
            wide_b[here, :lanes] = high
            merged = jnp.where(lane % span < rad, from_left[g], from_right[g])
            edge[g] = merged
            high = merged.astype(BF16).astype(F32)
            low = merged - high
            count_of = lanes // span
            highs = [pltpu.roll(high, span * i, 1) if i else high for i in range(count_of)]
            lows = [pltpu.roll(low, span * i, 1) if i else low for i in range(count_of)]
            for i in range(8):
                third = jnp.where(lane < 2 * span, lows[(1 - i) % count_of], highs[(2 - i) % count_of])
                terms = jnp.where(lane < span, highs[-i % count_of], third)
                first = size * place[g] + i * wide_y
                wide_b[first : first + wide_y, lanes:] = terms.astype(BF16)

    def spread_x(source, tap):
        pieces = []
        for e in range(wide_x):
            piece = None
            for a in range(rows):
                if 0 <= e - a < length:
                    term = tap(e - a) * source[a]
                    piece = term if piece is None else piece + term
            pieces.append(piece)
        return pieces

    def pairs_of(part, half):
        return beside(part[:half], part[half:])

    def blur_zy(p, chosen_groups, row_range, slot):
        blurred[slot, row_range] = dot(wide_a[row_range, :], ahead_a[p]) + dot(wide_b[row_range, :], ahead_b[p])
        for j in range(2):
            v = 2 * p + j
            for g in chosen_groups:
                first = size * place[g]
                high, low = split(blurred[slot, first : first + size, j * lanes : (j + 1) * lanes])
                line = dot(gath[v], stack(pairs_of(high, size // 2), pairs_of(low, size // 2)))
                half = block * cols
                line = line[:half] + line[half:]
                for which in range(2):
                    first = 8 * g + which * block
                    part = line[:, which * lanes : (which + 1) * lanes]
                    lined[v, first : first + block] = part.reshape(block, cols, lanes)

    drain_all(out_recv, sides=(0,))
    prepare(inner)

    for p in range(views // 2):
        blur_zy(p, inner, inner_rows, p)

    drain_all(weight_recv, rows_only=True)
    everyone = stack(*[weight[slot] for slot in range(27)], jnp.zeros((5, lanes), F32))
    counts = jnp.zeros(everyone.shape, F32)

    def along_y(rows_of, first):
        bands = [(rad, 0), (cols, 1), (rad, 2)]
        return stack(*[jnp.broadcast_to(rows_of[first + dy : first + dy + 1], (size, lanes)) for size, dy in bands])

    for v in range(views):
        theirs = weight_of(everyone, v)
        counts = counts + theirs
        for dx in range(3):
            mask[v, dx] = along_y(theirs, 9 + 3 * dx).astype(BF16)
    for dx in range(3):
        for side in range(2):
            part = along_y(everyone, 18 * side + 3 * dx)
            terms = scat_edge[...] * beside(part, part, part)
            mask_edge[dx, side * wide_y : (side + 1) * wide_y] = terms.astype(BF16)
    inverses[...] = jnp.where(counts > 0.0, 1.0 / jnp.maximum(counts, 1.0), 0.0)

    drain_all(far_recv, sides=(1,))
    if early_rounds < rounds:
        greet(early_rounds)
    prepare(outer)

    def two_views(p, slot):
        blur_zy(p, outer, outer_rows, slot)
        scattered = []
        for j in range(2):
            v = 2 * p + j
            blur = taps_ref[0, v, 0] * lined[v, 0:rows]
            for k in range(1, length):
                blur = blur + taps_ref[0, v, k] * lined[v, k : k + rows]
            ratio = (obs[v] / blur).reshape(rows * cols, lanes)
            ratio = beside(*split(ratio))
            back = folded(dot(ratio, astern[v]))
            fringe[...] += dot(ratio, astern_edge[v])
            spread[2 * slot + j] = back.reshape(rows, cols, lanes)
            pieces = spread_x(spread.at[2 * slot + j], lambda k: taps_ref[0, v, k])
            sent = []
            for g in range(groups):
                high, low = split(stack(*pieces[8 * g : 8 * g + 8]))
                high, low = (pairs_of(part, block * cols) for part in (high, low))
                sent.append(stack(high, low, high))
            scattered.append(sent)
        for g in range(groups):
            dx = side_of(g)
            reach = None
            for j in range(2):
                v = 2 * p + j
                here = stack(*[mask[v, dx]] * block)
                here = scat[v] * beside(here, here)[:, : scat.shape[2]]
                part = dot(here, scattered[j][g])
                reach = part if reach is None else reach + part
            for which in range(2):
                first = 8 * g + which * block
                part = reach[:, which * lanes : (which + 1) * lanes]
                total[first : first + block] += part.reshape(block, wide_y, lanes)

    pairs = views // 2
    at_once = 2 if pairs % 2 == 0 else 1
    last_hops = range(early_rounds, rounds)

    def some_views(t, carry):
        for which, hop in enumerate(last_hops[:-1]):

            @pl.when(t == min(which + 1, pairs // at_once - 1))
            def _():
                meet(hop)

        for which in range(at_once):
            two_views(at_once * t + which, which)
        return carry

    lax.fori_loop(0, pairs // at_once, some_views, 0)
    for hop in last_hops[-1:]:
        meet(hop)
    start(back_copies(True))
    def sums_a():
        for slot, offset in enumerate(ring_a):
            yield pltpu.make_async_remote_copy(
                src_ref=stat,
                dst_ref=stat_a.at[slot],
                send_sem=a_send,
                recv_sem=a_recv,
                device_id=partner(*offset),
                device_id_type=MESH,
            )

    def sums_b():
        for slot, offset in enumerate(ring_b):
            yield pltpu.make_async_remote_copy(
                src_ref=part_a,
                dst_ref=stat_b.at[slot],
                send_sem=b_send,
                recv_sem=b_recv,
                device_id=partner(*offset),
                device_id_type=MESH,
            )

    spread[0] = folded(fringe[...]).reshape(rows, cols, lanes)
    pieces = spread_x(spread.at[0], lambda k: taps_x[k : k + 1])
    lane = iota((cols, lanes), 1)
    for g in range(groups):
        turned = pieces[8 * g : 8 * g + 8]
        step = views // 2
        while step:
            low_half = (lane // span) // step % 2 == 0
            for i in range(views):
                if i // step % 2 == 0:
                    one, two = turned[i], turned[i + step]
                    turned[i] = jnp.where(low_half, one, pltpu.roll(two, step * span, 1))
                    turned[i + step] = jnp.where(low_half, pltpu.roll(one, lanes - step * span, 1), two)
            step //= 2
        high, low = split(stack(*turned))
        sides = dot(mask_edge[side_of(g)], stack(high, low, high))
        back_pack[g] = jnp.where(iota((wide_y, lanes), 1) % span < rad, sides[:wide_y], sides[wide_y:])
    lane = iota((wide_y, lanes), 1)
    seen = jnp.zeros((8, lanes), F32)
    for dx in range(3):
        for dy in range(3):
            first_y, last_y = ((0, rad), (rad, rad + cols), (rad + cols, wide_y))[dy]
            first_x, last_x = ((0, rad), (rad, rad + rows), (rad + rows, wide_x))[dx]
            part_y = slice(first_y, last_y)
            part = total[first_x:last_x, part_y, :] * ext[first_x:last_x, part_y, :]
            part = jnp.sum(part.reshape(-1, 8, lanes), axis=0)
            slot = 9 + 3 * dx + dy
            seen = seen + part * inverses[slot : slot + 1, :]
            part_x = slice(first_x // 8, last_x // 8)
            part = back_pack[part_x, part_y, :] * edge[part_x, part_y, :]
            part = jnp.sum(part.reshape(-1, 8, lanes), axis=0)
            left, right = (inverses[at : at + 1, :] for at in (slot - 9, slot + 9))
            seen = seen + part * jnp.where(lane[0:1] % (2 * rad) < rad, left, right)
    wanted = wanted + pltpu.roll(wanted, lanes // 2, 1)
    gotten = jnp.sum(seen, axis=0, keepdims=True)
    gotten = gotten + pltpu.roll(gotten, lanes // 2, 1)
    stat[...] = jnp.where(iota((1, lanes), 1) < lanes // 2, wanted, gotten)

    for copy in sums_a():
        copy.start()
    start(back_copies(False))
    drain_all(back_recv)
    near = back_xy[...]

    def fold(values, size, rad, axis):
        low = lax.slice_in_dim(values, 0, rad, axis=axis)
        mid = lax.slice_in_dim(values, rad, rad + size, axis=axis)
        top = lax.slice_in_dim(values, rad + size, 2 * rad + size, axis=axis)
        if size == 2 * rad:
            return mid + jnp.concatenate([low, top], axis=axis)
        gap_shape = list(low.shape)
        gap_shape[axis] = size - rad
        gap = jnp.zeros(gap_shape, F32)
        return mid + jnp.concatenate([low, gap], axis=axis) + jnp.concatenate([gap, top], axis=axis)

    near = fold(fold(near, rows, rad, 0), cols, rad, 1)
    ends = jnp.where((lane % (2 * rad) < rad)[None], back_right[...], back_left[...])
    ends = fold(fold(ends, pack_rows, pack_rad, 0), cols, rad, 1)
    lane = lax.broadcasted_iota(jnp.int32, (cols, lanes), 1)
    outer = (lane < rad) | (lane >= lanes - rad)
    for x in range(rows):
        rolled = pltpu.roll(ends[x // 8], lanes - (2 * rad * (x % 8) + rad), 1)
        summed = total[rad + x, rad : rad + cols, :] + near[x] + jnp.where(outer, rolled, 0.0)
        updated = ext[rad + x, own_y, :] * (summed / count)
        out_ref[x] = updated

    drain(a_recv, len(ring_a))
    everything = stat[...] + jnp.sum(stat_a[...], axis=0)
    if ring_b:
        part_a[...] = everything
        for copy in sums_b():
            copy.start()
        drain(b_recv, len(ring_b))
        everything = part_a[...] + jnp.sum(stat_b[...], axis=0)
    first_half = iota((1, lanes), 1) < lanes // 2
    wanted = jnp.sum(jnp.where(first_half, everything, 0.0), axis=1, keepdims=True)
    gotten = jnp.sum(jnp.where(first_half, 0.0, everything), axis=1, keepdims=True)
    factor = jnp.broadcast_to(wanted, (1, lanes)) / jnp.broadcast_to(gotten, (1, lanes))
    factor_ref[...] = factor

    drain_all(out_send)
    drain_all(weight_send, rows_only=True)
    drain_all(back_send)
    drain(a_send, len(ring_a))
    if ring_b:
        drain(b_send, len(ring_b))


def on_device(sizes, estimate, observed, coverage, psf_taps):
    rows, cols, lanes = estimate.shape
    views = observed.shape[0]
    rad = (psf_taps.shape[2] - 1) // 2
    wide_x, wide_y = rows + 2 * rad, cols + 2 * rad
    groups, block = wide_x // 8, lanes // wide_y
    _, ring_a, ring_b = rings(sizes)
    n_a, n_b = len(ring_a), max(1, len(ring_b))

    def vm(*shape, dtype=F32):
        return pltpu.VMEM(shape, dtype)

    def dma(*shape):
        return pltpu.SemaphoreType.DMA(shape)

    def in_hbm(values):
        return pltpu.with_memory_space_constraint(values, pltpu.HBM)

    views_all, dims, length = psf_taps.shape
    scratch = [
        pltpu.SMEM((dims, views_all, length), F32),
        pltpu.SMEM((views,), jnp.int32),
        vm(*observed.shape),
        vm(wide_x, wide_y, lanes),
        vm(wide_x * wide_y, 2 * lanes, dtype=BF16),
        vm(wide_x * wide_y, 2 * lanes, dtype=BF16),
        vm(rows // 8, cols, lanes),
        vm(groups, wide_y, lanes),
        vm(groups, wide_y, lanes),
        vm(groups, wide_y, lanes),
        vm(27, 1, lanes),
        vm(32, lanes),
        vm(views, 3, wide_y, lanes, dtype=BF16),
        vm(3, 2 * wide_y, 3 * lanes, dtype=BF16),
        vm(views // 2, 2 * lanes, 2 * lanes, dtype=BF16),
        vm(views // 2, 2 * lanes, 2 * lanes, dtype=BF16),
        vm(views, 2 * block * cols, 2 * lanes, dtype=BF16),
        vm(views, lanes, 3 * block * cols, dtype=BF16),
        vm(views, 2 * lanes, 2 * lanes, dtype=BF16),
        vm(views, 2 * lanes, 2 * lanes, dtype=BF16),
        vm(24, lanes),
        vm(wide_y, 3 * lanes),
        vm(views // 2, wide_x * wide_y, 2 * lanes),
        vm(views, wide_x, cols, lanes),
        vm(views, rows, cols, lanes),
        vm(rows * cols, 2 * lanes),
        vm(wide_x, wide_y, lanes),
        vm(groups, wide_y, lanes),
        vm(groups, wide_y, lanes),
        vm(groups, wide_y, lanes),
        vm(wide_x, wide_y, lanes),
        vm(1, lanes),
        vm(n_a, 1, lanes),
        vm(n_b, 1, lanes),
        vm(1, lanes),
        vm(5 * rows * cols, 1, lanes),
        dma(4),
        pltpu.SemaphoreType.REGULAR((max(1, min(3, sum(sizes) - 3) + late_rounds(sizes)),)),
        *[pltpu.SemaphoreType.DMA] * 11,
    ]
    updated, factor = pl.pallas_call(
        functools.partial(kernel, sizes),
        out_shape=(jax.ShapeDtypeStruct(estimate.shape, F32), jax.ShapeDtypeStruct((1, lanes), F32)),
        in_specs=[
            pl.BlockSpec(memory_space=pl.ANY),
            pl.BlockSpec(memory_space=pl.ANY),
            pl.BlockSpec(memory_space=pl.ANY),
            pl.BlockSpec(memory_space=pl.ANY),
        ],
        out_specs=(pl.BlockSpec(memory_space=pltpu.VMEM), pl.BlockSpec(memory_space=pltpu.VMEM)),
        scratch_shapes=scratch,
        compiler_params=pltpu.CompilerParams(collective_id=0, has_side_effects=True, vmem_limit_bytes=40 * 1024 * 1024),
    )(*map(in_hbm, (jnp.transpose(psf_taps, (1, 0, 2)), coverage.reshape(views), estimate, observed)))
    return updated * factor.reshape(1, 1, lanes)


def solution(mesh):
    sizes = tuple(mesh.shape[axis] for axis in ("bx", "by", "bz"))
    return jax.shard_map(
        functools.partial(on_device, sizes),
        mesh=mesh,
        in_specs=(P("bx", "by", "bz"), P(None, "bx", "by", "bz"), P(None, "bx", "by", "bz"), P()),
        out_specs=P("bx", "by", "bz"),
        check_vma=False,
    )
```

```python
import functools

import jax
import jax.numpy as jnp
from jax import lax
from jax.experimental import pallas as pl
from jax.experimental.pallas import tpu as pltpu
from jax.sharding import PartitionSpec as P

F32 = jnp.float32
BF16 = jnp.bfloat16
MESH = pl.DeviceIdType.MESH


def split(values):
    high = values.astype(BF16)
    low = (values - high.astype(F32)).astype(BF16)
    return high, low


def dot(left, right, dims=((1,), (0,))):
    return lax.dot_general(left, right, (dims, ((), ())), preferred_element_type=F32)


def folded(values):
    half = values.shape[1] // 2
    return values[:, :half] + values[:, half:]


def rings(sizes):
    offsets = [(i, j, k) for i in range(sizes[0]) for j in range(sizes[1]) for k in range(sizes[2])]
    offsets = offsets[1:]
    if len(offsets) < 64:
        return offsets, offsets, []
    return (
        offsets,
        [offset for offset in offsets if offset[0] == 0],
        [offset for offset in offsets if offset[1:] == (0, 0)],
    )


EARLY = 5


def stage_of(dx, dy, dz):
    return 3 if dx and dy else abs(dx) + abs(dy) + abs(dz)


def late_rounds(sizes):
    steps = (-1, 0, 1)
    near = [(i, j, k) for i in steps for j in steps for k in steps if (i, j, k) != (0, 0, 0)]
    everyone = [(i, j, k) for i in range(sizes[0]) for j in range(sizes[1]) for k in range(sizes[2])]
    known = {at: {at} for at in everyone}

    def beyond(at, offset):
        return tuple(a + b for a, b in zip(at, offset))

    def heard(sets, stages):
        return {
            at: set().union(
                sets[-1][at],
                *[
                    sets[min(stage_of(*offset), len(sets) - 1)].get(beyond(at, offset), set())
                    for offset in near
                    if stage_of(*offset) in stages
                ],
            )
            for at in everyone
        }

    history = [known]
    for _ in range(min(EARLY, sum(sizes) - 3)):
        history.append(heard([history[-1]] * 4, (1,)))
    now, rounds = heard(history, (1, 2, 3)), 0
    while any(len(now[at]) < len(everyone) for at in everyone):
        now, rounds = heard([now] * 4, (1,)), rounds + 1
    return rounds


def extent_y(n_y, cols, rad):
    return cols + (rad if n_y == 2 else 2 * rad)


def kernel(
    sizes,
    taps_hbm,
    cover_hbm,
    est_hbm,
    obs_hbm,
    out_ref,
    factor_ref,
    taps_ref,
    cover_ref,
    obs,
    ext,
    wide_a,
    wide_b,
    pack,
    from_left,
    from_right,
    edge,
    weight,
    inverses,
    mask,
    mask_edge,
    ahead_a,
    ahead_b,
    gath,
    scat,
    astern,
    astern_edge,
    taps_x,
    scat_edge,
    blurred,
    lined,
    spread,
    fringe,
    total,
    back_pack,
    back_left,
    back_right,
    back_xy,
    stat,
    stat_a,
    stat_b,
    part_a,
    marks,
    fetch_sem,
    hop_sem,
    out_send,
    out_recv,
    far_recv,
    weight_send,
    weight_recv,
    back_send,
    back_recv,
    a_send,
    a_recv,
    b_send,
    b_recv,
):
    n_x, n_y, n_z = sizes
    views, rows, cols, lanes = obs.shape
    length = taps_ref.shape[2]
    rad = (length - 1) // 2
    wide_x, wide_y = rows + 2 * rad, extent_y(n_y, cols, rad)
    groups = wide_x // 8
    first_y = wide_y - cols - rad
    bands_y = [(first_y, cols, 1), (first_y + cols, rad, 2)]
    if first_y:
        bands_y.insert(0, (0, rad, 0))
    me_x, me_y, me_z = lax.axis_index("bx"), lax.axis_index("by"), lax.axis_index("bz")

    own_x, own_y = slice(rad, rad + rows), slice(first_y, first_y + cols)
    own = ext.at[own_x, own_y, :]
    loads = [
        pltpu.make_async_copy(source, target, fetch_sem.at[which])
        for which, (source, target) in enumerate(
            ((est_hbm, own), (cover_hbm, cover_ref), (taps_hbm, taps_ref), (obs_hbm, obs))
        )
    ]
    for load in loads:
        load.start()

    def exists(dx, dy, dz):
        ok = None
        for step, me, count in ((dx, me_x, n_x), (dy, me_y, n_y), (dz, me_z, n_z)):
            if step == 0:
                continue
            inside = (me + step >= 0) & (me + step < count)
            ok = inside if ok is None else ok & inside
        return ok

    def device(dx, dy, dz):
        return {"bx": me_x + dx, "by": me_y + dy, "bz": me_z + dz}

    steps = (-1, 0, 1)
    around = [(dx, dy, dz) for dz in steps for dx in steps for dy in steps if (dx, dy, dz) != (0, 0, 0)]
    ring_all, ring_a, ring_b = rings(sizes)

    def partner(i, j, k):
        return {
            "bx": lax.rem(me_x + i, n_x),
            "by": lax.rem(me_y + j, n_y),
            "bz": lax.rem(me_z + k, n_z),
        }

    for part in ((slice(0, rad), slice(0, wide_y)), (slice(rad + rows, wide_x), slice(0, wide_y))):
        ext[part[0], part[1], :] = jnp.zeros((rad, wide_y, lanes), F32)
    for start_y, size_y, dy in bands_y:
        if dy != 1:
            ext[own_x, start_y : start_y + size_y, :] = jnp.zeros((rows, size_y, lanes), F32)
    from_left[...] = jnp.zeros(from_left.shape, F32)
    from_right[...] = jnp.zeros(from_right.shape, F32)
    weight[...] = jnp.zeros(weight.shape, F32)

    barrier = pltpu.get_barrier_semaphore()
    faces = [offset for offset in around if sum(map(abs, offset)) == 1]
    near_by = sum(exists(*offset).astype(jnp.int32) for offset in faces)
    early_rounds = min(EARLY, n_x + n_y + n_z - 3)
    rounds = early_rounds + late_rounds(sizes)

    def greet(which):
        semaphore = barrier if which == 0 else hop_sem.at[which - 1]
        for offset in faces:

            @pl.when(exists(*offset))
            def _():
                pl.semaphore_signal(semaphore, inc=1, device_id=device(*offset), device_id_type=MESH)

    def meet(which):
        pl.semaphore_wait(barrier if which == 0 else hop_sem.at[which - 1], near_by)
        if which + 1 < rounds and which + 1 != early_rounds:
            greet(which + 1)

    greet(0)

    back_xy[...] = jnp.zeros(back_xy.shape, F32)
    back_left[...] = jnp.zeros(back_left.shape, F32)
    back_right[...] = jnp.zeros(back_right.shape, F32)
    total[...] = jnp.zeros(total.shape, F32)
    fringe[...] = jnp.zeros(fringe.shape, F32)

    loads[1].wait()
    lane = lax.broadcasted_iota(jnp.int32, (1, lanes), 1)
    row = jnp.zeros((1, lanes), F32)
    for v in range(views):
        mine = jnp.full((1, lanes), cover_ref[v], jnp.int32).astype(F32)
        row = jnp.where(lane // (lanes // views) == v, mine, row)
    weight[13] = row
    loads[0].wait()

    def cut(step, size, width):
        return pl.ds(0, size) if step == 0 else pl.ds(0 if step < 0 else size - width, width)

    def wide(step, size, width):
        return pl.ds(width, size) if step == 0 else pl.ds(0 if step < 0 else width + size, width)

    def wide_cols(step):
        if step == 0:
            return pl.ds(first_y, cols)
        return pl.ds(0 if step < 0 and first_y else first_y + cols, rad)

    def place_y(row):
        return row - first_y if first_y else jnp.where(row < cols, row, row - me_y * wide_y)

    pack_rows, pack_rad = rows // 8, rad // 8

    def slot_of(dx, dy, dz):
        return 9 * (dz + 1) + 3 * (dx + 1) + dy + 1

    def out_copies(hops, what, flat=(True, False)):
        for dx, dy, dz in sorted(around, key=lambda offset: (abs(offset[0]), abs(offset[2]))):
            if stage_of(dx, dy, dz) not in hops or (dz == 0) not in flat:
                continue
            slot = slot_of(dx, dy, dz)
            size, width = (rows, rad) if dz == 0 else (pack_rows, pack_rad)
            source = own if dz == 0 else pack
            target = (from_right, ext, from_left)[dz + 1]
            pairs = (
                (weight.at[13], weight.at[slot_of(-dx, -dy if first_y else abs(dy), -dz)]),
                (
                    source.at[cut(dx, size, width), cut(dy, cols, rad), :],
                    target.at[wide(-dx, size, width), wide_cols(-dy), :],
                ),
            )
            sems = ((weight_send, weight_recv), (out_send, far_recv if dx else out_recv))
            copy = pltpu.make_async_remote_copy(
                src_ref=pairs[what][0],
                dst_ref=pairs[what][1],
                send_sem=sems[what][0],
                recv_sem=sems[what][1],
                device_id=device(dx, dy, dz),
                device_id_type=MESH,
            )
            yield exists(dx, dy, dz), [copy]

    def back_copies(flat):
        for dx, dy, dz in around:
            if (dz == 0) != flat:
                continue
            size, width = (rows, rad) if dz == 0 else (pack_rows, pack_rad)
            source = total if dz == 0 else back_pack
            target = (back_right, back_xy, back_left)[dz + 1]
            copy = pltpu.make_async_remote_copy(
                src_ref=source.at[wide(dx, size, width), wide_cols(dy), :],
                dst_ref=target.at[wide(-dx, size, width), wide_cols(-dy), :],
                send_sem=back_send,
                recv_sem=back_recv,
                device_id=device(dx, dy, dz),
                device_id_type=MESH,
            )
            yield exists(dx, dy, dz), [copy]

    def start(family):
        for sends, copies in family:

            @pl.when(sends)
            def _():
                for copy in copies:
                    copy.start()

    def drain(semaphore, amount):
        bytes_of = marks.at[pl.ds(0, amount)]
        pltpu.make_async_remote_copy(
            src_ref=bytes_of,
            dst_ref=bytes_of,
            send_sem=semaphore,
            recv_sem=semaphore,
            device_id=partner(*ring_all[0]),
            device_id_type=MESH,
        ).wait_recv()

    def drain_all(semaphore, sides=(0, 1), rows_only=False):
        counts_of = [
            (min(count - 1, 2), (me > 0).astype(jnp.int32) + (me < count - 1).astype(jnp.int32))
            for me, count in ((me_x, n_x), (me_y, n_y), (me_z, n_z))
        ]
        for c_x in range(min(1, n_x - 1), counts_of[0][0] + 1):
            for c_y in range(min(1, n_y - 1), counts_of[1][0] + 1):
                for c_z in range(min(1, n_z - 1), counts_of[2][0] + 1):
                    amount = 0
                    for dx, dy, dz in ((i, j, k) for i in (0, 1) for j in (0, 1) for k in (0, 1)):
                        if (dx, dy, dz) == (0, 0, 0) or dx not in sides:
                            continue
                        size, width = (rows, rad) if dz == 0 else (pack_rows, pack_rad)
                        message = 1 if rows_only else (width if dx else size) * (rad if dy else cols)
                        amount += (c_x if dx else 1) * (c_y if dy else 1) * (c_z if dz else 1) * message

                    if not amount:
                        continue

                    @pl.when((counts_of[0][1] == c_x) & (counts_of[1][1] == c_y) & (counts_of[2][1] == c_z))
                    def _():
                        drain(semaphore, amount)

    def iota(shape, dim):
        return lax.broadcasted_iota(jnp.int32, shape, dim)

    span = 2 * rad
    block = lanes // (cols + 2 * rad)
    part_rows = block * wide_y

    def stack(*parts):
        return jnp.concatenate(parts, axis=0)

    def beside(*parts):
        return jnp.concatenate(parts, axis=1)

    def build(p, carry):
        for j in range(2):
            v = 2 * p + j

            def summed(dim):
                values = [taps_ref[dim, v, k] for k in range(length)]
                while len(values) > 1:
                    values = [sum(values[i : i + 2]) for i in range(0, len(values), 2)]
                return jnp.full((8, lanes), values[0], F32)

            inverse = 1.0 / (summed(0) * summed(1) * summed(2))

            def chosen(offset, dim):
                result = jnp.zeros(offset.shape, F32)
                for k in range(length):
                    result = jnp.where(offset == k, taps_ref[dim, v, k], result)
                return result

            def scaled(part):
                return (part.reshape(-1, 8, lanes) * inverse[None]).reshape(part.shape)

            here = slice(j * lanes, (j + 1) * lanes)
            square = (lanes, lanes)
            main = scaled(chosen(iota(square, 0) - iota(square, 1) + rad, 2))
            row, col = iota((span, lanes), 0), iota((span, lanes), 1)
            edges = scaled(chosen(jnp.where(row < rad, row, row + lanes) - col, 2))
            high, low = split(main)
            ahead_a[p, :, here] = stack(high, high)
            ahead_b[p, :lanes, here] = low
            high, low = split(edges)
            ahead_b[p, lanes:, here] = stack(high, high, low, jnp.zeros((lanes - 3 * span, lanes), BF16))
            high, low = split(main.T)
            astern[v] = stack(beside(high, low), beside(high, jnp.zeros(square, BF16)))
            turned = jnp.where(iota(square, 1) // span == v, stack(*[edges] * views).T, 0.0)
            high, low = split(turned)
            astern_edge[v] = stack(beside(high, low), beside(high, jnp.zeros(square, BF16)))
            shape = (block * cols, lanes)
            row, col = iota(shape, 0), iota(shape, 1)
            offset = jnp.where(row // cols == col // wide_y, place_y(col % wide_y) + rad - row % cols, -1)
            blur_y = chosen(offset, 1)
            high, low = split(blur_y)
            high, low = high[:, :part_rows], low[:, :part_rows]
            gath[v] = stack(beside(high, high), beside(low, jnp.zeros(low.shape, BF16)))
            turned = blur_y.T[:part_rows]
            high = turned.astype(BF16).astype(F32)
            low = turned - high
            scat[v] = beside(high, high, low).astype(BF16)
        return carry

    def lines_of(dim):
        lane = iota((1, lanes), 1)
        lines = []
        for k in range(length):
            line = jnp.zeros((1, lanes), F32)
            for v in range(views):
                line = jnp.where(lane // span == v, taps_ref[dim, v, k], line)
            lines.append(line)
        return lines

    meet(0)
    start(out_copies((1,), 1, (True,)))
    lane = lax.broadcasted_iota(jnp.int32, (cols, lanes), 1)
    for g in range(rows // 8):
        merged = jnp.zeros((cols, lanes), F32)
        for i in range(8):
            rolled = pltpu.roll(ext[rad + 8 * g + i, own_y, :], 2 * rad * i + rad, 1)
            merged = jnp.where(lane // (2 * rad) == i, rolled, merged)
        pack[g] = merged

    start(out_copies((1,), 0))
    start(out_copies((1,), 1, (False,)))
    loads[2].wait()
    stops = [min(stop, views // 2) for stop in (0, 1, 2, views // 2)]
    for hop in range(1, 4):
        lax.fori_loop(stops[hop - 1], stops[hop], build, 0)
        if hop < min(3, early_rounds):
            meet(hop)
        if hop in (1, 2):
            start(out_copies((hop + 1,), 0))
            start(out_copies((hop + 1,), 1))

    for k, line in enumerate(lines_of(0)):
        taps_x[k : k + 1] = line
    shape = (wide_y, lanes)
    offset = place_y(iota(shape, 0)) + rad - iota(shape, 1) % cols
    base = jnp.zeros(shape, F32)
    for k, line in enumerate(lines_of(1)):
        base = jnp.where(offset == k, line, base)
    high = base.astype(BF16).astype(F32)
    scat_edge[...] = beside(high, high, base - high)

    loads[3].wait()
    def weight_of(rows_of, v):
        first = v * (lanes // views)
        return jnp.broadcast_to(rows_of[:, first : first + 1], rows_of.shape)

    mine = jnp.broadcast_to(weight[13], (8, lanes))
    count = jnp.zeros((8, lanes), F32)
    seen = jnp.zeros((8, lanes), F32)
    for v in range(views):
        weight_v = weight_of(mine, v)
        count = count + weight_v
        seen = seen + weight_v * jnp.sum(obs[v].reshape(-1, 8, lanes), axis=0)
    count = count[0:1]
    wanted = jnp.sum(seen, axis=0, keepdims=True) / count

    def side_of(g):
        return 0 if 8 * g < rad else (1 if 8 * g < rad + rows else 2)

    inner = [g for g in range(groups) if side_of(g) == 1]
    outer = [g for g in range(groups) if side_of(g) != 1]
    place = {g: which for which, g in enumerate(inner + outer)}
    size = 8 * wide_y
    inner_rows, outer_rows = slice(0, size * len(inner)), slice(size * len(inner), size * groups)

    def prepare(chosen_groups):
        lane = iota((wide_y, lanes), 1)
        for g in chosen_groups:
            here = slice(size * place[g], size * (place[g] + 1))
            high, low = split(ext[8 * g : 8 * g + 8].reshape(size, lanes))
            wide_a[here, :lanes] = high
            wide_a[here, lanes:] = low
            wide_b[here, :lanes] = high
            merged = jnp.where(lane % span < rad, from_left[g], from_right[g])
            edge[g] = merged
            high = merged.astype(BF16).astype(F32)
            low = merged - high
            count_of = lanes // span
            highs = [pltpu.roll(high, span * i, 1) if i else high for i in range(count_of)]
            lows = [pltpu.roll(low, span * i, 1) if i else low for i in range(count_of)]
            rows_of = []
            for i in range(8):
                third = jnp.where(lane < 2 * span, lows[(1 - i) % count_of], highs[(2 - i) % count_of])
                terms = jnp.where(lane < span, highs[-i % count_of], third)
                rows_of.append(terms)
            wide_b[here, lanes:] = stack(*rows_of).astype(BF16)

    def spread_x(source, tap):
        pieces = []
        for e in range(wide_x):
            piece = None
            for a in range(rows):
                if 0 <= e - a < length:
                    term = tap(e - a) * source[a]
                    piece = term if piece is None else piece + term
            pieces.append(piece)
        return pieces

    def pairs_of(part, half):
        return beside(part[:half], part[half:])

    def blur_zy(p, chosen_groups, row_range, slot):
        blurred[slot, row_range] = dot(wide_a[row_range, :], ahead_a[p]) + dot(wide_b[row_range, :], ahead_b[p])
        for j in range(2):
            v = 2 * p + j
            for g in chosen_groups:
                first = size * place[g]
                high, low = split(blurred[slot, first : first + size, j * lanes : (j + 1) * lanes])
                line = dot(gath[v], stack(pairs_of(high, size // 2), pairs_of(low, size // 2)))
                half = block * cols
                line = line[:half] + line[half:]
                for which in range(2):
                    first = 8 * g + which * block
                    part = line[:, which * lanes : (which + 1) * lanes]
                    lined[v, first : first + block] = part.reshape(block, cols, lanes)

    drain_all(out_recv, sides=(0,))
    if early_rounds > 3:
        meet(3)
    prepare(inner)

    for p in range(views // 2):
        blur_zy(p, inner, inner_rows, p)

    for hop in range(4, early_rounds):
        meet(hop)
    drain_all(weight_recv, rows_only=True)
    everyone = stack(*[weight[slot] for slot in range(27)], jnp.zeros((5, lanes), F32))
    counts = jnp.zeros(everyone.shape, F32)

    def along_y(rows_of, first):
        return stack(*[jnp.broadcast_to(rows_of[first + dy : first + dy + 1], (size_y, lanes)) for _, size_y, dy in bands_y])

    for v in range(views):
        theirs = weight_of(everyone, v)
        counts = counts + theirs
        for dx in range(3):
            mask[v, dx] = stack(*[along_y(theirs, 9 + 3 * dx)] * block).astype(BF16)
    for dx in range(3):
        terms = []
        for side in range(2):
            part = along_y(everyone, 18 * side + 3 * dx)
            terms.append(scat_edge[...] * beside(part, part, part))
        mask_edge[dx] = stack(*terms).astype(BF16)
    inverses[...] = jnp.where(counts > 0.0, 1.0 / jnp.maximum(counts, 1.0), 0.0)

    drain_all(far_recv, sides=(1,))
    if early_rounds < rounds:
        greet(early_rounds)
    prepare(outer)

    def two_views(p, slot):
        blur_zy(p, outer, outer_rows, slot)
        scattered = []
        for j in range(2):
            v = 2 * p + j
            blur = taps_ref[0, v, 0] * lined[v, 0:rows]
            for k in range(1, length):
                blur = blur + taps_ref[0, v, k] * lined[v, k : k + rows]
            ratio = (obs[v] / blur).reshape(rows * cols, lanes)
            ratio = beside(*split(ratio))
            back = folded(dot(ratio, astern[v]))
            fringe[...] += dot(ratio, astern_edge[v])
            spread[2 * slot + j] = back.reshape(rows, cols, lanes)
            pieces = spread_x(spread.at[2 * slot + j], lambda k: taps_ref[0, v, k])
            sent = []
            for g in range(groups):
                high, low = split(stack(*pieces[8 * g : 8 * g + 8]))
                high, low = (pairs_of(part, block * cols) for part in (high, low))
                sent.append(stack(high, low, high))
            scattered.append(sent)
        for g in range(groups):
            dx = side_of(g)
            reach = None
            for j in range(2):
                v = 2 * p + j
                here = mask[v, dx]
                here = scat[v] * beside(here, here)[:, : scat.shape[2]]
                part = dot(here, scattered[j][g])
                reach = part if reach is None else reach + part
            for which in range(2):
                first = 8 * g + which * block
                part = reach[:, which * lanes : (which + 1) * lanes]
                total[first : first + block] += part.reshape(block, wide_y, lanes)

    for p in range(views // 2):
        two_views(p, p)
    for hop in range(early_rounds, rounds):
        meet(hop)
    start(back_copies(True))
    def sums_a():
        for slot, offset in enumerate(ring_a):
            yield pltpu.make_async_remote_copy(
                src_ref=stat,
                dst_ref=stat_a.at[slot],
                send_sem=a_send,
                recv_sem=a_recv,
                device_id=partner(*offset),
                device_id_type=MESH,
            )

    def sums_b():
        for slot, offset in enumerate(ring_b):
            yield pltpu.make_async_remote_copy(
                src_ref=part_a,
                dst_ref=stat_b.at[slot],
                send_sem=b_send,
                recv_sem=b_recv,
                device_id=partner(*offset),
                device_id_type=MESH,
            )

    spread[0] = folded(fringe[...]).reshape(rows, cols, lanes)
    pieces = spread_x(spread.at[0], lambda k: taps_x[k : k + 1])
    lane = iota((cols, lanes), 1)
    for g in range(groups):
        turned = pieces[8 * g : 8 * g + 8]
        step = views // 2
        while step:
            low_half = (lane // span) // step % 2 == 0
            for i in range(views):
                if i // step % 2 == 0:
                    one, two = turned[i], turned[i + step]
                    turned[i] = jnp.where(low_half, one, pltpu.roll(two, step * span, 1))
                    turned[i + step] = jnp.where(low_half, pltpu.roll(one, lanes - step * span, 1), two)
            step //= 2
        high, low = split(stack(*turned))
        sides = dot(mask_edge[side_of(g)], stack(high, low, high))
        back_pack[g] = jnp.where(iota((wide_y, lanes), 1) % span < rad, sides[:wide_y], sides[wide_y:])
    lane = iota((wide_y, lanes), 1)
    seen = jnp.zeros((8, lanes), F32)
    for dx in range(3):
        for start_y, size_y, dy in bands_y:
            first_x, last_x = ((0, rad), (rad, rad + rows), (rad + rows, wide_x))[dx]
            part_y = slice(start_y, start_y + size_y)
            part = total[first_x:last_x, part_y, :] * ext[first_x:last_x, part_y, :]
            part = jnp.sum(part.reshape(-1, 8, lanes), axis=0)
            slot = 9 + 3 * dx + dy
            seen = seen + part * inverses[slot : slot + 1, :]
            part_x = slice(first_x // 8, last_x // 8)
            part = back_pack[part_x, part_y, :] * edge[part_x, part_y, :]
            part = jnp.sum(part.reshape(-1, 8, lanes), axis=0)
            left, right = (inverses[at : at + 1, :] for at in (slot - 9, slot + 9))
            seen = seen + part * jnp.where(lane[0:1] % (2 * rad) < rad, left, right)
    wanted = wanted + pltpu.roll(wanted, lanes // 2, 1)
    gotten = jnp.sum(seen, axis=0, keepdims=True)
    gotten = gotten + pltpu.roll(gotten, lanes // 2, 1)
    stat[...] = jnp.where(iota((1, lanes), 1) < lanes // 2, wanted, gotten)

    for copy in sums_a():
        copy.start()
    start(back_copies(False))
    drain_all(back_recv)
    near = back_xy[...]

    def fold(values, size, rad, axis):
        low = lax.slice_in_dim(values, 0, rad, axis=axis)
        mid = lax.slice_in_dim(values, rad, rad + size, axis=axis)
        top = lax.slice_in_dim(values, rad + size, 2 * rad + size, axis=axis)
        if size == 2 * rad:
            return mid + jnp.concatenate([low, top], axis=axis)
        gap_shape = list(low.shape)
        gap_shape[axis] = size - rad
        gap = jnp.zeros(gap_shape, F32)
        return mid + jnp.concatenate([low, gap], axis=axis) + jnp.concatenate([gap, top], axis=axis)

    def fold_y(values):
        if first_y:
            return fold(values, cols, rad, 1)
        part = values[:, cols:]
        gap = jnp.zeros((part.shape[0], cols - rad, lanes), F32)
        before, after = (jnp.concatenate(pair, axis=1) for pair in ((part, gap), (gap, part)))
        return values[:, :cols] + jnp.where(me_y == 0, after, before)

    near = fold_y(fold(near, rows, rad, 0))
    ends = jnp.where((lane % (2 * rad) < rad)[None], back_right[...], back_left[...])
    ends = fold_y(fold(ends, pack_rows, pack_rad, 0))
    lane = lax.broadcasted_iota(jnp.int32, (cols, lanes), 1)
    outer = (lane < rad) | (lane >= lanes - rad)
    for x in range(rows):
        rolled = pltpu.roll(ends[x // 8], lanes - (2 * rad * (x % 8) + rad), 1)
        summed = total[rad + x, own_y, :] + near[x] + jnp.where(outer, rolled, 0.0)
        updated = ext[rad + x, own_y, :] * (summed / count)
        out_ref[x] = updated

    drain(a_recv, len(ring_a))
    everything = stat[...] + jnp.sum(stat_a[...], axis=0)
    if ring_b:
        part_a[...] = everything
        for copy in sums_b():
            copy.start()
        drain(b_recv, len(ring_b))
        everything = part_a[...] + jnp.sum(stat_b[...], axis=0)
    first_half = iota((1, lanes), 1) < lanes // 2
    wanted = jnp.sum(jnp.where(first_half, everything, 0.0), axis=1, keepdims=True)
    gotten = jnp.sum(jnp.where(first_half, 0.0, everything), axis=1, keepdims=True)
    factor = jnp.broadcast_to(wanted, (1, lanes)) / jnp.broadcast_to(gotten, (1, lanes))
    factor_ref[...] = factor

    drain_all(out_send)
    drain_all(weight_send, rows_only=True)
    drain_all(back_send)
    drain(a_send, len(ring_a))
    if ring_b:
        drain(b_send, len(ring_b))


def on_device(sizes, estimate, observed, coverage, psf_taps):
    rows, cols, lanes = estimate.shape
    views = observed.shape[0]
    rad = (psf_taps.shape[2] - 1) // 2
    wide_x, wide_y = rows + 2 * rad, extent_y(sizes[1], cols, rad)
    groups, block = wide_x // 8, lanes // (cols + 2 * rad)
    _, ring_a, ring_b = rings(sizes)
    n_a, n_b = len(ring_a), max(1, len(ring_b))

    def vm(*shape, dtype=F32):
        return pltpu.VMEM(shape, dtype)

    def dma(*shape):
        return pltpu.SemaphoreType.DMA(shape)

    def in_hbm(values):
        return pltpu.with_memory_space_constraint(values, pltpu.HBM)

    views_all, dims, length = psf_taps.shape
    scratch = [
        pltpu.SMEM((dims, views_all, length), F32),
        pltpu.SMEM((views,), jnp.int32),
        vm(*observed.shape),
        vm(wide_x, wide_y, lanes),
        vm(wide_x * wide_y, 2 * lanes, dtype=BF16),
        vm(wide_x * wide_y, 2 * lanes, dtype=BF16),
        vm(rows // 8, cols, lanes),
        vm(groups, wide_y, lanes),
        vm(groups, wide_y, lanes),
        vm(groups, wide_y, lanes),
        vm(27, 1, lanes),
        vm(32, lanes),
        vm(views, 3, block * wide_y, lanes, dtype=BF16),
        vm(3, 2 * wide_y, 3 * lanes, dtype=BF16),
        vm(views // 2, 2 * lanes, 2 * lanes, dtype=BF16),
        vm(views // 2, 2 * lanes, 2 * lanes, dtype=BF16),
        vm(views, 2 * block * cols, 2 * block * wide_y, dtype=BF16),
        vm(views, block * wide_y, 3 * block * cols, dtype=BF16),
        vm(views, 2 * lanes, 2 * lanes, dtype=BF16),
        vm(views, 2 * lanes, 2 * lanes, dtype=BF16),
        vm(24, lanes),
        vm(wide_y, 3 * lanes),
        vm(views // 2, wide_x * wide_y, 2 * lanes),
        vm(views, wide_x, cols, lanes),
        vm(views, rows, cols, lanes),
        vm(rows * cols, 2 * lanes),
        vm(wide_x, wide_y, lanes),
        vm(groups, wide_y, lanes),
        vm(groups, wide_y, lanes),
        vm(groups, wide_y, lanes),
        vm(wide_x, wide_y, lanes),
        vm(1, lanes),
        vm(n_a, 1, lanes),
        vm(n_b, 1, lanes),
        vm(1, lanes),
        vm(5 * rows * cols, 1, lanes),
        dma(4),
        pltpu.SemaphoreType.REGULAR((max(1, min(EARLY, sum(sizes) - 3) + late_rounds(sizes)),)),
        *[pltpu.SemaphoreType.DMA] * 11,
    ]
    updated, factor = pl.pallas_call(
        functools.partial(kernel, sizes),
        out_shape=(jax.ShapeDtypeStruct(estimate.shape, F32), jax.ShapeDtypeStruct((1, lanes), F32)),
        in_specs=[
            pl.BlockSpec(memory_space=pl.ANY),
            pl.BlockSpec(memory_space=pl.ANY),
            pl.BlockSpec(memory_space=pl.ANY),
            pl.BlockSpec(memory_space=pl.ANY),
        ],
        out_specs=(pl.BlockSpec(memory_space=pltpu.VMEM), pl.BlockSpec(memory_space=pltpu.VMEM)),
        scratch_shapes=scratch,
        compiler_params=pltpu.CompilerParams(collective_id=0, has_side_effects=True, vmem_limit_bytes=40 * 1024 * 1024),
    )(*map(in_hbm, (jnp.transpose(psf_taps, (1, 0, 2)), coverage.reshape(views), estimate, observed)))
    return updated * factor.reshape(1, 1, lanes)


def solution(mesh):
    sizes = tuple(mesh.shape[axis] for axis in ("bx", "by", "bz"))
    return jax.shard_map(
        functools.partial(on_device, sizes),
        mesh=mesh,
        in_specs=(P("bx", "by", "bz"), P(None, "bx", "by", "bz"), P(None, "bx", "by", "bz"), P()),
        out_specs=P("bx", "by", "bz"),
        check_vma=False,
    )
```

```python
import functools

import jax
import jax.numpy as jnp
from jax import lax
from jax.experimental import pallas as pl
from jax.experimental.pallas import tpu as pltpu
from jax.sharding import PartitionSpec as P

F32 = jnp.float32
BF16 = jnp.bfloat16
MESH = pl.DeviceIdType.MESH


def split(values):
    high = values.astype(BF16)
    low = (values - high.astype(F32)).astype(BF16)
    return high, low


def dot(left, right, dims=((1,), (0,))):
    return lax.dot_general(left, right, (dims, ((), ())), preferred_element_type=F32)


def folded(values):
    half = values.shape[1] // 2
    return values[:, :half] + values[:, half:]


def rings(sizes):
    offsets = [(i, j, k) for i in range(sizes[0]) for j in range(sizes[1]) for k in range(sizes[2])]
    offsets = offsets[1:]
    if len(offsets) < 64:
        return offsets, offsets, []
    return (
        offsets,
        [offset for offset in offsets if offset[0] == 0],
        [offset for offset in offsets if offset[1:] == (0, 0)],
    )


EARLY = 5


def stage_of(dx, dy, dz):
    return 3 if dx and dy else abs(dx) + abs(dy) + abs(dz)


def late_rounds(sizes):
    steps = (-1, 0, 1)
    near = [(i, j, k) for i in steps for j in steps for k in steps if (i, j, k) != (0, 0, 0)]
    everyone = [(i, j, k) for i in range(sizes[0]) for j in range(sizes[1]) for k in range(sizes[2])]
    known = {at: {at} for at in everyone}

    def beyond(at, offset):
        return tuple(a + b for a, b in zip(at, offset))

    def heard(sets, stages):
        return {
            at: set().union(
                sets[-1][at],
                *[
                    sets[min(stage_of(*offset), len(sets) - 1)].get(beyond(at, offset), set())
                    for offset in near
                    if stage_of(*offset) in stages
                ],
            )
            for at in everyone
        }

    history = [known]
    for _ in range(min(EARLY, sum(sizes) - 3)):
        history.append(heard([history[-1]] * 4, (1,)))
    now, rounds = heard(history, (1, 2, 3)), 0
    while any(len(now[at]) < len(everyone) for at in everyone):
        now, rounds = heard([now] * 4, (1,)), rounds + 1
    return rounds


def extent_y(n_y, cols, rad):
    return cols + (rad if n_y == 2 else 2 * rad)


def kernel(
    sizes,
    taps_hbm,
    cover_hbm,
    est_hbm,
    obs_hbm,
    out_ref,
    factor_ref,
    taps_ref,
    cover_ref,
    obs,
    ext,
    wide_a,
    wide_b,
    pack,
    from_left,
    from_right,
    edge,
    weight,
    inverses,
    mask,
    mask_edge,
    ahead_a,
    ahead_b,
    gath,
    scat,
    astern,
    astern_edge,
    taps_x,
    scat_edge,
    blurred,
    lined,
    spread,
    fringe,
    total,
    back_pack,
    back_left,
    back_right,
    back_xy,
    stat,
    stat_a,
    stat_b,
    part_a,
    marks,
    fetch_sem,
    hop_sem,
    out_send,
    out_recv,
    far_recv,
    weight_send,
    weight_recv,
    back_send,
    back_recv,
    a_send,
    a_recv,
    b_send,
    b_recv,
):
    n_x, n_y, n_z = sizes
    views, rows, cols, lanes = obs.shape
    length = taps_ref.shape[2]
    rad = (length - 1) // 2
    wide_x, wide_y = rows + 2 * rad, extent_y(n_y, cols, rad)
    groups = wide_x // 8
    first_y = wide_y - cols - rad
    bands_y = [(first_y, cols, 1), (first_y + cols, rad, 2)]
    if first_y:
        bands_y.insert(0, (0, rad, 0))
    me_x, me_y, me_z = lax.axis_index("bx"), lax.axis_index("by"), lax.axis_index("bz")

    own_x, own_y = slice(rad, rad + rows), slice(first_y, first_y + cols)
    own = ext.at[own_x, own_y, :]
    loads = [
        pltpu.make_async_copy(source, target, fetch_sem.at[which])
        for which, (source, target) in enumerate(
            ((est_hbm, own), (cover_hbm, cover_ref), (taps_hbm, taps_ref), (obs_hbm, obs))
        )
    ]
    for load in loads:
        load.start()

    def exists(dx, dy, dz):
        ok = None
        for step, me, count in ((dx, me_x, n_x), (dy, me_y, n_y), (dz, me_z, n_z)):
            if step == 0:
                continue
            inside = (me + step >= 0) & (me + step < count)
            ok = inside if ok is None else ok & inside
        return ok

    def device(dx, dy, dz):
        return {"bx": me_x + dx, "by": me_y + dy, "bz": me_z + dz}

    steps = (-1, 0, 1)
    around = [(dx, dy, dz) for dz in steps for dx in steps for dy in steps if (dx, dy, dz) != (0, 0, 0)]
    ring_all, ring_a, ring_b = rings(sizes)

    def partner(i, j, k):
        return {
            "bx": lax.rem(me_x + i, n_x),
            "by": lax.rem(me_y + j, n_y),
            "bz": lax.rem(me_z + k, n_z),
        }

    for part in ((slice(0, rad), slice(0, wide_y)), (slice(rad + rows, wide_x), slice(0, wide_y))):
        ext[part[0], part[1], :] = jnp.zeros((rad, wide_y, lanes), F32)
    for start_y, size_y, dy in bands_y:
        if dy != 1:
            ext[own_x, start_y : start_y + size_y, :] = jnp.zeros((rows, size_y, lanes), F32)
    from_left[...] = jnp.zeros(from_left.shape, F32)
    from_right[...] = jnp.zeros(from_right.shape, F32)
    weight[...] = jnp.zeros(weight.shape, F32)

    barrier = pltpu.get_barrier_semaphore()
    faces = [offset for offset in around if sum(map(abs, offset)) == 1]
    near_by = sum(exists(*offset).astype(jnp.int32) for offset in faces)
    early_rounds = min(EARLY, n_x + n_y + n_z - 3)
    rounds = early_rounds + late_rounds(sizes)

    def greet(which):
        semaphore = barrier if which == 0 else hop_sem.at[which - 1]
        for offset in faces:

            @pl.when(exists(*offset))
            def _():
                pl.semaphore_signal(semaphore, inc=1, device_id=device(*offset), device_id_type=MESH)

    def meet(which):
        pl.semaphore_wait(barrier if which == 0 else hop_sem.at[which - 1], near_by)
        if which + 1 < rounds and which + 1 != early_rounds:
            greet(which + 1)

    greet(0)

    back_xy[...] = jnp.zeros(back_xy.shape, F32)
    back_left[...] = jnp.zeros(back_left.shape, F32)
    back_right[...] = jnp.zeros(back_right.shape, F32)
    total[...] = jnp.zeros(total.shape, F32)
    fringe[...] = jnp.zeros(fringe.shape, F32)

    loads[1].wait()
    lane = lax.broadcasted_iota(jnp.int32, (1, lanes), 1)
    row = jnp.zeros((1, lanes), F32)
    for v in range(views):
        mine = jnp.full((1, lanes), cover_ref[v], jnp.int32).astype(F32)
        row = jnp.where(lane // (lanes // views) == v, mine, row)
    weight[13] = row
    loads[0].wait()

    def cut(step, size, width):
        return pl.ds(0, size) if step == 0 else pl.ds(0 if step < 0 else size - width, width)

    def wide(step, size, width):
        return pl.ds(width, size) if step == 0 else pl.ds(0 if step < 0 else width + size, width)

    def wide_cols(step):
        if step == 0:
            return pl.ds(first_y, cols)
        return pl.ds(0 if step < 0 and first_y else first_y + cols, rad)

    def place_y(row):
        return row - first_y if first_y else jnp.where(row < cols, row, row - me_y * wide_y)

    pack_rows, pack_rad = rows // 8, rad // 8

    def slot_of(dx, dy, dz):
        return 9 * (dz + 1) + 3 * (dx + 1) + dy + 1

    def out_copies(hops, what, flat=(True, False)):
        for dx, dy, dz in sorted(around, key=lambda offset: (abs(offset[0]), abs(offset[2]) if stage_of(*offset) < 3 else -abs(offset[2]))):
            if stage_of(dx, dy, dz) not in hops or (dz == 0) not in flat:
                continue
            slot = slot_of(dx, dy, dz)
            size, width = (rows, rad) if dz == 0 else (pack_rows, pack_rad)
            source = own if dz == 0 else pack
            target = (from_right, ext, from_left)[dz + 1]
            pairs = (
                (weight.at[13], weight.at[slot_of(-dx, -dy if first_y else abs(dy), -dz)]),
                (
                    source.at[cut(dx, size, width), cut(dy, cols, rad), :],
                    target.at[wide(-dx, size, width), wide_cols(-dy), :],
                ),
            )
            sems = ((weight_send, weight_recv), (out_send, far_recv if dx else out_recv))
            copy = pltpu.make_async_remote_copy(
                src_ref=pairs[what][0],
                dst_ref=pairs[what][1],
                send_sem=sems[what][0],
                recv_sem=sems[what][1],
                device_id=device(dx, dy, dz),
                device_id_type=MESH,
            )
            yield exists(dx, dy, dz), [copy]

    def back_copies(flat):
        for dx, dy, dz in sorted(around, key=lambda offset: -sum(map(abs, offset))):
            if (dz == 0) != flat:
                continue
            size, width = (rows, rad) if dz == 0 else (pack_rows, pack_rad)
            source = total if dz == 0 else back_pack
            target = (back_right, back_xy, back_left)[dz + 1]
            copy = pltpu.make_async_remote_copy(
                src_ref=source.at[wide(dx, size, width), wide_cols(dy), :],
                dst_ref=target.at[wide(-dx, size, width), wide_cols(-dy), :],
                send_sem=back_send,
                recv_sem=back_recv,
                device_id=device(dx, dy, dz),
                device_id_type=MESH,
            )
            yield exists(dx, dy, dz), [copy]

    def start(family):
        for sends, copies in family:

            @pl.when(sends)
            def _():
                for copy in copies:
                    copy.start()

    def drain(semaphore, amount):
        bytes_of = marks.at[pl.ds(0, amount)]
        pltpu.make_async_remote_copy(
            src_ref=bytes_of,
            dst_ref=bytes_of,
            send_sem=semaphore,
            recv_sem=semaphore,
            device_id=partner(*ring_all[0]),
            device_id_type=MESH,
        ).wait_recv()

    def drain_all(semaphore, sides=(0, 1), rows_only=False):
        counts_of = [
            (min(count - 1, 2), (me > 0).astype(jnp.int32) + (me < count - 1).astype(jnp.int32))
            for me, count in ((me_x, n_x), (me_y, n_y), (me_z, n_z))
        ]
        for c_x in range(min(1, n_x - 1), counts_of[0][0] + 1):
            for c_y in range(min(1, n_y - 1), counts_of[1][0] + 1):
                for c_z in range(min(1, n_z - 1), counts_of[2][0] + 1):
                    amount = 0
                    for dx, dy, dz in ((i, j, k) for i in (0, 1) for j in (0, 1) for k in (0, 1)):
                        if (dx, dy, dz) == (0, 0, 0) or dx not in sides:
                            continue
                        size, width = (rows, rad) if dz == 0 else (pack_rows, pack_rad)
                        message = 1 if rows_only else (width if dx else size) * (rad if dy else cols)
                        amount += (c_x if dx else 1) * (c_y if dy else 1) * (c_z if dz else 1) * message

                    if not amount:
                        continue

                    @pl.when((counts_of[0][1] == c_x) & (counts_of[1][1] == c_y) & (counts_of[2][1] == c_z))
                    def _():
                        drain(semaphore, amount)

    def iota(shape, dim):
        return lax.broadcasted_iota(jnp.int32, shape, dim)

    span = 2 * rad
    block = lanes // (cols + 2 * rad)
    part_rows = block * wide_y

    def stack(*parts):
        return jnp.concatenate(parts, axis=0)

    def beside(*parts):
        return jnp.concatenate(parts, axis=1)

    def build(p, carry):
        for j in range(2):
            v = 2 * p + j

            def summed(dim):
                values = [taps_ref[dim, v, k] for k in range(length)]
                while len(values) > 1:
                    values = [sum(values[i : i + 2]) for i in range(0, len(values), 2)]
                return jnp.full((8, lanes), values[0], F32)

            inverse = 1.0 / (summed(0) * summed(1) * summed(2))

            def chosen(offset, dim):
                result = jnp.zeros(offset.shape, F32)
                for k in range(length):
                    result = jnp.where(offset == k, taps_ref[dim, v, k], result)
                return result

            def scaled(part):
                return (part.reshape(-1, 8, lanes) * inverse[None]).reshape(part.shape)

            here = slice(j * lanes, (j + 1) * lanes)
            square = (lanes, lanes)
            main = scaled(chosen(iota(square, 0) - iota(square, 1) + rad, 2))
            row, col = iota((span, lanes), 0), iota((span, lanes), 1)
            edges = scaled(chosen(jnp.where(row < rad, row, row + lanes) - col, 2))
            high, low = split(main)
            ahead_a[p, :, here] = stack(high, high)
            ahead_b[p, :lanes, here] = low
            high, low = split(edges)
            ahead_b[p, lanes:, here] = stack(high, high, low, jnp.zeros((lanes - 3 * span, lanes), BF16))
            high, low = split(main.T)
            astern[v] = stack(beside(high, low), beside(high, jnp.zeros(square, BF16)))
            turned = jnp.where(iota(square, 1) // span == v, stack(*[edges] * views).T, 0.0)
            high, low = split(turned)
            astern_edge[v] = stack(beside(high, low), beside(high, jnp.zeros(square, BF16)))
            shape = (block * cols, lanes)
            row, col = iota(shape, 0), iota(shape, 1)
            offset = jnp.where(row // cols == col // wide_y, place_y(col % wide_y) + rad - row % cols, -1)
            blur_y = chosen(offset, 1)
            high, low = split(blur_y)
            high, low = high[:, :part_rows], low[:, :part_rows]
            gath[v] = stack(beside(high, high), beside(low, jnp.zeros(low.shape, BF16)))
            turned = blur_y.T[:part_rows]
            high = turned.astype(BF16).astype(F32)
            low = turned - high
            scat[v] = beside(high, high, low).astype(BF16)
        return carry

    def lines_of(dim):
        lane = iota((1, lanes), 1)
        lines = []
        for k in range(length):
            line = jnp.zeros((1, lanes), F32)
            for v in range(views):
                line = jnp.where(lane // span == v, taps_ref[dim, v, k], line)
            lines.append(line)
        return lines

    meet(0)
    start(out_copies((1,), 1, (True,)))
    lane = lax.broadcasted_iota(jnp.int32, (cols, lanes), 1)
    for g in range(rows // 8):
        merged = jnp.zeros((cols, lanes), F32)
        for i in range(8):
            rolled = pltpu.roll(ext[rad + 8 * g + i, own_y, :], 2 * rad * i + rad, 1)
            merged = jnp.where(lane // (2 * rad) == i, rolled, merged)
        pack[g] = merged

    start(out_copies((1,), 0))
    start(out_copies((1,), 1, (False,)))
    loads[2].wait()
    stops = [min(stop, views // 2) for stop in (0, 1, 2, views // 2)]
    for hop in range(1, 4):
        lax.fori_loop(stops[hop - 1], stops[hop], build, 0)
        if hop < min(3, early_rounds):
            meet(hop)
        if hop in (1, 2):
            start(out_copies((hop + 1,), 0))
            start(out_copies((hop + 1,), 1))

    for k, line in enumerate(lines_of(0)):
        taps_x[k : k + 1] = line
    shape = (wide_y, lanes)
    offset = place_y(iota(shape, 0)) + rad - iota(shape, 1) % cols
    base = jnp.zeros(shape, F32)
    for k, line in enumerate(lines_of(1)):
        base = jnp.where(offset == k, line, base)
    high = base.astype(BF16).astype(F32)
    scat_edge[...] = beside(high, high, base - high)

    loads[3].wait()
    def weight_of(rows_of, v):
        first = v * (lanes // views)
        return jnp.broadcast_to(rows_of[:, first : first + 1], rows_of.shape)

    mine = jnp.broadcast_to(weight[13], (8, lanes))
    count = jnp.zeros((8, lanes), F32)
    seen = jnp.zeros((8, lanes), F32)
    for v in range(views):
        weight_v = weight_of(mine, v)
        count = count + weight_v
        seen = seen + weight_v * jnp.sum(obs[v].reshape(-1, 8, lanes), axis=0)
    count = count[0:1]
    wanted = jnp.sum(seen, axis=0, keepdims=True) / count

    def side_of(g):
        return 0 if 8 * g < rad else (1 if 8 * g < rad + rows else 2)

    inner = [g for g in range(groups) if side_of(g) == 1]
    outer = [g for g in range(groups) if side_of(g) != 1]
    place = {g: which for which, g in enumerate(inner + outer)}
    size = 8 * wide_y
    inner_rows, outer_rows = slice(0, size * len(inner)), slice(size * len(inner), size * groups)

    def prepare(chosen_groups):
        lane = iota((wide_y, lanes), 1)
        for g in chosen_groups:
            here = slice(size * place[g], size * (place[g] + 1))
            high, low = split(ext[8 * g : 8 * g + 8].reshape(size, lanes))
            wide_a[here, :lanes] = high
            wide_a[here, lanes:] = low
            wide_b[here, :lanes] = high
            merged = jnp.where(lane % span < rad, from_left[g], from_right[g])
            edge[g] = merged
            high = merged.astype(BF16).astype(F32)
            low = merged - high
            count_of = lanes // span
            highs = [pltpu.roll(high, span * i, 1) if i else high for i in range(count_of)]
            lows = [pltpu.roll(low, span * i, 1) if i else low for i in range(count_of)]
            rows_of = []
            for i in range(8):
                third = jnp.where(lane < 2 * span, lows[(1 - i) % count_of], highs[(2 - i) % count_of])
                terms = jnp.where(lane < span, highs[-i % count_of], third)
                rows_of.append(terms)
            wide_b[here, lanes:] = stack(*rows_of).astype(BF16)

    def weighed(terms):
        result = None
        for factor, value in terms:
            term = factor * value
            result = term if result is None else result + term
        return result

    def added(one, two):
        if one is None or two is None:
            return two if one is None else one
        return one + two

    def blur_x(source, tap):
        taps = [tap(k) for k in range(length)]
        even, odd = taps[0::2], [None] + taps[1::2]
        both = [added(one, two) for one, two in zip(even, odd)]
        reach, columns = len(even), []
        for first in range(0, cols, 8):
            values = [source[e, first : first + 8, :] for e in range(wide_x)]
            left, right = values[0::2], values[1::2]
            joined = [one + two for one, two in zip(left, right)]
            lines, before = [], weighed([(odd[j], right[j - 1]) for j in range(1, reach)])
            for m in range(rows // 2):
                one = weighed([(even[j], left[m + j]) for j in range(reach)])
                two = weighed([(odd[j], right[m + j]) for j in range(1, reach)])
                three = weighed([(both[j], joined[m + j]) for j in range(reach)])
                lines += [one + before, three - (one + two)]
                before = two
            columns.append(lines)
        return [stack(*parts) for parts in zip(*columns)]

    def spread_x(source, tap):
        taps = [tap(k) for k in range(length)]
        even, odd = taps[0::2], taps[1::2] + [None]
        both = [added(one, two) for one, two in zip(even, odd)]
        columns = []
        for first in range(0, cols, 8):
            values = [source[a, first : first + 8, :] for a in range(rows)]
            left, right = values[0::2], values[1::2]
            joined = [one + two for one, two in zip(left, right)]

            def product(factors, parts, n):
                pairs = [(factors[n - i], parts[i]) for i in range(len(parts)) if 0 <= n - i < len(factors)]
                return weighed([pair for pair in pairs if pair[0] is not None])

            lines, before = [], None
            for n in range(wide_x // 2):
                one, two = product(even, left, n), product(odd, right, n)
                three = product(both, joined, n)
                lines += [added(one, before), three - added(one, two)]
                before = two
            columns.append(lines)
        return [stack(*parts) for parts in zip(*columns)]

    def pairs_of(part, half):
        return beside(part[:half], part[half:])

    def blur_zy(p, chosen_groups, row_range, slot):
        blurred[slot, row_range] = dot(wide_a[row_range, :], ahead_a[p]) + dot(wide_b[row_range, :], ahead_b[p])
        for j in range(2):
            v = 2 * p + j
            for g in chosen_groups:
                first = size * place[g]
                high, low = split(blurred[slot, first : first + size, j * lanes : (j + 1) * lanes])
                line = dot(gath[v], stack(pairs_of(high, size // 2), pairs_of(low, size // 2)))
                half = block * cols
                line = line[:half] + line[half:]
                for which in range(2):
                    first = 8 * g + which * block
                    part = line[:, which * lanes : (which + 1) * lanes]
                    lined[v, first : first + block] = part.reshape(block, cols, lanes)

    drain_all(out_recv, sides=(0,))
    if early_rounds > 3:
        meet(3)
    prepare(inner)

    for p in range(views // 2):
        blur_zy(p, inner, inner_rows, p)

    for hop in range(4, early_rounds):
        meet(hop)
    drain_all(weight_recv, rows_only=True)
    everyone = stack(*[weight[slot] for slot in range(27)], jnp.zeros((5, lanes), F32))
    counts = jnp.zeros(everyone.shape, F32)

    def along_y(rows_of, first):
        return stack(*[jnp.broadcast_to(rows_of[first + dy : first + dy + 1], (size_y, lanes)) for _, size_y, dy in bands_y])

    for v in range(views):
        theirs = weight_of(everyone, v)
        counts = counts + theirs
        for dx in range(3):
            mask[v, dx] = stack(*[along_y(theirs, 9 + 3 * dx)] * block).astype(BF16)
    for dx in range(3):
        terms = []
        for side in range(2):
            part = along_y(everyone, 18 * side + 3 * dx)
            terms.append(scat_edge[...] * beside(part, part, part))
        mask_edge[dx] = stack(*terms).astype(BF16)
    inverses[...] = jnp.where(counts > 0.0, 1.0 / jnp.maximum(counts, 1.0), 0.0)

    drain_all(far_recv, sides=(1,))
    if early_rounds < rounds:
        greet(early_rounds)
    prepare(outer)

    def two_views(p, slot):
        blur_zy(p, outer, outer_rows, slot)
        scattered = []
        for j in range(2):
            v = 2 * p + j
            blur = blur_x(lined.at[v], lambda k: taps_ref[0, v, k])
            ratio = obs[v].reshape(rows * cols, lanes) / stack(*blur)
            ratio = beside(*split(ratio))
            back = folded(dot(ratio, astern[v]))
            fringe[...] += dot(ratio, astern_edge[v])
            spread[2 * slot + j] = back.reshape(rows, cols, lanes)
            pieces = spread_x(spread.at[2 * slot + j], lambda k: taps_ref[0, v, k])
            sent = []
            for g in range(groups):
                high, low = split(stack(*pieces[8 * g : 8 * g + 8]))
                high, low = (pairs_of(part, block * cols) for part in (high, low))
                sent.append(stack(high, low, high))
            scattered.append(sent)
        for g in range(groups):
            dx = side_of(g)
            reach = None
            for j in range(2):
                v = 2 * p + j
                here = mask[v, dx]
                here = scat[v] * beside(here, here)[:, : scat.shape[2]]
                part = dot(here, scattered[j][g])
                reach = part if reach is None else reach + part
            for which in range(2):
                first = 8 * g + which * block
                part = reach[:, which * lanes : (which + 1) * lanes]
                total[first : first + block] += part.reshape(block, wide_y, lanes)

    for p in range(views // 2):
        two_views(p, p)
    for hop in range(early_rounds, rounds):
        meet(hop)
    start(back_copies(True))
    def sums_a():
        for slot, offset in enumerate(ring_a):
            yield pltpu.make_async_remote_copy(
                src_ref=stat,
                dst_ref=stat_a.at[slot],
                send_sem=a_send,
                recv_sem=a_recv,
                device_id=partner(*offset),
                device_id_type=MESH,
            )

    def sums_b():
        for slot, offset in enumerate(ring_b):
            yield pltpu.make_async_remote_copy(
                src_ref=part_a,
                dst_ref=stat_b.at[slot],
                send_sem=b_send,
                recv_sem=b_recv,
                device_id=partner(*offset),
                device_id_type=MESH,
            )

    spread[0] = folded(fringe[...]).reshape(rows, cols, lanes)
    pieces = spread_x(spread.at[0], lambda k: taps_x[k : k + 1])
    lane = iota((cols, lanes), 1)
    for g in range(groups):
        turned = pieces[8 * g : 8 * g + 8]
        step = views // 2
        while step:
            low_half = (lane // span) // step % 2 == 0
            for i in range(views):
                if i // step % 2 == 0:
                    one, two = turned[i], turned[i + step]
                    turned[i] = jnp.where(low_half, one, pltpu.roll(two, step * span, 1))
                    turned[i + step] = jnp.where(low_half, pltpu.roll(one, lanes - step * span, 1), two)
            step //= 2
        high, low = split(stack(*turned))
        sides = dot(mask_edge[side_of(g)], stack(high, low, high))
        back_pack[g] = jnp.where(iota((wide_y, lanes), 1) % span < rad, sides[:wide_y], sides[wide_y:])
    lane = iota((wide_y, lanes), 1)
    seen = jnp.zeros((8, lanes), F32)
    for dx in range(3):
        for start_y, size_y, dy in bands_y:
            first_x, last_x = ((0, rad), (rad, rad + rows), (rad + rows, wide_x))[dx]
            part_y = slice(start_y, start_y + size_y)
            part = total[first_x:last_x, part_y, :] * ext[first_x:last_x, part_y, :]
            part = jnp.sum(part.reshape(-1, 8, lanes), axis=0)
            slot = 9 + 3 * dx + dy
            seen = seen + part * inverses[slot : slot + 1, :]
            part_x = slice(first_x // 8, last_x // 8)
            part = back_pack[part_x, part_y, :] * edge[part_x, part_y, :]
            part = jnp.sum(part.reshape(-1, 8, lanes), axis=0)
            left, right = (inverses[at : at + 1, :] for at in (slot - 9, slot + 9))
            seen = seen + part * jnp.where(lane[0:1] % (2 * rad) < rad, left, right)
    wanted = wanted + pltpu.roll(wanted, lanes // 2, 1)
    gotten = jnp.sum(seen, axis=0, keepdims=True)
    gotten = gotten + pltpu.roll(gotten, lanes // 2, 1)
    stat[...] = jnp.where(iota((1, lanes), 1) < lanes // 2, wanted, gotten)

    for copy in sums_a():
        copy.start()
    start(back_copies(False))
    drain_all(back_recv)
    near = back_xy[...]

    def fold(values, size, rad, axis):
        low = lax.slice_in_dim(values, 0, rad, axis=axis)
        mid = lax.slice_in_dim(values, rad, rad + size, axis=axis)
        top = lax.slice_in_dim(values, rad + size, 2 * rad + size, axis=axis)
        if size == 2 * rad:
            return mid + jnp.concatenate([low, top], axis=axis)
        gap_shape = list(low.shape)
        gap_shape[axis] = size - rad
        gap = jnp.zeros(gap_shape, F32)
        return mid + jnp.concatenate([low, gap], axis=axis) + jnp.concatenate([gap, top], axis=axis)

    def fold_y(values):
        if first_y:
            return fold(values, cols, rad, 1)
        part = values[:, cols:]
        gap = jnp.zeros((part.shape[0], cols - rad, lanes), F32)
        before, after = (jnp.concatenate(pair, axis=1) for pair in ((part, gap), (gap, part)))
        return values[:, :cols] + jnp.where(me_y == 0, after, before)

    near = fold_y(fold(near, rows, rad, 0))
    ends = jnp.where((lane % (2 * rad) < rad)[None], back_right[...], back_left[...])
    ends = fold_y(fold(ends, pack_rows, pack_rad, 0))
    lane = lax.broadcasted_iota(jnp.int32, (cols, lanes), 1)
    outer = (lane < rad) | (lane >= lanes - rad)
    for x in range(rows):
        rolled = pltpu.roll(ends[x // 8], lanes - (2 * rad * (x % 8) + rad), 1)
        summed = total[rad + x, own_y, :] + near[x] + jnp.where(outer, rolled, 0.0)
        updated = ext[rad + x, own_y, :] * (summed / count)
        out_ref[x] = updated

    drain(a_recv, len(ring_a))
    everything = stat[...] + jnp.sum(stat_a[...], axis=0)
    if ring_b:
        part_a[...] = everything
        for copy in sums_b():
            copy.start()
        drain(b_recv, len(ring_b))
        everything = part_a[...] + jnp.sum(stat_b[...], axis=0)
    first_half = iota((1, lanes), 1) < lanes // 2
    wanted = jnp.sum(jnp.where(first_half, everything, 0.0), axis=1, keepdims=True)
    gotten = jnp.sum(jnp.where(first_half, 0.0, everything), axis=1, keepdims=True)
    factor = jnp.broadcast_to(wanted, (1, lanes)) / jnp.broadcast_to(gotten, (1, lanes))
    factor_ref[...] = factor

    drain_all(out_send)
    drain_all(weight_send, rows_only=True)
    drain_all(back_send)
    drain(a_send, len(ring_a))
    if ring_b:
        drain(b_send, len(ring_b))


def on_device(sizes, estimate, observed, coverage, psf_taps):
    rows, cols, lanes = estimate.shape
    views = observed.shape[0]
    rad = (psf_taps.shape[2] - 1) // 2
    wide_x, wide_y = rows + 2 * rad, extent_y(sizes[1], cols, rad)
    groups, block = wide_x // 8, lanes // (cols + 2 * rad)
    _, ring_a, ring_b = rings(sizes)
    n_a, n_b = len(ring_a), max(1, len(ring_b))

    def vm(*shape, dtype=F32):
        return pltpu.VMEM(shape, dtype)

    def dma(*shape):
        return pltpu.SemaphoreType.DMA(shape)

    def in_hbm(values):
        return pltpu.with_memory_space_constraint(values, pltpu.HBM)

    views_all, dims, length = psf_taps.shape
    scratch = [
        pltpu.SMEM((dims, views_all, length), F32),
        pltpu.SMEM((views,), jnp.int32),
        vm(*observed.shape),
        vm(wide_x, wide_y, lanes),
        vm(wide_x * wide_y, 2 * lanes, dtype=BF16),
        vm(wide_x * wide_y, 2 * lanes, dtype=BF16),
        vm(rows // 8, cols, lanes),
        vm(groups, wide_y, lanes),
        vm(groups, wide_y, lanes),
        vm(groups, wide_y, lanes),
        vm(27, 1, lanes),
        vm(32, lanes),
        vm(views, 3, block * wide_y, lanes, dtype=BF16),
        vm(3, 2 * wide_y, 3 * lanes, dtype=BF16),
        vm(views // 2, 2 * lanes, 2 * lanes, dtype=BF16),
        vm(views // 2, 2 * lanes, 2 * lanes, dtype=BF16),
        vm(views, 2 * block * cols, 2 * block * wide_y, dtype=BF16),
        vm(views, block * wide_y, 3 * block * cols, dtype=BF16),
        vm(views, 2 * lanes, 2 * lanes, dtype=BF16),
        vm(views, 2 * lanes, 2 * lanes, dtype=BF16),
        vm(24, lanes),
        vm(wide_y, 3 * lanes),
        vm(views // 2, wide_x * wide_y, 2 * lanes),
        vm(views, wide_x, cols, lanes),
        vm(views, rows, cols, lanes),
        vm(rows * cols, 2 * lanes),
        vm(wide_x, wide_y, lanes),
        vm(groups, wide_y, lanes),
        vm(groups, wide_y, lanes),
        vm(groups, wide_y, lanes),
        vm(wide_x, wide_y, lanes),
        vm(1, lanes),
        vm(n_a, 1, lanes),
        vm(n_b, 1, lanes),
        vm(1, lanes),
        vm(5 * rows * cols, 1, lanes),
        dma(4),
        pltpu.SemaphoreType.REGULAR((max(1, min(EARLY, sum(sizes) - 3) + late_rounds(sizes)),)),
        *[pltpu.SemaphoreType.DMA] * 11,
    ]
    updated, factor = pl.pallas_call(
        functools.partial(kernel, sizes),
        out_shape=(jax.ShapeDtypeStruct(estimate.shape, F32), jax.ShapeDtypeStruct((1, lanes), F32)),
        in_specs=[
            pl.BlockSpec(memory_space=pl.ANY),
            pl.BlockSpec(memory_space=pl.ANY),
            pl.BlockSpec(memory_space=pl.ANY),
            pl.BlockSpec(memory_space=pl.ANY),
        ],
        out_specs=(pl.BlockSpec(memory_space=pltpu.VMEM), pl.BlockSpec(memory_space=pltpu.VMEM)),
        scratch_shapes=scratch,
        compiler_params=pltpu.CompilerParams(collective_id=0, has_side_effects=True, vmem_limit_bytes=40 * 1024 * 1024),
    )(*map(in_hbm, (jnp.transpose(psf_taps, (1, 0, 2)), coverage.reshape(views), estimate, observed)))
    return updated * factor.reshape(1, 1, lanes)


def solution(mesh):
    sizes = tuple(mesh.shape[axis] for axis in ("bx", "by", "bz"))
    return jax.shard_map(
        functools.partial(on_device, sizes),
        mesh=mesh,
        in_specs=(P("bx", "by", "bz"), P(None, "bx", "by", "bz"), P(None, "bx", "by", "bz"), P()),
        out_specs=P("bx", "by", "bz"),
        check_vma=False,
    )
```

```python
import functools

import jax
import jax.numpy as jnp
from jax import lax
from jax.experimental import pallas as pl
from jax.experimental.pallas import tpu as pltpu
from jax.sharding import PartitionSpec as P

F32 = jnp.float32
BF16 = jnp.bfloat16
MESH = pl.DeviceIdType.MESH


def split(values):
    high = values.astype(BF16)
    low = (values - high.astype(F32)).astype(BF16)
    return high, low


def dot(left, right, dims=((1,), (0,))):
    return lax.dot_general(left, right, (dims, ((), ())), preferred_element_type=F32)


def folded(values):
    half = values.shape[1] // 2
    return values[:, :half] + values[:, half:]


def rings(sizes):
    offsets = [(i, j, k) for i in range(sizes[0]) for j in range(sizes[1]) for k in range(sizes[2])]
    offsets = offsets[1:]
    if len(offsets) < 64:
        return offsets, offsets, []
    return (
        offsets,
        [offset for offset in offsets if offset[0] == 0],
        [offset for offset in offsets if offset[1:] == (0, 0)],
    )


EARLY = 5


def stage_of(dx, dy, dz):
    return 3 if dx and dy else abs(dx) + abs(dy) + abs(dz)


def late_rounds(sizes):
    steps = (-1, 0, 1)
    near = [(i, j, k) for i in steps for j in steps for k in steps if (i, j, k) != (0, 0, 0)]
    everyone = [(i, j, k) for i in range(sizes[0]) for j in range(sizes[1]) for k in range(sizes[2])]
    known = {at: {at} for at in everyone}

    def beyond(at, offset):
        return tuple(a + b for a, b in zip(at, offset))

    def heard(sets, stages):
        return {
            at: set().union(
                sets[-1][at],
                *[
                    sets[min(stage_of(*offset), len(sets) - 1)].get(beyond(at, offset), set())
                    for offset in near
                    if stage_of(*offset) in stages
                ],
            )
            for at in everyone
        }

    history = [known]
    for _ in range(min(EARLY, sum(sizes) - 3)):
        history.append(heard([history[-1]] * 4, (1,)))
    now, rounds = heard(history, (1, 2, 3)), 0
    while any(len(now[at]) < len(everyone) for at in everyone):
        now, rounds = heard([now] * 4, (1,)), rounds + 1
    return rounds


def extent_y(n_y, cols, rad):
    return cols + (rad if n_y == 2 else 2 * rad)


def kernel(
    sizes,
    taps_hbm,
    cover_hbm,
    est_hbm,
    obs_hbm,
    out_ref,
    factor_ref,
    taps_ref,
    cover_ref,
    obs,
    ext,
    wide_a,
    wide_b,
    pack,
    from_left,
    from_right,
    edge,
    weight,
    inverses,
    mask,
    mask_edge,
    ahead_a,
    ahead_b,
    gath,
    scat,
    astern,
    astern_edge,
    taps_x,
    scat_edge,
    blurred,
    lined,
    spread,
    fringe,
    total,
    back_pack,
    back_left,
    back_right,
    back_xy,
    stat,
    stat_a,
    stat_b,
    part_a,
    marks,
    fetch_sem,
    hop_sem,
    out_send,
    out_recv,
    far_recv,
    weight_send,
    weight_recv,
    back_send,
    back_recv,
    a_send,
    a_recv,
    b_send,
    b_recv,
):
    n_x, n_y, n_z = sizes
    views, rows, cols, lanes = obs.shape
    length = taps_ref.shape[2]
    rad = (length - 1) // 2
    wide_x, wide_y = rows + 2 * rad, extent_y(n_y, cols, rad)
    groups = wide_x // 8
    first_y = wide_y - cols - rad
    bands_y = [(first_y, cols, 1), (first_y + cols, rad, 2)]
    if first_y:
        bands_y.insert(0, (0, rad, 0))
    me_x, me_y, me_z = lax.axis_index("bx"), lax.axis_index("by"), lax.axis_index("bz")

    own_x, own_y = slice(rad, rad + rows), slice(first_y, first_y + cols)
    own = ext.at[own_x, own_y, :]
    loads = [
        pltpu.make_async_copy(source, target, fetch_sem.at[which])
        for which, (source, target) in enumerate(
            ((est_hbm, own), (cover_hbm, cover_ref), (taps_hbm, taps_ref), (obs_hbm, obs))
        )
    ]
    for load in loads:
        load.start()

    def exists(dx, dy, dz):
        ok = None
        for step, me, count in ((dx, me_x, n_x), (dy, me_y, n_y), (dz, me_z, n_z)):
            if step == 0:
                continue
            inside = (me + step >= 0) & (me + step < count)
            ok = inside if ok is None else ok & inside
        return ok

    def device(dx, dy, dz):
        return {"bx": me_x + dx, "by": me_y + dy, "bz": me_z + dz}

    steps = (-1, 0, 1)
    around = [(dx, dy, dz) for dz in steps for dx in steps for dy in steps if (dx, dy, dz) != (0, 0, 0)]
    ring_all, ring_a, ring_b = rings(sizes)

    def partner(i, j, k):
        return {
            "bx": lax.rem(me_x + i, n_x),
            "by": lax.rem(me_y + j, n_y),
            "bz": lax.rem(me_z + k, n_z),
        }

    for part in ((slice(0, rad), slice(0, wide_y)), (slice(rad + rows, wide_x), slice(0, wide_y))):
        ext[part[0], part[1], :] = jnp.zeros((rad, wide_y, lanes), F32)
    for start_y, size_y, dy in bands_y:
        if dy != 1:
            ext[own_x, start_y : start_y + size_y, :] = jnp.zeros((rows, size_y, lanes), F32)
    from_left[...] = jnp.zeros(from_left.shape, F32)
    from_right[...] = jnp.zeros(from_right.shape, F32)
    weight[...] = jnp.zeros(weight.shape, F32)

    barrier = pltpu.get_barrier_semaphore()
    faces = [offset for offset in around if sum(map(abs, offset)) == 1]
    near_by = sum(exists(*offset).astype(jnp.int32) for offset in faces)
    early_rounds = min(EARLY, n_x + n_y + n_z - 3)
    rounds = early_rounds + late_rounds(sizes)

    def greet(which):
        semaphore = barrier if which == 0 else hop_sem.at[which - 1]
        for offset in faces:

            @pl.when(exists(*offset))
            def _():
                pl.semaphore_signal(semaphore, inc=1, device_id=device(*offset), device_id_type=MESH)

    def meet(which):
        pl.semaphore_wait(barrier if which == 0 else hop_sem.at[which - 1], near_by)
        if which + 1 < rounds and which + 1 != early_rounds:
            greet(which + 1)

    greet(0)

    back_xy[...] = jnp.zeros(back_xy.shape, F32)
    back_left[...] = jnp.zeros(back_left.shape, F32)
    back_right[...] = jnp.zeros(back_right.shape, F32)
    total[...] = jnp.zeros(total.shape, F32)
    fringe[...] = jnp.zeros(fringe.shape, F32)

    loads[1].wait()
    lane = lax.broadcasted_iota(jnp.int32, (1, lanes), 1)
    row = jnp.zeros((1, lanes), F32)
    for v in range(views):
        mine = jnp.full((1, lanes), cover_ref[v], jnp.int32).astype(F32)
        row = jnp.where(lane // (lanes // views) == v, mine, row)
    weight[13] = row
    loads[0].wait()

    def cut(step, size, width):
        return pl.ds(0, size) if step == 0 else pl.ds(0 if step < 0 else size - width, width)

    def wide(step, size, width):
        return pl.ds(width, size) if step == 0 else pl.ds(0 if step < 0 else width + size, width)

    def wide_cols(step):
        if step == 0:
            return pl.ds(first_y, cols)
        return pl.ds(0 if step < 0 and first_y else first_y + cols, rad)

    def place_y(row):
        return row - first_y if first_y else jnp.where(row < cols, row, row - me_y * wide_y)

    pack_rows, pack_rad = rows // 8, rad // 8

    def slot_of(dx, dy, dz):
        return 9 * (dz + 1) + 3 * (dx + 1) + dy + 1

    def out_copies(hops, what, flat=(True, False)):
        for dx, dy, dz in sorted(around, key=lambda offset: (abs(offset[0]), abs(offset[2]) if stage_of(*offset) < 3 else -abs(offset[2]))):
            if stage_of(dx, dy, dz) not in hops or (dz == 0) not in flat:
                continue
            slot = slot_of(dx, dy, dz)
            size, width = (rows, rad) if dz == 0 else (pack_rows, pack_rad)
            source = own if dz == 0 else pack
            target = (from_right, ext, from_left)[dz + 1]
            pairs = (
                (weight.at[13], weight.at[slot_of(-dx, -dy if first_y else abs(dy), -dz)]),
                (
                    source.at[cut(dx, size, width), cut(dy, cols, rad), :],
                    target.at[wide(-dx, size, width), wide_cols(-dy), :],
                ),
            )
            sems = ((weight_send, weight_recv), (out_send, far_recv if dx else out_recv))
            copy = pltpu.make_async_remote_copy(
                src_ref=pairs[what][0],
                dst_ref=pairs[what][1],
                send_sem=sems[what][0],
                recv_sem=sems[what][1],
                device_id=device(dx, dy, dz),
                device_id_type=MESH,
            )
            yield exists(dx, dy, dz), [copy]

    def back_copies(flat):
        for dx, dy, dz in sorted(around, key=lambda offset: -sum(map(abs, offset))):
            if (dz == 0) != flat:
                continue
            size, width = (rows, rad) if dz == 0 else (pack_rows, pack_rad)
            source = total if dz == 0 else back_pack
            target = (back_right, back_xy, back_left)[dz + 1]
            copy = pltpu.make_async_remote_copy(
                src_ref=source.at[wide(dx, size, width), wide_cols(dy), :],
                dst_ref=target.at[wide(-dx, size, width), wide_cols(-dy), :],
                send_sem=back_send,
                recv_sem=back_recv,
                device_id=device(dx, dy, dz),
                device_id_type=MESH,
            )
            yield exists(dx, dy, dz), [copy]

    def start(family):
        for sends, copies in family:

            @pl.when(sends)
            def _():
                for copy in copies:
                    copy.start()

    def drain(semaphore, amount):
        bytes_of = marks.at[pl.ds(0, amount)]
        pltpu.make_async_remote_copy(
            src_ref=bytes_of,
            dst_ref=bytes_of,
            send_sem=semaphore,
            recv_sem=semaphore,
            device_id=partner(*ring_all[0]),
            device_id_type=MESH,
        ).wait_recv()

    def drain_all(semaphore, sides=(0, 1), rows_only=False):
        counts_of = [
            (min(count - 1, 2), (me > 0).astype(jnp.int32) + (me < count - 1).astype(jnp.int32))
            for me, count in ((me_x, n_x), (me_y, n_y), (me_z, n_z))
        ]
        for c_x in range(min(1, n_x - 1), counts_of[0][0] + 1):
            for c_y in range(min(1, n_y - 1), counts_of[1][0] + 1):
                for c_z in range(min(1, n_z - 1), counts_of[2][0] + 1):
                    amount = 0
                    for dx, dy, dz in ((i, j, k) for i in (0, 1) for j in (0, 1) for k in (0, 1)):
                        if (dx, dy, dz) == (0, 0, 0) or dx not in sides:
                            continue
                        size, width = (rows, rad) if dz == 0 else (pack_rows, pack_rad)
                        message = 1 if rows_only else (width if dx else size) * (rad if dy else cols)
                        amount += (c_x if dx else 1) * (c_y if dy else 1) * (c_z if dz else 1) * message

                    if not amount:
                        continue

                    @pl.when((counts_of[0][1] == c_x) & (counts_of[1][1] == c_y) & (counts_of[2][1] == c_z))
                    def _():
                        drain(semaphore, amount)

    def iota(shape, dim):
        return lax.broadcasted_iota(jnp.int32, shape, dim)

    span = 2 * rad
    block = lanes // (cols + 2 * rad)
    part_rows = block * wide_y

    def stack(*parts):
        return jnp.concatenate(parts, axis=0)

    def beside(*parts):
        return jnp.concatenate(parts, axis=1)

    def build(p, carry):
        for j in range(2):
            v = 2 * p + j

            def summed(dim):
                values = [taps_ref[dim, v, k] for k in range(length)]
                while len(values) > 1:
                    values = [sum(values[i : i + 2]) for i in range(0, len(values), 2)]
                return jnp.full((8, lanes), values[0], F32)

            inverse = 1.0 / (summed(0) * summed(1) * summed(2))

            def chosen(offset, dim):
                result = jnp.zeros(offset.shape, F32)
                for k in range(length):
                    result = jnp.where(offset == k, taps_ref[dim, v, k], result)
                return result

            def scaled(part):
                return (part.reshape(-1, 8, lanes) * inverse[None]).reshape(part.shape)

            here = slice(j * lanes, (j + 1) * lanes)
            square = (lanes, lanes)
            main = scaled(chosen(iota(square, 0) - iota(square, 1) + rad, 2))
            row, col = iota((span, lanes), 0), iota((span, lanes), 1)
            edges = scaled(chosen(jnp.where(row < rad, row, row + lanes) - col, 2))
            high, low = split(main)
            ahead_a[p, :, here] = stack(high, high)
            ahead_b[p, :lanes, here] = low
            high, low = split(edges)
            ahead_b[p, lanes:, here] = stack(high, high, low, jnp.zeros((lanes - 3 * span, lanes), BF16))
            high, low = split(main.T)
            astern[v] = stack(beside(high, low), beside(high, jnp.zeros(square, BF16)))
            turned = jnp.where(iota(square, 1) // span == v, stack(*[edges] * views).T, 0.0)
            high, low = split(turned)
            astern_edge[v] = stack(beside(high, low), beside(high, jnp.zeros(square, BF16)))
            shape = (block * cols, lanes)
            row, col = iota(shape, 0), iota(shape, 1)
            offset = jnp.where(row // cols == col // wide_y, place_y(col % wide_y) + rad - row % cols, -1)
            blur_y = chosen(offset, 1)
            high, low = split(blur_y)
            high, low = high[:, :part_rows], low[:, :part_rows]
            gath[v] = stack(beside(high, high), beside(low, jnp.zeros(low.shape, BF16)))
            turned = blur_y.T[:part_rows]
            high = turned.astype(BF16).astype(F32)
            low = turned - high
            scat[v] = beside(high, high, low).astype(BF16)
        return carry

    def lines_of(dim):
        lane = iota((1, lanes), 1)
        lines = []
        for k in range(length):
            line = jnp.zeros((1, lanes), F32)
            for v in range(views):
                line = jnp.where(lane // span == v, taps_ref[dim, v, k], line)
            lines.append(line)
        return lines

    meet(0)
    start(out_copies((1,), 1, (True,)))
    lane = lax.broadcasted_iota(jnp.int32, (cols, lanes), 1)
    for g in range(rows // 8):
        merged = jnp.zeros((cols, lanes), F32)
        for i in range(8):
            rolled = pltpu.roll(ext[rad + 8 * g + i, own_y, :], 2 * rad * i + rad, 1)
            merged = jnp.where(lane // (2 * rad) == i, rolled, merged)
        pack[g] = merged

    start(out_copies((1,), 0))
    start(out_copies((1,), 1, (False,)))
    loads[2].wait()
    stops = [min(stop, views // 2) for stop in (0, 1, 2, views // 2)]
    for hop in range(1, 4):
        lax.fori_loop(stops[hop - 1], stops[hop], build, 0)
        if hop < min(3, early_rounds):
            meet(hop)
        if hop in (1, 2):
            start(out_copies((hop + 1,), 0))
            start(out_copies((hop + 1,), 1))

    for k, line in enumerate(lines_of(0)):
        taps_x[k : k + 1] = line
    shape = (wide_y, lanes)
    offset = place_y(iota(shape, 0)) + rad - iota(shape, 1) % cols
    base = jnp.zeros(shape, F32)
    for k, line in enumerate(lines_of(1)):
        base = jnp.where(offset == k, line, base)
    high = base.astype(BF16).astype(F32)
    scat_edge[...] = beside(high, high, base - high)

    loads[3].wait()
    def weight_of(rows_of, v):
        first = v * (lanes // views)
        return jnp.broadcast_to(rows_of[:, first : first + 1], rows_of.shape)

    mine = jnp.broadcast_to(weight[13], (8, lanes))
    count = jnp.zeros((8, lanes), F32)
    seen = jnp.zeros((8, lanes), F32)
    for v in range(views):
        weight_v = weight_of(mine, v)
        count = count + weight_v
        seen = seen + weight_v * jnp.sum(obs[v].reshape(-1, 8, lanes), axis=0)
    count = count[0:1]
    wanted = jnp.sum(seen, axis=0, keepdims=True) / count

    def side_of(g):
        return 0 if 8 * g < rad else (1 if 8 * g < rad + rows else 2)

    inner = [g for g in range(groups) if side_of(g) == 1]
    outer = [g for g in range(groups) if side_of(g) != 1]
    place = {g: which for which, g in enumerate(inner + outer)}
    size = 8 * wide_y
    inner_rows, outer_rows = slice(0, size * len(inner)), slice(size * len(inner), size * groups)

    def prepare(chosen_groups):
        lane = iota((wide_y, lanes), 1)
        for g in chosen_groups:
            here = slice(size * place[g], size * (place[g] + 1))
            high, low = split(ext[8 * g : 8 * g + 8].reshape(size, lanes))
            wide_a[here, :lanes] = high
            wide_a[here, lanes:] = low
            wide_b[here, :lanes] = high
            merged = jnp.where(lane % span < rad, from_left[g], from_right[g])
            edge[g] = merged
            high = merged.astype(BF16).astype(F32)
            low = merged - high
            count_of = lanes // span
            highs = [pltpu.roll(high, span * i, 1) if i else high for i in range(count_of)]
            lows = [pltpu.roll(low, span * i, 1) if i else low for i in range(count_of)]
            rows_of = []
            for i in range(8):
                third = jnp.where(lane < 2 * span, lows[(1 - i) % count_of], highs[(2 - i) % count_of])
                terms = jnp.where(lane < span, highs[-i % count_of], third)
                rows_of.append(terms)
            wide_b[here, lanes:] = stack(*rows_of).astype(BF16)

    def weighed(terms):
        result = None
        for factor, value in terms:
            term = factor * value
            result = term if result is None else result + term
        return result

    def added(one, two):
        if one is None or two is None:
            return two if one is None else one
        return one + two

    def blur_x(source, tap):
        taps = [tap(k) for k in range(length)]
        even, odd = taps[0::2], [None] + taps[1::2]
        both = [added(one, two) for one, two in zip(even, odd)]
        reach, columns = len(even), []
        for first in range(0, cols, 8):
            values = [source[e, first : first + 8, :] for e in range(wide_x)]
            left, right = values[0::2], values[1::2]
            joined = [one + two for one, two in zip(left, right)]
            lines, before = [], weighed([(odd[j], right[j - 1]) for j in range(1, reach)])
            for m in range(rows // 2):
                one = weighed([(even[j], left[m + j]) for j in range(reach)])
                two = weighed([(odd[j], right[m + j]) for j in range(1, reach)])
                three = weighed([(both[j], joined[m + j]) for j in range(reach)])
                lines += [one + before, three - (one + two)]
                before = two
            columns.append(lines)
        return [stack(*parts) for parts in zip(*columns)]

    def spread_x(source, tap):
        taps = [tap(k) for k in range(length)]
        even, odd = taps[0::2], taps[1::2] + [None]
        both = [added(one, two) for one, two in zip(even, odd)]
        columns = []
        for first in range(0, cols, 8):
            values = [source[a, first : first + 8, :] for a in range(rows)]
            left, right = values[0::2], values[1::2]
            joined = [one + two for one, two in zip(left, right)]

            def product(factors, parts, n):
                pairs = [(factors[n - i], parts[i]) for i in range(len(parts)) if 0 <= n - i < len(factors)]
                return weighed([pair for pair in pairs if pair[0] is not None])

            lines, before = [], None
            for n in range(wide_x // 2):
                one, two = product(even, left, n), product(odd, right, n)
                three = product(both, joined, n)
                lines += [added(one, before), three - added(one, two)]
                before = two
            columns.append(lines)
        return [stack(*parts) for parts in zip(*columns)]

    def pairs_of(part, half):
        return beside(part[:half], part[half:])

    def blur_zy(p, chosen_groups, row_range, slot):
        blurred[slot, row_range] = dot(wide_a[row_range, :], ahead_a[p]) + dot(wide_b[row_range, :], ahead_b[p])
        for j in range(2):
            v = 2 * p + j
            for g in chosen_groups:
                first = size * place[g]
                high, low = split(blurred[slot, first : first + size, j * lanes : (j + 1) * lanes])
                line = dot(gath[v], stack(pairs_of(high, size // 2), pairs_of(low, size // 2)))
                half = block * cols
                line = line[:half] + line[half:]
                for which in range(2):
                    first = 8 * g + which * block
                    part = line[:, which * lanes : (which + 1) * lanes]
                    lined[v, first : first + block] = part.reshape(block, cols, lanes)

    drain_all(out_recv, sides=(0,))
    if early_rounds > 3:
        meet(3)
    prepare(inner)

    for p in range(views // 2):
        blur_zy(p, inner, inner_rows, p)

    for hop in range(4, early_rounds):
        meet(hop)
    drain_all(weight_recv, rows_only=True)
    drain_all(far_recv, sides=(1,))
    if early_rounds < rounds:
        greet(early_rounds)
    everyone = stack(*[weight[slot] for slot in range(27)], jnp.zeros((5, lanes), F32))
    counts = jnp.zeros(everyone.shape, F32)

    def along_y(rows_of, first):
        return stack(*[jnp.broadcast_to(rows_of[first + dy : first + dy + 1], (size_y, lanes)) for _, size_y, dy in bands_y])

    for v in range(views):
        theirs = weight_of(everyone, v)
        counts = counts + theirs
        for dx in range(3):
            mask[v, dx] = stack(*[along_y(theirs, 9 + 3 * dx)] * block).astype(BF16)
    for dx in range(3):
        terms = []
        for side in range(2):
            part = along_y(everyone, 18 * side + 3 * dx)
            terms.append(scat_edge[...] * beside(part, part, part))
        mask_edge[dx] = stack(*terms).astype(BF16)
    inverses[...] = jnp.where(counts > 0.0, 1.0 / jnp.maximum(counts, 1.0), 0.0)

    prepare(outer)

    def two_views(p, slot):
        blur_zy(p, outer, outer_rows, slot)
        scattered = []
        for j in range(2):
            v = 2 * p + j
            blur = blur_x(lined.at[v], lambda k: taps_ref[0, v, k])
            ratio = obs[v].reshape(rows * cols, lanes) / stack(*blur)
            ratio = beside(*split(ratio))
            back = folded(dot(ratio, astern[v]))
            fringe[...] += dot(ratio, astern_edge[v])
            spread[2 * slot + j] = back.reshape(rows, cols, lanes)
            pieces = spread_x(spread.at[2 * slot + j], lambda k: taps_ref[0, v, k])
            sent = []
            for g in range(groups):
                high, low = split(stack(*pieces[8 * g : 8 * g + 8]))
                high, low = (pairs_of(part, block * cols) for part in (high, low))
                sent.append(stack(high, low, high))
            scattered.append(sent)
        for g in range(groups):
            dx = side_of(g)
            reach = None
            for j in range(2):
                v = 2 * p + j
                here = mask[v, dx]
                here = scat[v] * beside(here, here)[:, : scat.shape[2]]
                part = dot(here, scattered[j][g])
                reach = part if reach is None else reach + part
            for which in range(2):
                first = 8 * g + which * block
                part = reach[:, which * lanes : (which + 1) * lanes]
                total[first : first + block] += part.reshape(block, wide_y, lanes)

    for p in range(views // 2):
        two_views(p, p)
    for hop in range(early_rounds, rounds):
        meet(hop)
    start(back_copies(True))
    def sums_a():
        for slot, offset in enumerate(ring_a):
            yield pltpu.make_async_remote_copy(
                src_ref=stat,
                dst_ref=stat_a.at[slot],
                send_sem=a_send,
                recv_sem=a_recv,
                device_id=partner(*offset),
                device_id_type=MESH,
            )

    def sums_b():
        for slot, offset in enumerate(ring_b):
            yield pltpu.make_async_remote_copy(
                src_ref=part_a,
                dst_ref=stat_b.at[slot],
                send_sem=b_send,
                recv_sem=b_recv,
                device_id=partner(*offset),
                device_id_type=MESH,
            )

    spread[0] = folded(fringe[...]).reshape(rows, cols, lanes)
    pieces = spread_x(spread.at[0], lambda k: taps_x[k : k + 1])
    lane = iota((cols, lanes), 1)
    for g in range(groups):
        turned = pieces[8 * g : 8 * g + 8]
        step = views // 2
        while step:
            low_half = (lane // span) // step % 2 == 0
            for i in range(views):
                if i // step % 2 == 0:
                    one, two = turned[i], turned[i + step]
                    turned[i] = jnp.where(low_half, one, pltpu.roll(two, step * span, 1))
                    turned[i + step] = jnp.where(low_half, pltpu.roll(one, lanes - step * span, 1), two)
            step //= 2
        high, low = split(stack(*turned))
        sides = dot(mask_edge[side_of(g)], stack(high, low, high))
        back_pack[g] = jnp.where(iota((wide_y, lanes), 1) % span < rad, sides[:wide_y], sides[wide_y:])
    lane = iota((wide_y, lanes), 1)
    seen = jnp.zeros((8, lanes), F32)
    for dx in range(3):
        for start_y, size_y, dy in bands_y:
            first_x, last_x = ((0, rad), (rad, rad + rows), (rad + rows, wide_x))[dx]
            part_y = slice(start_y, start_y + size_y)
            part = total[first_x:last_x, part_y, :] * ext[first_x:last_x, part_y, :]
            part = jnp.sum(part.reshape(-1, 8, lanes), axis=0)
            slot = 9 + 3 * dx + dy
            seen = seen + part * inverses[slot : slot + 1, :]
            part_x = slice(first_x // 8, last_x // 8)
            part = back_pack[part_x, part_y, :] * edge[part_x, part_y, :]
            part = jnp.sum(part.reshape(-1, 8, lanes), axis=0)
            left, right = (inverses[at : at + 1, :] for at in (slot - 9, slot + 9))
            seen = seen + part * jnp.where(lane[0:1] % (2 * rad) < rad, left, right)
    wanted = wanted + pltpu.roll(wanted, lanes // 2, 1)
    gotten = jnp.sum(seen, axis=0, keepdims=True)
    gotten = gotten + pltpu.roll(gotten, lanes // 2, 1)
    stat[...] = jnp.where(iota((1, lanes), 1) < lanes // 2, wanted, gotten)

    for copy in sums_a():
        copy.start()
    start(back_copies(False))
    drain_all(back_recv)
    near = back_xy[...]

    def fold(values, size, rad, axis):
        low = lax.slice_in_dim(values, 0, rad, axis=axis)
        mid = lax.slice_in_dim(values, rad, rad + size, axis=axis)
        top = lax.slice_in_dim(values, rad + size, 2 * rad + size, axis=axis)
        if size == 2 * rad:
            return mid + jnp.concatenate([low, top], axis=axis)
        gap_shape = list(low.shape)
        gap_shape[axis] = size - rad
        gap = jnp.zeros(gap_shape, F32)
        return mid + jnp.concatenate([low, gap], axis=axis) + jnp.concatenate([gap, top], axis=axis)

    def fold_y(values):
        if first_y:
            return fold(values, cols, rad, 1)
        part = values[:, cols:]
        gap = jnp.zeros((part.shape[0], cols - rad, lanes), F32)
        before, after = (jnp.concatenate(pair, axis=1) for pair in ((part, gap), (gap, part)))
        return values[:, :cols] + jnp.where(me_y == 0, after, before)

    near = fold_y(fold(near, rows, rad, 0))
    ends = jnp.where((lane % (2 * rad) < rad)[None], back_right[...], back_left[...])
    ends = fold_y(fold(ends, pack_rows, pack_rad, 0))
    lane = lax.broadcasted_iota(jnp.int32, (cols, lanes), 1)
    outer = (lane < rad) | (lane >= lanes - rad)
    for x in range(rows):
        rolled = pltpu.roll(ends[x // 8], lanes - (2 * rad * (x % 8) + rad), 1)
        summed = total[rad + x, own_y, :] + near[x] + jnp.where(outer, rolled, 0.0)
        updated = ext[rad + x, own_y, :] * (summed / count)
        out_ref[x] = updated

    drain(a_recv, len(ring_a))
    everything = stat[...] + jnp.sum(stat_a[...], axis=0)
    if ring_b:
        part_a[...] = everything
        for copy in sums_b():
            copy.start()
        drain(b_recv, len(ring_b))
        everything = part_a[...] + jnp.sum(stat_b[...], axis=0)
    first_half = iota((1, lanes), 1) < lanes // 2
    wanted = jnp.sum(jnp.where(first_half, everything, 0.0), axis=1, keepdims=True)
    gotten = jnp.sum(jnp.where(first_half, 0.0, everything), axis=1, keepdims=True)
    factor = jnp.broadcast_to(wanted, (1, lanes)) / jnp.broadcast_to(gotten, (1, lanes))
    factor_ref[...] = factor

    drain_all(out_send)
    drain_all(weight_send, rows_only=True)
    drain_all(back_send)
    drain(a_send, len(ring_a))
    if ring_b:
        drain(b_send, len(ring_b))


def on_device(sizes, estimate, observed, coverage, psf_taps):
    rows, cols, lanes = estimate.shape
    views = observed.shape[0]
    rad = (psf_taps.shape[2] - 1) // 2
    wide_x, wide_y = rows + 2 * rad, extent_y(sizes[1], cols, rad)
    groups, block = wide_x // 8, lanes // (cols + 2 * rad)
    _, ring_a, ring_b = rings(sizes)
    n_a, n_b = len(ring_a), max(1, len(ring_b))

    def vm(*shape, dtype=F32):
        return pltpu.VMEM(shape, dtype)

    def dma(*shape):
        return pltpu.SemaphoreType.DMA(shape)

    def in_hbm(values):
        return pltpu.with_memory_space_constraint(values, pltpu.HBM)

    views_all, dims, length = psf_taps.shape
    scratch = [
        pltpu.SMEM((dims, views_all, length), F32),
        pltpu.SMEM((views,), jnp.int32),
        vm(*observed.shape),
        vm(wide_x, wide_y, lanes),
        vm(wide_x * wide_y, 2 * lanes, dtype=BF16),
        vm(wide_x * wide_y, 2 * lanes, dtype=BF16),
        vm(rows // 8, cols, lanes),
        vm(groups, wide_y, lanes),
        vm(groups, wide_y, lanes),
        vm(groups, wide_y, lanes),
        vm(27, 1, lanes),
        vm(32, lanes),
        vm(views, 3, block * wide_y, lanes, dtype=BF16),
        vm(3, 2 * wide_y, 3 * lanes, dtype=BF16),
        vm(views // 2, 2 * lanes, 2 * lanes, dtype=BF16),
        vm(views // 2, 2 * lanes, 2 * lanes, dtype=BF16),
        vm(views, 2 * block * cols, 2 * block * wide_y, dtype=BF16),
        vm(views, block * wide_y, 3 * block * cols, dtype=BF16),
        vm(views, 2 * lanes, 2 * lanes, dtype=BF16),
        vm(views, 2 * lanes, 2 * lanes, dtype=BF16),
        vm(24, lanes),
        vm(wide_y, 3 * lanes),
        vm(views // 2, wide_x * wide_y, 2 * lanes),
        vm(views, wide_x, cols, lanes),
        vm(views, rows, cols, lanes),
        vm(rows * cols, 2 * lanes),
        vm(wide_x, wide_y, lanes),
        vm(groups, wide_y, lanes),
        vm(groups, wide_y, lanes),
        vm(groups, wide_y, lanes),
        vm(wide_x, wide_y, lanes),
        vm(1, lanes),
        vm(n_a, 1, lanes),
        vm(n_b, 1, lanes),
        vm(1, lanes),
        vm(5 * rows * cols, 1, lanes),
        dma(4),
        pltpu.SemaphoreType.REGULAR((max(1, min(EARLY, sum(sizes) - 3) + late_rounds(sizes)),)),
        *[pltpu.SemaphoreType.DMA] * 11,
    ]
    updated, factor = pl.pallas_call(
        functools.partial(kernel, sizes),
        out_shape=(jax.ShapeDtypeStruct(estimate.shape, F32), jax.ShapeDtypeStruct((1, lanes), F32)),
        in_specs=[
            pl.BlockSpec(memory_space=pl.ANY),
            pl.BlockSpec(memory_space=pl.ANY),
            pl.BlockSpec(memory_space=pl.ANY),
            pl.BlockSpec(memory_space=pl.ANY),
        ],
        out_specs=(pl.BlockSpec(memory_space=pltpu.VMEM), pl.BlockSpec(memory_space=pltpu.VMEM)),
        scratch_shapes=scratch,
        compiler_params=pltpu.CompilerParams(collective_id=0, has_side_effects=True, vmem_limit_bytes=40 * 1024 * 1024),
    )(*map(in_hbm, (jnp.transpose(psf_taps, (1, 0, 2)), coverage.reshape(views), estimate, observed)))
    return updated * factor.reshape(1, 1, lanes)


def solution(mesh):
    sizes = tuple(mesh.shape[axis] for axis in ("bx", "by", "bz"))
    return jax.shard_map(
        functools.partial(on_device, sizes),
        mesh=mesh,
        in_specs=(P("bx", "by", "bz"), P(None, "bx", "by", "bz"), P(None, "bx", "by", "bz"), P()),
        out_specs=P("bx", "by", "bz"),
        check_vma=False,
    )
```
